256 devices in a mesh: tok: 32 (over y, z_hi, core), cand: 8 (over x, z_lo).
Axes of the slice: x: 4, y: 4, z: 8 (z_hi: 4, z_lo: 2; z = z_hi * 2 + z_lo), core: 2. Of those that a mesh axis runs over, the one named last changes fastest.
Arguments:
- dec_hidden: bfloat16 [2, 64, 32, 2048], P(None, 'cand'), may hold values from -6 to 6
- enc_keys: bfloat16 [2, 4096, 2048], P(None, 'tok'), may hold values from -250 to 250
- enc_values: bfloat16 [2, 4096, 2048], P(None, 'tok'), may hold values from -72 to 72
- enc_lengths: int32 [2], replicated, may hold values from 1024 to 4096, as said below
- cand_counts: int32 [2], replicated, may hold values from 16 to 64, as said below
- gold_ids: int32 [2, 64, 32], P(None, 'cand'), may hold values from 0 to 32127
- gain_cross: float32 [2048], replicated, may hold values from 0.25 to 1.75
- w_query: bfloat16 [2048, 2048], P('cand', 'tok'), may hold values from -0.125 to 0.125
- w_out: bfloat16 [2048, 2048], P('tok', 'cand'), may hold values from -0.125 to 0.125
- gain_ffn: float32 [2048], replicated, may hold values from 0.25 to 1.75
- w_in_gate: bfloat16 [2048, 5120], P('cand', 'tok'), may hold values from -0.125 to 0.125
- w_in_up: bfloat16 [2048, 5120], P('cand', 'tok'), may hold values from -0.125 to 0.125
- w_ffn_out: bfloat16 [5120, 2048], P('tok', 'cand'), may hold values from -0.25 to 0.25
- gain_final: float32 [2048], replicated, may hold values from 0.25 to 1.75
- w_vocab: bfloat16 [2048, 32128], P('cand', 'tok'), may hold values from -20 to 20
Outputs:
- cand_scores: float32 [2, 64], P(None, 'cand')
- best_score: float32 [2], replicated
The draws below stay inside these ranges and needn't reach their ends.
Inputs may be any that keep to these rules, and one draw needn't show every extreme that they name: `enc_lengths`: some query has all 4096 encoder tokens live. `cand_counts`: some query has all 64 candidates live.
All inputs are finite; a program needn't handle non-finite values.
Results may differ from the reference program's by a relative error of at most 0.0014.
The reference program's roundings to bfloat16 on the way count: a program that leaves them out, or rounds other values in their place, can miss the bound.
Values may be sent and summed in bfloat16 or wider, within the bound.
A program may use at most 64 MiB of HBM per device.

```python
import math
import jax
import jax.numpy as jnp
import numpy as np
from jax import lax

D = 2048
HEADS = 32
HEAD_DIM = 64
FF = 5120
VOCAB = 32128
QUERIES = 2
LENGTH = 32
CANDS = 64
SRC = 4096


def draw_enc_keys(key, part):
    base = 0.25 * jax.random.truncated_normal(key, -6.0, 6.0, (QUERIES, SRC, D), jnp.float32)
    return base.astype(jnp.bfloat16)


def draw_w_vocab(key, part):
    base = 4.0 * jax.random.truncated_normal(key, -6.0, 6.0, (D, VOCAB), jnp.float32) / jnp.sqrt(float(D))
    return jnp.clip(base, -20.0, 20.0).astype(jnp.bfloat16)


def draw_enc_lengths(key, part):
    drawn = jax.random.randint(key, (QUERIES,), SRC // 4, SRC + 1)
    chosen = jax.random.randint(jax.random.fold_in(key, 7), (), 0, QUERIES)
    return jnp.where(jnp.arange(QUERIES) == chosen, SRC, drawn).astype(jnp.int32)


def draw_cand_counts(key, part):
    drawn = jax.random.randint(key, (QUERIES,), CANDS // 4, CANDS + 1)
    chosen = jax.random.randint(jax.random.fold_in(key, 11), (), 0, QUERIES)
    return jnp.where(jnp.arange(QUERIES) == chosen, CANDS, drawn).astype(jnp.int32)


def set_ends(values, stream_key, smallest, largest):
    place = [jax.random.randint(jax.random.fold_in(stream_key, axis), (), 0, length) for axis, length in enumerate(values.shape)]
    longest = values.shape.index(max(values.shape))
    beside = place[:longest] + [(place[longest] + 1) % values.shape[longest]] + place[longest + 1:]
    return values.at[tuple(place)].set(smallest).at[tuple(beside)].set(largest)


def block_levels(own_key, dims, split, smallest, top_value):
    level, own = 1.0, jax.random.fold_in(own_key, 6)
    for axis_at, blocks in split:
        heights = jnp.exp(jax.random.uniform(jax.random.fold_in(own, axis_at), (blocks,), jnp.float32, smallest / len(split), top_value / len(split)))
        level = level * jnp.repeat(heights, dims[axis_at] // blocks).reshape([-1 if axis == axis_at else 1 for axis in range(len(dims))])
    return level


def rank_table(count, skew):
    portions = [(1 << 20) // math.isqrt(rank ** skew) + 1 for rank in range(1, count + 1)]
    width = 1 + sum(portions) // (1 << 30)
    return np.cumsum(np.array([max(1, weight // width) for weight in portions]))


def ranked(own_key, shape, number_of, slope):
    grid = rank_table(number_of, slope)
    lot = jax.random.randint(jax.random.fold_in(own_key, 1), shape, 0, int(grid[number_of - 1]))
    grade = jnp.searchsorted(jnp.asarray(grid, jnp.int32), lot, side="right")
    return jax.random.permutation(jax.random.fold_in(own_key, 2), number_of)[grade].astype(jnp.int32)


def centred(stream_key, extent, deviation, limit, shards=(), kind=jnp.bfloat16):
    values = jax.random.normal(stream_key, extent, jnp.float32) * deviation
    if len(shards) > 0:
        values = block_levels(stream_key, extent, shards, -0.22, 0.18) * values
    return jnp.clip(values, min=-limit, max=limit).astype(kind)


def setup_inputs(seed: int = 0) -> dict:
    keys = jax.random.split(jax.random.key(seed), 16)
    return {
        "dec_hidden": centred(keys[0], (QUERIES, CANDS, LENGTH, D), 1.0, 6.0, ((1, 8),)),
        "enc_keys": draw_enc_keys(jax.random.fold_in(keys[15], 71), 0),
        "enc_values": centred(keys[2], (QUERIES, SRC, D), 12.0, 72.0, ((1, 32),)),
        "enc_lengths": draw_enc_lengths(jax.random.fold_in(keys[15], 71), 0),
        "cand_counts": draw_cand_counts(jax.random.fold_in(keys[15], 71), 0),
        "gold_ids": set_ends(ranked(keys[5], (QUERIES, CANDS, LENGTH), VOCAB, 2), jax.random.fold_in(keys[5], 3), 0, VOCAB - 1).astype(jnp.int32),
        "gain_cross": jnp.clip(1.0 + 0.15 * jax.random.normal(keys[6], (D,), jnp.float32), 0.25, 1.75),
        "w_query": centred(keys[7], (D, D), D ** -0.5, 0.125, ((0, 8), (1, 32))),
        "w_out": centred(keys[8], (D, D), D ** -0.5, 0.125, ((0, 32), (1, 8))),
        "gain_ffn": jnp.clip(1.0 + 0.15 * jax.random.normal(keys[9], (D,), jnp.float32), 0.25, 1.75),
        "w_in_gate": centred(keys[10], (D, FF), D ** -0.5, 0.125, ((0, 8), (1, 32))),
        "w_in_up": centred(keys[11], (D, FF), D ** -0.5, 0.125, ((0, 8), (1, 32))),
        "w_ffn_out": centred(keys[12], (FF, D), (FF // 9) ** -0.5, 0.25, ((0, 32), (1, 8))),
        "gain_final": jnp.clip(1.0 + 0.15 * jax.random.normal(keys[13], (D,), jnp.float32), 0.25, 1.75),
        "w_vocab": draw_w_vocab(jax.random.fold_in(keys[15], 71), 0),
    }


norm_eps = 0.25

def root_norm(values, gain):
    squares = lax.optimization_barrier(jnp.mean(values * values, axis=-1, keepdims=True))
    return values * lax.rsqrt(squares + norm_eps) * gain

def reference(dec_hidden, enc_keys, enc_values, enc_lengths, cand_counts, gold_ids, gain_cross, w_query, w_out, gain_ffn, w_in_gate, w_in_up, w_ffn_out, gain_final, w_vocab):
    total_rows = QUERIES * CANDS * LENGTH
    inputs_flat = dec_hidden.reshape(total_rows, D).astype(jnp.float32)
    normed = root_norm(inputs_flat, gain_cross).astype(jnp.bfloat16)
    queries_all = jnp.dot(normed, w_query, preferred_element_type=jnp.float32).astype(jnp.bfloat16)
    queries_all = lax.optimization_barrier(queries_all)
    query_heads = queries_all.reshape(QUERIES, CANDS * LENGTH, HEADS, HEAD_DIM).transpose(2, 0, 1, 3).astype(jnp.float32)
    key_heads = enc_keys.reshape(QUERIES, SRC, HEADS, HEAD_DIM).transpose(2, 0, 1, 3).astype(jnp.float32)
    value_heads = enc_values.reshape(QUERIES, SRC, HEADS, HEAD_DIM).transpose(2, 0, 1, 3).astype(jnp.float32)
    live_keys = jnp.arange(SRC, dtype=jnp.int32)[None, :] < enc_lengths[:, None]

    def attend(operands):
        query_head, key_head, value_head = operands
        scores = jnp.einsum('brd,bsd->brs', query_head, key_head, precision=lax.Precision.HIGHEST)
        scores = jnp.where(live_keys[:, None, :], scores, -1e+30)
        row_max = lax.optimization_barrier(jnp.max(scores, axis=-1, keepdims=True))
        weights = jnp.where(live_keys[:, None, :], jnp.exp(scores - row_max), 0.0)
        denominator = lax.optimization_barrier(jnp.sum(weights, axis=-1, keepdims=True))
        rounded = lax.optimization_barrier(weights.astype(jnp.bfloat16)).astype(jnp.float32)
        mixed_values = jnp.einsum('brs,bsd->brd', rounded, value_head, precision=lax.Precision.HIGHEST)
        return (mixed_values / denominator).astype(jnp.bfloat16)
    attended = lax.map(attend, (query_heads, key_heads, value_heads))
    attended = attended.transpose(1, 2, 0, 3).reshape(total_rows, D)
    after_cross = inputs_flat + jnp.dot(attended, w_out, preferred_element_type=jnp.float32)
    normed_ffn = root_norm(after_cross, gain_ffn).astype(jnp.bfloat16)
    gate_part = jnp.dot(normed_ffn, w_in_gate, preferred_element_type=jnp.float32)
    up_part = jnp.dot(normed_ffn, w_in_up, preferred_element_type=jnp.float32)
    hidden = (jax.nn.gelu(gate_part, approximate=True) * up_part).astype(jnp.bfloat16)
    after_ffn = after_cross + jnp.dot(hidden, w_ffn_out, preferred_element_type=jnp.float32)
    normed_final = root_norm(after_ffn, gain_final).astype(jnp.bfloat16)
    block_rows = 512 if total_rows % 512 == 0 else total_rows

    def score_block(operands):
        rows_block, gold_block = operands
        logits = jnp.dot(rows_block, w_vocab, preferred_element_type=jnp.float32)
        row_max = lax.optimization_barrier(jnp.max(logits, axis=1))
        sum_exp = lax.optimization_barrier(jnp.sum(jnp.exp(logits - row_max[:, None]), axis=1))
        picked = jnp.take_along_axis(logits, gold_block[:, None], axis=1)[:, 0]
        return picked - row_max - jnp.log(sum_exp)
    logprob = lax.map(score_block, (normed_final.reshape(-1, block_rows, D), gold_ids.reshape(-1, block_rows)))
    per_cand = lax.optimization_barrier(jnp.mean(logprob.reshape(QUERIES, CANDS, LENGTH), axis=2))
    valid_cand = jnp.arange(CANDS, dtype=jnp.int32)[None, :] < cand_counts[:, None]
    cand_scores = jnp.where(valid_cand, per_cand, 0.0)
    best_score = lax.optimization_barrier(jnp.max(jnp.where(valid_cand, per_cand, -1e+30), axis=1))
    return (cand_scores, best_score)
```

```python
import functools

import jax
import jax.numpy as jnp
from jax import lax
from jax.experimental import pallas as pl
from jax.experimental.pallas import tpu as pltpu
from jax.sharding import PartitionSpec as P

MESH = pl.DeviceIdType.MESH
EPS = 0.25
NY, NZ, NX = 4, 4, 4
TOK, CAND = 32, 8
D = 2048
HALF = 1024
ROWS = 256
NEG = -1e30
BF = jnp.bfloat16
F32 = jnp.float32


def rms(v, gain):
    squares = jnp.mean(v * v, axis=-1, keepdims=True)
    return v * lax.rsqrt(squares + EPS) * gain


def gelu(v):
    inner = 0.7978845608028654 * (v + 0.044715 * (v * v * v))
    return 0.5 * v * (1.0 + jnp.tanh(inner))


def landed(ref, sem):
    pltpu.make_async_copy(ref, ref, sem).wait()


def kernel(
    x_in, keys, vals, lens, counts, gold, gain1, wq_in, wo_in, gain2, wi_in, fo_in, gain3, wv_in,
    scores_out, best_out,
    xv, nx, q2, kb, vb, sc, pb, at,
    wq, wo, wi, fo, wv,
    part, ryf, ryd, rya, sy, by, rzf, rzd, rza, sz, ac, nf,
    hid, st, f1, f2,
    kv_recv, kv_send, g_recv, g_send, g_own, g_dual, g_dsend,
    rs_recv, rs_send, ag_recv, ag_send, f_recv, f_send, l_sem,
):
    t = lax.axis_index("tok")
    c = lax.axis_index("cand")
    k = lax.rem(t, 2)
    j = lax.div(t, 2)
    y = lax.div(j, NZ)
    z = lax.rem(j, NZ)
    xx = lax.div(c, 2)
    zl = lax.rem(c, 2)

    def tok_of(yy, zz):
        return (lax.rem(yy, NY) * NZ + lax.rem(zz, NZ)) * 2 + k

    def cand_of(x_at, z_at):
        return lax.rem(x_at, NX) * 2 + z_at

    partner = t + 1 - 2 * k
    cz = cand_of(xx, 1 - zl)
    cp, cm = cand_of(xx + 1, zl), cand_of(xx + 3, zl)
    cpz, cmz = cand_of(xx + 1, 1 - zl), cand_of(xx + 3, 1 - zl)
    co, coz = cand_of(xx + 2, zl), cand_of(xx + 2, 1 - zl)

    def send(src, dst, s_sem, r_sem, tok, cand):
        pltpu.make_async_remote_copy(
            src_ref=src, dst_ref=dst, send_sem=s_sem, recv_sem=r_sem,
            device_id=(tok, cand), device_id_type=MESH,
        ).start()

    x_copy = pltpu.make_async_copy(x_in.at[k], xv, l_sem.at[0])
    x_copy.start()

    barrier = pltpu.get_barrier_semaphore()

    @pl.loop(1, TOK)
    def _(d):
        pl.semaphore_signal(
            barrier, inc=1, device_id=(lax.rem(t + d, TOK), c), device_id_type=MESH
        )

    @pl.loop(1, CAND)
    def _(d):
        pl.semaphore_signal(
            barrier, inc=1, device_id=(t, lax.rem(c + d, CAND)), device_id_type=MESH
        )
        pl.semaphore_signal(
            barrier, inc=1, device_id=(partner, lax.rem(c + d, CAND)), device_id_type=MESH
        )

    def q_at(cc, part=None):
        if part is None:
            return wq.at[k, pl.ds(256 * cc, 256), :]
        return wq.at[k, pl.ds(256 * cc + 128 * part, 128), :]

    def o_at(cc, part=None):
        if part is None:
            return wo.at[cc, pl.ds(64 * k, 64), :]
        return wo.at[cc, pl.ds(64 * k + 32 * part, 32), :]

    def i_at(cc, part=None):
        if part is None:
            return wi.at[k, pl.ds(256 * cc, 256), :]
        return wi.at[k, pl.ds(256 * cc + 128 * part, 128), :]

    def fo_at(cc, part=None):
        if part is None:
            return fo.at[cc, pl.ds(160 * k, 160), :]
        return fo.at[cc, pl.ds(160 * k + 80 * part, 80), :]

    def v_at(cc, part=None):
        if part is None:
            return wv.at[k, pl.ds(256 * cc, 256), :]
        return wv.at[k, pl.ds(256 * cc + 128 * part, 128), :]

    def kv_at(ref):
        def at_(cc, part=None):
            if part is None:
                return ref.at[pl.ds(512 * cc, 512), :]
            return ref.at[pl.ds(512 * cc + 256 * part, 256), :]
        return at_

    places = [q_at, o_at, i_at, fo_at, v_at, kv_at(kb), kv_at(vb)]
    whole = [
        lambda h: wq.at[h], lambda h: wo.at[:, pl.ds(64 * h, 64), :], lambda h: wi.at[h],
        lambda h: fo.at[:, pl.ds(160 * h, 160), :], lambda h: wv.at[h],
    ]
    inputs = [wq_in, wo_in, wi_in, fo_in, wv_in]

    def own_copy(n):
        return pltpu.make_async_copy(inputs[n], places[n](c), g_own.at[n])

    def g_send_to(n, slot, src, dst, cand):
        send(src, dst, g_send.at[n, slot], g_recv.at[n, slot], t, cand)

    def step1(n):
        at_, src = places[n], (inputs[n] if n < 5 else places[n](c))
        g_send_to(n, 0, src, at_(c), cz)
        g_send_to(n, 1, src, at_(c), cp)
        g_send_to(n, 2, src, at_(c), cm)

    def step2(n):
        at_ = places[n]
        landed(at_(cz), g_recv.at[n, 0])
        g_send_to(n, 3, at_(cz), at_(cz), cp)
        g_send_to(n, 4, at_(cz), at_(cz), cm)
        landed(at_(cm), g_recv.at[n, 1])
        g_send_to(n, 5, at_(cm, 0), at_(cm, 0), cp)
        landed(at_(cp), g_recv.at[n, 2])
        g_send_to(n, 6, at_(cp, 1), at_(cp, 1), cm)

    def step3(n):
        at_ = places[n]
        landed(at_(cmz), g_recv.at[n, 3])
        g_send_to(n, 7, at_(cmz, 0), at_(cmz, 0), cp)
        landed(at_(cpz), g_recv.at[n, 4])
        g_send_to(n, 8, at_(cpz, 1), at_(cpz, 1), cm)

    def step4(n):
        at_ = places[n]
        landed(at_(co, 0), g_recv.at[n, 5])
        landed(at_(co, 1), g_recv.at[n, 6])
        landed(at_(coz, 0), g_recv.at[n, 7])
        landed(at_(coz, 1), g_recv.at[n, 8])
        if n < 5:
            own_copy(n).wait()
            send(whole[n](k), whole[n](k), g_dsend.at[n], g_dual.at[n], partner, c)

    def both(n):
        landed(whole[n](1 - k), g_dual.at[n])

    for n in range(5):
        own_copy(n).start()

    x_copy.wait()

    @pl.loop(0, 8)
    def _(i):
        rows = xv[i].astype(F32)
        nx[pl.ds(pl.multiple_of(32 * i, 32), 32), :] = rms(rows, gain1[...]).astype(BF)

    pl.semaphore_wait(barrier, TOK - 1 + 2 * (CAND - 1))

    step1(0)

    for n, (src, dst) in enumerate(((keys, kb), (vals, vb))):
        here = dst.at[pl.ds(512 * c + 16 * t, 16), :]
        pltpu.make_async_copy(
            src.at[k, pl.ds(16 * c, 16), pl.ds(pl.multiple_of(128 * j, 128), 128)],
            here, l_sem.at[1 + n],
        ).start()

        @pl.loop(1, TOK)
        def _(d, src=src, n=n, here=here):
            to = lax.rem(t + d, TOK)
            send(
                src.at[
                    lax.rem(to, 2), pl.ds(16 * c, 16),
                    pl.ds(pl.multiple_of(128 * lax.div(to, 2), 128), 128),
                ],
                here, kv_send.at[n], kv_recv.at[n], to, c,
            )

    def kv_mine(n):
        ref = (kb, vb)[n]
        pltpu.make_async_copy(
            ref.at[pl.ds(0, 16), :], ref.at[pl.ds(512 * c + 16 * t, 16), :], l_sem.at[1 + n]
        ).wait()
        landed(ref.at[pl.ds(0, 496), :], kv_recv.at[n])

    step1(1)
    step1(2)
    step1(3)

    step2(0)
    step3(0)
    step4(0)
    kv_mine(0)
    step1(5)
    kv_mine(1)
    step1(6)
    both(0)
    zero = jnp.zeros((ROWS, 64), BF)
    first = jnp.dot(nx[...], wq[0], preferred_element_type=F32).astype(BF)
    q2[pl.ds(0, ROWS), :] = jnp.concatenate([first, zero], axis=1)
    second = jnp.dot(nx[...], wq[1], preferred_element_type=F32).astype(BF)
    q2[pl.ds(ROWS, ROWS), :] = jnp.concatenate([zero, second], axis=1)

    length = lens[k]

    def score(cc):
        place = lax.broadcasted_iota(jnp.int32, (1, 512), 1)
        token = lax.div(place, 16) * 128 + 16 * cc + lax.rem(place, 16)
        live = token < length
        block = kb[pl.ds(pl.multiple_of(512 * cc, 512), 512), :]

        @pl.loop(0, 4)
        def _(r):
            rows = pl.ds(pl.multiple_of(128 * r, 128), 128)
            s = lax.dot_general(
                q2[rows, :], block, (((1,), (1,)), ((), ())), preferred_element_type=F32
            )
            sc[cc, rows, :] = jnp.where(live, s, NEG)

    step2(5)
    step2(6)
    score(c)
    step3(5)
    step3(6)
    step1(4)
    score(cz)
    score(cm)
    score(cp)
    step2(1)
    step2(2)
    step2(3)
    score(cmz)
    score(cpz)
    step4(5)
    score(co)
    score(coz)
    step3(1)
    step3(2)
    step3(3)

    @pl.loop(0, 16)
    def _(r):
        rows = pl.ds(pl.multiple_of(32 * r, 32), 32)
        high = sc[0, rows, :]
        for cc in range(1, CAND):
            high = jnp.maximum(high, sc[cc, rows, :])
        top = jnp.max(high, axis=1, keepdims=True)
        total = jnp.zeros((32, 512), F32)
        for cc in range(CAND):
            w = jnp.exp(sc[cc, rows, :] - top)
            total = total + w
            pb[rows, pl.ds(512 * cc, 512)] = w.astype(BF)
        st[rows, :] = jnp.broadcast_to(jnp.sum(total, axis=1, keepdims=True), (32, 128))

    step4(1)
    step4(2)
    step4(3)
    step4(6)

    @pl.loop(0, 4)
    def _(r):
        low = pl.ds(pl.multiple_of(64 * r, 64), 64)
        upp = pl.ds(pl.multiple_of(64 * r + ROWS, 64), 64)
        a = jnp.dot(pb[low, :], vb[...], preferred_element_type=F32) / st[low, :]
        b = jnp.dot(pb[upp, :], vb[...], preferred_element_type=F32) / st[upp, :]
        lane = lax.broadcasted_iota(jnp.int32, (64, 128), 1)
        at[low, :] = jnp.where(lane < 64, a, b).astype(BF)

    both(1)
    for cc in range(CAND):
        part[0, cc // 4, :, pl.ds(256 * (cc % 4), 256)] = jnp.dot(
            at[...], wo[cc], preferred_element_type=F32
        ).astype(BF)

    ty, tm = tok_of(y + 1, z), tok_of(y + 3, z)
    tz, tn = tok_of(y, z + 1), tok_of(y, z + 3)

    def y_rows(dy):
        return pl.ds(pl.multiple_of(64 * lax.rem(y + dy, NY), 64), 64)

    def z_rows(dz):
        return pl.ds(pl.multiple_of(16 * lax.rem(z + dz, NZ), 16), 16)

    my_rows = pl.ds(pl.multiple_of(64 * y + 16 * z, 16), 16)

    def reduce_sums(p):
        def go(n, src, dst, tok):
            send(src, dst, rs_send.at[p, n], rs_recv.at[p, n], tok, c)

        go(0, part.at[p, 0, y_rows(2)], ryf.at[p, 0], ty)
        go(1, part.at[p, 1, y_rows(2)], ryf.at[p, 1], tm)
        go(2, part.at[p, 1, y_rows(1)], ryd.at[p, 1], ty)
        go(3, part.at[p, 0, y_rows(3)], ryd.at[p, 0], tm)
        landed(ryf.at[p, 0], rs_recv.at[p, 0])
        sy[p, 0] = (ryf[p, 0].astype(F32) + part[p, 0, y_rows(1)].astype(F32)).astype(BF)
        go(4, sy.at[p, 0], rya.at[p, 0], ty)
        landed(ryf.at[p, 1], rs_recv.at[p, 1])
        sy[p, 1] = (ryf[p, 1].astype(F32) + part[p, 1, y_rows(3)].astype(F32)).astype(BF)
        go(5, sy.at[p, 1], rya.at[p, 1], tm)
        landed(ryd.at[p, 1], rs_recv.at[p, 2])
        landed(ryd.at[p, 0], rs_recv.at[p, 3])
        for h in range(2):
            landed(rya.at[p, h], rs_recv.at[p, 4 + h])
            by[p, h] = (
                rya[p, h].astype(F32) + ryd[p, h].astype(F32)
                + part[p, h, y_rows(0)].astype(F32)
            ).astype(BF)
        go(6, by.at[p, 0, z_rows(2)], rzf.at[p, 0], tz)
        go(7, by.at[p, 1, z_rows(2)], rzf.at[p, 1], tn)
        go(8, by.at[p, 1, z_rows(1)], rzd.at[p, 1], tz)
        go(9, by.at[p, 0, z_rows(3)], rzd.at[p, 0], tn)
        landed(rzf.at[p, 0], rs_recv.at[p, 6])
        sz[p, 0] = (rzf[p, 0].astype(F32) + by[p, 0, z_rows(1)].astype(F32)).astype(BF)
        go(10, sz.at[p, 0], rza.at[p, 0], tz)
        landed(rzf.at[p, 1], rs_recv.at[p, 7])
        sz[p, 1] = (rzf[p, 1].astype(F32) + by[p, 1, z_rows(3)].astype(F32)).astype(BF)
        go(11, sz.at[p, 1], rza.at[p, 1], tn)
        landed(rzd.at[p, 1], rs_recv.at[p, 8])
        landed(rzd.at[p, 0], rs_recv.at[p, 9])
        sums = []
        for h in range(2):
            landed(rza.at[p, h], rs_recv.at[p, 10 + h])
            sums.append(
                rza[p, h].astype(F32) + rzd[p, h].astype(F32)
                + by[p, h, z_rows(0)].astype(F32)
            )
        return jnp.concatenate(sums, axis=1)

    def spread(p, value):
        nf[p, 0, my_rows, :] = value[:, :HALF]
        nf[p, 1, my_rows, :] = value[:, HALF:]

        def go(n, where, tok):
            send(where, where, ag_send.at[p, n], ag_recv.at[p, n], tok, c)

        def z_block(dz):
            return pl.ds(pl.multiple_of(64 * y + 16 * lax.rem(z + dz, NZ), 16), 16)

        go(0, nf.at[p, :, my_rows, :], tz)
        go(1, nf.at[p, :, my_rows, :], tn)
        landed(nf.at[p, :, z_block(3), :], ag_recv.at[p, 0])
        go(2, nf.at[p, 0, z_block(3), :], tz)
        landed(nf.at[p, :, z_block(1), :], ag_recv.at[p, 1])
        go(3, nf.at[p, 1, z_block(1), :], tn)
        landed(nf.at[p, 0, z_block(2), :], ag_recv.at[p, 2])
        landed(nf.at[p, 1, z_block(2), :], ag_recv.at[p, 3])
        go(4, nf.at[p, :, y_rows(0), :], ty)
        go(5, nf.at[p, :, y_rows(0), :], tm)
        landed(nf.at[p, :, y_rows(3), :], ag_recv.at[p, 4])
        go(6, nf.at[p, 0, y_rows(3), :], ty)
        landed(nf.at[p, :, y_rows(1), :], ag_recv.at[p, 5])
        go(7, nf.at[p, 1, y_rows(1), :], tm)
        landed(nf.at[p, 0, y_rows(2), :], ag_recv.at[p, 6])
        landed(nf.at[p, 1, y_rows(2), :], ag_recv.at[p, 7])

    mine = xv[2 * y + lax.div(z, 2), pl.ds(pl.multiple_of(16 * lax.rem(z, 2), 16), 16), :]
    ac[...] = mine.astype(F32) + reduce_sums(0)
    step2(4)
    spread(0, rms(ac[...], gain2[...]).astype(BF))
    step3(4)
    both(2)
    both(3)

    @pl.loop(0, 4)
    def _(r):
        rows = pl.ds(pl.multiple_of(64 * r, 64), 64)
        for h in range(2):
            o = jnp.dot(
                nf[0, 0, rows, :], wi[h, pl.ds(0, HALF), :], preferred_element_type=F32
            ) + jnp.dot(
                nf[0, 1, rows, :], wi[h, pl.ds(HALF, HALF), :], preferred_element_type=F32
            )
            hid[h, rows, :] = (gelu(o[:, :160]) * o[:, 160:320]).astype(BF)
        for cc in range(CAND):
            part[1, cc // 4, rows, pl.ds(256 * (cc % 4), 256)] = (
                jnp.dot(hid[0, rows, :], fo[cc, pl.ds(0, 160), :], preferred_element_type=F32)
                + jnp.dot(hid[1, rows, :], fo[cc, pl.ds(160, 160), :], preferred_element_type=F32)
            ).astype(BF)

    after = ac[...] + reduce_sums(1)
    step4(4)
    spread(1, rms(after, gain3[...]).astype(BF))
    both(4)

    width = wv.shape[2]
    ids = gold[k].astype(F32)
    eye = lax.broadcasted_iota(jnp.int32, (32, 32), 0) == lax.broadcasted_iota(jnp.int32, (32, 32), 1)
    start = [((2 * j + h) * width).astype(F32) for h in range(2)]

    for i in range(8):
        column = jnp.sum(
            jnp.where(eye, jnp.broadcast_to(ids[i : i + 1, :], (32, 32)), 0.0), axis=1, keepdims=True
        )
        st[pl.ds(32 * i, 32), :] = jnp.broadcast_to(column, (32, 128))

    @pl.loop(0, 4)
    def _(r):
        rows = pl.ds(pl.multiple_of(64 * r, 64), 64)
        wanted = st[rows, :][:, :1]
        logits = []
        for h in range(2):
            logits.append(
                jnp.dot(nf[1, 0, rows, :], wv[h, pl.ds(0, HALF), :], preferred_element_type=F32)
                + jnp.dot(nf[1, 1, rows, :], wv[h, pl.ds(HALF, HALF), :], preferred_element_type=F32)
            )
        high = jnp.maximum(
            jnp.max(logits[0], axis=1, keepdims=True), jnp.max(logits[1], axis=1, keepdims=True)
        )
        total = jnp.zeros((64, 1), F32)
        picked = jnp.zeros((64, 1), F32)
        for h in range(2):
            total = total + jnp.sum(jnp.exp(logits[h] - high), axis=1, keepdims=True)
            at_col = lax.broadcasted_iota(jnp.int32, (64, width), 1).astype(F32) + start[h]
            picked = picked + jnp.sum(
                jnp.where(at_col == wanted, logits[h], 0.0), axis=1, keepdims=True
            )
        lane = lax.broadcasted_iota(jnp.int32, (64, 128), 1)
        st[pl.ds(pl.multiple_of(256 + 64 * r, 64), 64), :] = jnp.where(
            lane == 0, high, jnp.where(lane == 1, total, picked)
        )

    stats = st[pl.ds(256, 256), :].T
    f1[j] = stats[0:8, :]

    @pl.loop(1, 16)
    def _(d):
        to = lax.rem(j + d, 16) * 2 + k
        send(f1.at[j], f1.at[j], f_send.at[0], f_recv.at[0], to, c)

    landed(f1.at[pl.ds(0, 15)], f_recv.at[0])
    top = f1[0][0:1, :]
    for n in range(1, 16):
        top = jnp.maximum(top, f1[n][0:1, :])
    total = jnp.zeros((1, ROWS), F32)
    picked = jnp.zeros((1, ROWS), F32)
    for n in range(16):
        total = total + f1[n][1:2, :] * jnp.exp(f1[n][0:1, :] - top)
        picked = picked + f1[n][2:3, :]
    logprob = picked - top - jnp.log(total)
    group = lax.div(lax.broadcasted_iota(jnp.int32, (8, ROWS), 1), 32)
    whose = lax.broadcasted_iota(jnp.int32, (8, ROWS), 0)
    per = jnp.sum(jnp.where(group == whose, logprob, 0.0), axis=1, keepdims=True) * (1.0 / 32)
    diag = lax.broadcasted_iota(jnp.int32, (8, 128), 0) == lax.broadcasted_iota(jnp.int32, (8, 128), 1)
    row = jnp.sum(jnp.where(diag, per, 0.0), axis=0, keepdims=True)
    f2[8 * k + c] = jnp.broadcast_to(row, (8, 128))

    @pl.loop(1, CAND)
    def _(d):
        to = lax.rem(c + d, CAND)
        send(f2.at[8 * k + c], f2.at[8 * k + c], f_send.at[1], f_recv.at[1], t, to)
        send(f2.at[8 * k + c], f2.at[8 * k + c], f_send.at[1], f_recv.at[1], partner, to)

    send(f2.at[8 * k + c], f2.at[8 * k + c], f_send.at[1], f_recv.at[1], partner, c)
    landed(f2.at[pl.ds(0, 15)], f_recv.at[1])
    lane = lax.broadcasted_iota(jnp.int32, (8, 8, 128), 2)
    cand = lax.broadcasted_iota(jnp.int32, (8, 8, 128), 0) * 8 + lane
    for b in range(2):
        count = counts[b]
        inside = jnp.where((cand < count) & (lane < 8), f2[pl.ds(8 * b, 8)], NEG)
        best_out[b] = jnp.max(inside)
        own_lane = lax.broadcasted_iota(jnp.int32, (1, 128), 1)
        own = f2[8 * b + c][0:1, :]
        scores_out[pl.ds(b, 1), :] = jnp.where(own_lane + 8 * c < count, own, 0.0)[:, :8]

    for n in range(2):
        landed(kb.at[pl.ds(0, 496), :], kv_send.at[n])
    for n in range(7):
        at_ = places[n]
        for slot in range(9):
            landed(at_(c) if slot < 5 else at_(c, 0), g_send.at[n, slot])
        if n < 5:
            landed(whole[n](k), g_dsend.at[n])
    for p in range(2):
        for n in range(6):
            landed(sy.at[p, 0], rs_send.at[p, n])
            landed(sz.at[p, 0], rs_send.at[p, 6 + n])
        for n, ref in enumerate(
            [nf.at[p, :, my_rows, :]] * 2 + [nf.at[p, 0, my_rows, :]] * 2
            + [nf.at[p, :, y_rows(0), :]] * 2 + [nf.at[p, 0, y_rows(0), :]] * 2
        ):
            landed(ref, ag_send.at[p, n])
    landed(f1.at[pl.ds(0, 15)], f_send.at[0])
    landed(f2.at[pl.ds(0, 15)], f_send.at[1])


def body(
    dec_hidden, enc_keys, enc_values, enc_lengths, cand_counts, gold_ids, gain_cross, w_query,
    w_out, gain_ffn, w_in_gate, w_in_up, w_ffn_out, gain_final, w_vocab,
):
    units = w_in_gate.shape[1]
    width = w_vocab.shape[1]
    w_in = jnp.concatenate([w_in_gate, w_in_up], axis=1)
    anywhere = pl.BlockSpec(memory_space=pl.ANY)
    vmem = pl.BlockSpec(memory_space=pltpu.VMEM)
    smem = pl.BlockSpec(memory_space=pltpu.SMEM)
    dma = pltpu.SemaphoreType.DMA
    return pl.pallas_call(
        kernel,
        name="layer",
        out_shape=(
            jax.ShapeDtypeStruct((2, 8), F32),
            jax.ShapeDtypeStruct((2,), F32),
        ),
        in_specs=[
            anywhere, anywhere, anywhere, smem, smem, vmem, vmem, anywhere, anywhere, vmem,
            anywhere, anywhere, vmem, anywhere,
        ],
        out_specs=(vmem, smem),
        scratch_shapes=[
            pltpu.VMEM((8, 32, D), BF),
            pltpu.VMEM((ROWS, D), BF),
            pltpu.VMEM((2 * ROWS, 128), BF),
            pltpu.VMEM((4096, 128), BF),
            pltpu.VMEM((4096, 128), BF),
            pltpu.VMEM((8, 2 * ROWS, 512), F32),
            pltpu.VMEM((2 * ROWS, 4096), BF),
            pltpu.VMEM((ROWS, 128), BF),
            pltpu.VMEM((2, D, 64), BF),
            pltpu.VMEM((8, 128, 256), BF),
            pltpu.VMEM((2, D, 2 * units), BF),
            pltpu.VMEM((8, 2 * units, 256), BF),
            pltpu.VMEM((2, D, width), BF),
            pltpu.VMEM((2, 2, ROWS, HALF), BF),
            pltpu.VMEM((2, 2, 64, HALF), BF),
            pltpu.VMEM((2, 2, 64, HALF), BF),
            pltpu.VMEM((2, 2, 64, HALF), BF),
            pltpu.VMEM((2, 2, 64, HALF), BF),
            pltpu.VMEM((2, 2, 64, HALF), BF),
            pltpu.VMEM((2, 2, 16, HALF), BF),
            pltpu.VMEM((2, 2, 16, HALF), BF),
            pltpu.VMEM((2, 2, 16, HALF), BF),
            pltpu.VMEM((2, 2, 16, HALF), BF),
            pltpu.VMEM((16, D), F32),
            pltpu.VMEM((2, 2, ROWS, HALF), BF),
            pltpu.VMEM((2, ROWS, units), BF),
            pltpu.VMEM((2 * ROWS, 128), F32),
            pltpu.VMEM((16, 8, ROWS), F32),
            pltpu.VMEM((16, 8, 128), F32),
            dma((2,)), dma((2,)), dma((7, 9)), dma((7, 9)), dma((5,)), dma((5,)), dma((5,)),
            dma((2, 12)), dma((2, 12)), dma((2, 8)), dma((2, 8)), dma((2,)), dma((2,)), dma((3,)),
        ],
        compiler_params=pltpu.CompilerParams(
            collective_id=0, has_side_effects=True, vmem_limit_bytes=62 * 1024 * 1024
        ),
    )(
        dec_hidden, enc_keys, enc_values, enc_lengths, cand_counts, gold_ids,
        gain_cross.reshape(1, -1), w_query, w_out, gain_ffn.reshape(1, -1), w_in, w_ffn_out,
        gain_final.reshape(1, -1), w_vocab,
    )


def solution(mesh):
    in_specs = (
        P(None, "cand", None, None), P(None, "tok", None), P(None, "tok", None), P(), P(),
        P(None, "cand", None), P(), P("cand", "tok"), P("tok", "cand"), P(), P("cand", "tok"),
        P("cand", "tok"), P("tok", "cand"), P(), P("cand", "tok"),
    )
    return jax.shard_map(
        body, mesh=mesh, in_specs=in_specs, out_specs=(P(None, "cand"), P()), check_vma=False
    )
```

```python
import functools

import jax
import jax.numpy as jnp
from jax import lax
from jax.experimental import pallas as pl
from jax.experimental.pallas import tpu as pltpu
from jax.sharding import PartitionSpec as P

MESH = pl.DeviceIdType.MESH
EPS = 0.25
NY, NZ, NX = 4, 4, 4
TOK, CAND = 32, 8
D = 2048
HALF = 1024
ROWS = 256
NEG = -1e30
BF = jnp.bfloat16
F32 = jnp.float32


def rms(v, gain):
    squares = jnp.mean(v * v, axis=-1, keepdims=True)
    return v * lax.rsqrt(squares + EPS) * gain


def gelu(v):
    inner = 0.7978845608028654 * (v + 0.044715 * (v * v * v))
    return 0.5 * v * (1.0 + jnp.tanh(inner))


def dot_t(a, b):
    return lax.dot_general(a, b, (((1,), (1,)), ((), ())), preferred_element_type=F32)


def landed(ref, sem):
    pltpu.make_async_copy(ref, ref, sem).wait()


def kernel(
    x_in, keys, vals, lens, counts, gold, gain1, wq_in, wo_in, gain2, wg_in, wu_in, fo_in, gain3, wv_in,
    scores_out, best_out,
    xv, nx, q2, kb, vb, sc, pb, at,
    wq, wo, wi, fo, wv,
    part, ryf, ryd, rya, sy, by, rzf, rzd, rza, sz, ac, nf,
    hid, st, f1, f2,
    kv_recv, kv_send, g_recv, g_send, g_own, g_dual, g_dsend,
    rs_recv, rs_send, ag_recv, ag_send, f_recv, f_send, l_sem,
):
    t = lax.axis_index("tok")
    c = lax.axis_index("cand")
    k = lax.rem(t, 2)
    j = lax.div(t, 2)
    y = lax.div(j, NZ)
    z = lax.rem(j, NZ)
    xx = lax.div(c, 2)
    zl = lax.rem(c, 2)

    def tok_of(yy, zz):
        return (lax.rem(yy, NY) * NZ + lax.rem(zz, NZ)) * 2 + k

    def cand_of(x_at, z_at):
        return lax.rem(x_at, NX) * 2 + z_at

    partner = t + 1 - 2 * k
    cz = cand_of(xx, 1 - zl)
    cp, cm = cand_of(xx + 1, zl), cand_of(xx + 3, zl)
    cpz, cmz = cand_of(xx + 1, 1 - zl), cand_of(xx + 3, 1 - zl)
    co, coz = cand_of(xx + 2, zl), cand_of(xx + 2, 1 - zl)

    def send(src, dst, s_sem, r_sem, tok, cand):
        pltpu.make_async_remote_copy(
            src_ref=src, dst_ref=dst, send_sem=s_sem, recv_sem=r_sem,
            device_id=(tok, cand), device_id_type=MESH,
        ).start()

    x_copy = pltpu.make_async_copy(x_in.at[k], xv, l_sem.at[0])
    x_copy.start()

    barrier = pltpu.get_barrier_semaphore()

    @pl.loop(1, TOK)
    def _(d):
        pl.semaphore_signal(
            barrier, inc=1, device_id=(lax.rem(t + d, TOK), c), device_id_type=MESH
        )

    @pl.loop(1, CAND)
    def _(d):
        pl.semaphore_signal(
            barrier, inc=1, device_id=(t, lax.rem(c + d, CAND)), device_id_type=MESH
        )
        pl.semaphore_signal(
            barrier, inc=1, device_id=(partner, lax.rem(c + d, CAND)), device_id_type=MESH
        )

    def stacked(ref, size):
        def at_(cc, part=None):
            if part is None:
                return ref.at[cc, pl.ds(size * k, size), :]
            return ref.at[cc, pl.ds(size * k + size // 2 * part, size // 2), :]
        return at_

    def i_at(cc, part=None):
        if part is None:
            return wi.at[:, cc, pl.ds(160 * k, 160), :]
        return wi.at[:, cc, pl.ds(160 * k + 80 * part, 80), :]

    width = wv.shape[2]

    def v_at(cc, part=None):
        if part is None:
            return wv.at[k, cc]
        return wv.at[k, cc, pl.ds(0, 512), :] if part == 0 else wv.at[k, cc, pl.ds(512, width - 512), :]

    def kv_at(ref):
        def at_(cc, part=None):
            if part is None:
                return ref.at[pl.ds(512 * cc, 512), :]
            return ref.at[pl.ds(512 * cc + 256 * part, 256), :]
        return at_

    places = [stacked(wq, 64), stacked(wo, 64), i_at, stacked(fo, 160), v_at, kv_at(kb), kv_at(vb)]
    whole = [
        lambda h: wq.at[:, pl.ds(64 * h, 64), :], lambda h: wo.at[:, pl.ds(64 * h, 64), :],
        lambda h: wi.at[:, :, pl.ds(160 * h, 160), :], lambda h: fo.at[:, pl.ds(160 * h, 160), :],
        lambda h: wv.at[h],
    ]

    def own_copies():
        for n, src in ((0, wq_in), (1, wo_in), (3, fo_in), (4, wv_in)):
            pltpu.make_async_copy(src, places[n](c), g_own.at[n]).start()
        for m, src in enumerate((wg_in, wu_in)):
            pltpu.make_async_copy(
                src, wi.at[m, c, pl.ds(160 * k, 160), :], g_own.at[2]
            ).start()

    def g_send_to(n, slot, src, dst, cand):
        send(src, dst, g_send.at[n, slot], g_recv.at[n, slot], t, cand)

    def step1(n):
        at_ = places[n]
        src = at_(c)
        if n < 5:
            landed(src, g_own.at[n])
        g_send_to(n, 0, src, at_(c), cz)
        g_send_to(n, 1, src, at_(c), cp)
        g_send_to(n, 2, src, at_(c), cm)

    def step2(n):
        at_ = places[n]
        landed(at_(cz), g_recv.at[n, 0])
        g_send_to(n, 3, at_(cz), at_(cz), cp)
        g_send_to(n, 4, at_(cz), at_(cz), cm)
        landed(at_(cm), g_recv.at[n, 1])
        g_send_to(n, 5, at_(cm, 0), at_(cm, 0), cp)
        landed(at_(cp), g_recv.at[n, 2])
        g_send_to(n, 6, at_(cp, 1), at_(cp, 1), cm)

    def step3(n):
        at_ = places[n]
        landed(at_(cmz), g_recv.at[n, 3])
        g_send_to(n, 7, at_(cmz, 0), at_(cmz, 0), cp)
        landed(at_(cpz), g_recv.at[n, 4])
        g_send_to(n, 8, at_(cpz, 1), at_(cpz, 1), cm)

    def step4(n):
        at_ = places[n]
        landed(at_(co, 0), g_recv.at[n, 5])
        landed(at_(co, 1), g_recv.at[n, 6])
        landed(at_(coz, 0), g_recv.at[n, 7])
        landed(at_(coz, 1), g_recv.at[n, 8])
        if n < 5:
            send(whole[n](k), whole[n](k), g_dsend.at[n], g_dual.at[n], partner, c)

    def both(n):
        landed(whole[n](1 - k), g_dual.at[n])


    own_copies()

    x_copy.wait()

    @pl.loop(0, 8)
    def _(i):
        rows = xv[i].astype(F32)
        nx[pl.ds(pl.multiple_of(32 * i, 32), 32), :] = rms(rows, gain1[...]).astype(BF)

    pl.semaphore_wait(barrier, TOK - 1 + 2 * (CAND - 1))

    step1(0)

    for n, (src, dst) in enumerate(((keys, kb), (vals, vb))):
        here = dst.at[pl.ds(512 * c + 16 * t, 16), :]
        pltpu.make_async_copy(
            src.at[k, pl.ds(16 * c, 16), pl.ds(pl.multiple_of(128 * j, 128), 128)],
            here, l_sem.at[1 + n],
        ).start()

        @pl.loop(1, TOK)
        def _(d, src=src, n=n, here=here):
            to = lax.rem(t + d, TOK)
            send(
                src.at[
                    lax.rem(to, 2), pl.ds(16 * c, 16),
                    pl.ds(pl.multiple_of(128 * lax.div(to, 2), 128), 128),
                ],
                here, kv_send.at[n], kv_recv.at[n], to, c,
            )

    def kv_mine(n):
        ref = (kb, vb)[n]
        pltpu.make_async_copy(
            ref.at[pl.ds(0, 16), :], ref.at[pl.ds(512 * c + 16 * t, 16), :], l_sem.at[1 + n]
        ).wait()
        landed(ref.at[pl.ds(0, 496), :], kv_recv.at[n])

    step2(0)
    step1(3)
    step3(0)
    step1(1)
    step1(2)
    step4(0)
    kv_mine(0)
    step1(5)
    kv_mine(1)
    step1(6)
    both(0)
    zero = jnp.zeros((ROWS, 64), BF)
    query = jnp.zeros((ROWS, 128), F32)
    for cc in range(CAND):
        query = query + dot_t(nx[:, 256 * cc : 256 * cc + 256], wq[cc])
    query = query.astype(BF)
    q2[pl.ds(0, ROWS), :] = jnp.concatenate([query[:, :64], zero], axis=1)
    q2[pl.ds(ROWS, ROWS), :] = jnp.concatenate([zero, query[:, 64:]], axis=1)

    length = lens[k]

    def score(cc):
        place = lax.broadcasted_iota(jnp.int32, (1, 512), 1)
        token = lax.div(place, 16) * 128 + 16 * cc + lax.rem(place, 16)
        live = token < length
        block = kb[pl.ds(pl.multiple_of(512 * cc, 512), 512), :]

        @pl.loop(0, 4)
        def _(r):
            rows = pl.ds(pl.multiple_of(128 * r, 128), 128)
            s = dot_t(q2[rows, :], block)
            sc[cc, rows, :] = jnp.where(live, s, NEG)

    step2(5)
    step2(6)
    score(c)
    step3(5)
    score(cz)
    score(cm)
    step3(6)
    step2(1)
    step2(2)
    step2(3)
    score(cp)
    score(cmz)
    score(cpz)
    step4(5)
    score(co)
    score(coz)

    @pl.loop(0, 16)
    def _(r):
        rows = pl.ds(pl.multiple_of(32 * r, 32), 32)
        high = sc[0, rows, :]
        for cc in range(1, CAND):
            high = jnp.maximum(high, sc[cc, rows, :])
        top = jnp.max(high, axis=1, keepdims=True)
        total = jnp.zeros((32, 512), F32)
        for cc in range(CAND):
            w = jnp.exp(sc[cc, rows, :] - top)
            total = total + w
            pb[rows, pl.ds(512 * cc, 512)] = w.astype(BF)
        st[rows, :] = jnp.broadcast_to(jnp.sum(total, axis=1, keepdims=True), (32, 128))

    step3(1)
    step4(6)

    @pl.loop(0, 4)
    def _(r):
        low = pl.ds(pl.multiple_of(64 * r, 64), 64)
        upp = pl.ds(pl.multiple_of(64 * r + ROWS, 64), 64)
        a = jnp.dot(pb[low, :], vb[...], preferred_element_type=F32) / st[low, :]
        b = jnp.dot(pb[upp, :], vb[...], preferred_element_type=F32) / st[upp, :]
        lane = lax.broadcasted_iota(jnp.int32, (64, 128), 1)
        at[low, :] = jnp.where(lane < 64, a, b).astype(BF)

    step4(1)
    both(1)
    for cc in range(CAND):
        part[0, cc // 4, :, pl.ds(256 * (cc % 4), 256)] = jnp.dot(
            at[...], wo[cc], preferred_element_type=F32
        ).astype(BF)

    ty, tm = tok_of(y + 1, z), tok_of(y + 3, z)
    tz, tn = tok_of(y, z + 1), tok_of(y, z + 3)

    def y_rows(dy):
        return pl.ds(pl.multiple_of(64 * lax.rem(y + dy, NY), 64), 64)

    def z_rows(dz):
        return pl.ds(pl.multiple_of(16 * lax.rem(z + dz, NZ), 16), 16)

    my_rows = pl.ds(pl.multiple_of(64 * y + 16 * z, 16), 16)

    def reduce_sums(p, meanwhile):
        def go(n, src, dst, tok):
            send(src, dst, rs_send.at[p, n], rs_recv.at[p, n], tok, c)

        go(0, part.at[p, 0, y_rows(2)], ryf.at[p, 0], ty)
        go(1, part.at[p, 1, y_rows(2)], ryf.at[p, 1], tm)
        go(2, part.at[p, 1, y_rows(1)], ryd.at[p, 1], ty)
        go(3, part.at[p, 0, y_rows(3)], ryd.at[p, 0], tm)
        meanwhile()
        landed(ryf.at[p, 0], rs_recv.at[p, 0])
        sy[p, 0] = (ryf[p, 0].astype(F32) + part[p, 0, y_rows(1)].astype(F32)).astype(BF)
        go(4, sy.at[p, 0], rya.at[p, 0], ty)
        landed(ryf.at[p, 1], rs_recv.at[p, 1])
        sy[p, 1] = (ryf[p, 1].astype(F32) + part[p, 1, y_rows(3)].astype(F32)).astype(BF)
        go(5, sy.at[p, 1], rya.at[p, 1], tm)
        landed(ryd.at[p, 1], rs_recv.at[p, 2])
        landed(ryd.at[p, 0], rs_recv.at[p, 3])
        for h in range(2):
            landed(rya.at[p, h], rs_recv.at[p, 4 + h])
            by[p, h] = (
                rya[p, h].astype(F32) + ryd[p, h].astype(F32)
                + part[p, h, y_rows(0)].astype(F32)
            ).astype(BF)
        go(6, by.at[p, 0, z_rows(2)], rzf.at[p, 0], tz)
        go(7, by.at[p, 1, z_rows(2)], rzf.at[p, 1], tn)
        go(8, by.at[p, 1, z_rows(1)], rzd.at[p, 1], tz)
        go(9, by.at[p, 0, z_rows(3)], rzd.at[p, 0], tn)
        landed(rzf.at[p, 0], rs_recv.at[p, 6])
        sz[p, 0] = (rzf[p, 0].astype(F32) + by[p, 0, z_rows(1)].astype(F32)).astype(BF)
        go(10, sz.at[p, 0], rza.at[p, 0], tz)
        landed(rzf.at[p, 1], rs_recv.at[p, 7])
        sz[p, 1] = (rzf[p, 1].astype(F32) + by[p, 1, z_rows(3)].astype(F32)).astype(BF)
        go(11, sz.at[p, 1], rza.at[p, 1], tn)
        landed(rzd.at[p, 1], rs_recv.at[p, 8])
        landed(rzd.at[p, 0], rs_recv.at[p, 9])
        sums = []
        for h in range(2):
            landed(rza.at[p, h], rs_recv.at[p, 10 + h])
            sums.append(
                rza[p, h].astype(F32) + rzd[p, h].astype(F32)
                + by[p, h, z_rows(0)].astype(F32)
            )
        return jnp.concatenate(sums, axis=1)

    def spread(p, value):
        nf[p, 0, my_rows, :] = value[:, :HALF]
        nf[p, 1, my_rows, :] = value[:, HALF:]

        def go(n, where, tok):
            send(where, where, ag_send.at[p, n], ag_recv.at[p, n], tok, c)

        def z_block(dz):
            return pl.ds(pl.multiple_of(64 * y + 16 * lax.rem(z + dz, NZ), 16), 16)

        go(0, nf.at[p, :, my_rows, :], tz)
        go(1, nf.at[p, :, my_rows, :], tn)
        landed(nf.at[p, :, z_block(3), :], ag_recv.at[p, 0])
        go(2, nf.at[p, 0, z_block(3), :], tz)
        landed(nf.at[p, :, z_block(1), :], ag_recv.at[p, 1])
        go(3, nf.at[p, 1, z_block(1), :], tn)
        landed(nf.at[p, 0, z_block(2), :], ag_recv.at[p, 2])
        landed(nf.at[p, 1, z_block(2), :], ag_recv.at[p, 3])
        go(4, nf.at[p, :, y_rows(0), :], ty)
        go(5, nf.at[p, :, y_rows(0), :], tm)
        landed(nf.at[p, :, y_rows(3), :], ag_recv.at[p, 4])
        go(6, nf.at[p, 0, y_rows(3), :], ty)
        landed(nf.at[p, :, y_rows(1), :], ag_recv.at[p, 5])
        go(7, nf.at[p, 1, y_rows(1), :], tm)
        landed(nf.at[p, 0, y_rows(2), :], ag_recv.at[p, 6])
        landed(nf.at[p, 1, y_rows(2), :], ag_recv.at[p, 7])

    def later():
        step3(2)
        step3(3)
        step1(4)

    mine = xv[2 * y + lax.div(z, 2), pl.ds(pl.multiple_of(16 * lax.rem(z, 2), 16), 16), :]
    ac[...] = mine.astype(F32) + reduce_sums(0, later)
    step4(2)
    step4(3)
    spread(0, rms(ac[...], gain2[...]).astype(BF))
    step2(4)
    both(2)
    both(3)

    @pl.loop(0, 4)
    def _(r):
        rows = pl.ds(pl.multiple_of(64 * r, 64), 64)
        gate = up = jnp.zeros((64, 320), F32)
        for cc in range(CAND):
            block = nf[0, cc // 4, rows, pl.ds(256 * (cc % 4), 256)]
            gate = gate + dot_t(block, wi[0, cc])
            up = up + dot_t(block, wi[1, cc])
        hid[rows, :] = (gelu(gate) * up).astype(BF)
        for cc in range(CAND):
            part[1, cc // 4, rows, pl.ds(256 * (cc % 4), 256)] = jnp.dot(
                hid[rows, :], fo[cc], preferred_element_type=F32
            ).astype(BF)

    after = ac[...] + reduce_sums(1, lambda: step3(4))
    step4(4)
    spread(1, rms(after, gain3[...]).astype(BF))
    both(4)

    ids = gold[k].astype(F32)
    eye = lax.broadcasted_iota(jnp.int32, (32, 32), 0) == lax.broadcasted_iota(jnp.int32, (32, 32), 1)
    start = [((2 * j + h) * width).astype(F32) for h in range(2)]

    for i in range(8):
        column = jnp.sum(
            jnp.where(eye, jnp.broadcast_to(ids[i : i + 1, :], (32, 32)), 0.0), axis=1, keepdims=True
        )
        st[pl.ds(32 * i, 32), :] = jnp.broadcast_to(column, (32, 128))

    @pl.loop(0, 4)
    def _(r):
        rows = pl.ds(pl.multiple_of(64 * r, 64), 64)
        wanted = st[rows, :][:, :1]
        logits = []
        for h in range(2):
            one = jnp.zeros((64, width), F32)
            for cc in range(CAND):
                one = one + dot_t(nf[1, cc // 4, rows, pl.ds(256 * (cc % 4), 256)], wv[h, cc])
            logits.append(one)
        high = jnp.maximum(
            jnp.max(logits[0], axis=1, keepdims=True), jnp.max(logits[1], axis=1, keepdims=True)
        )
        total = jnp.zeros((64, 1), F32)
        picked = jnp.zeros((64, 1), F32)
        for h in range(2):
            total = total + jnp.sum(jnp.exp(logits[h] - high), axis=1, keepdims=True)
            at_col = lax.broadcasted_iota(jnp.int32, (64, width), 1).astype(F32) + start[h]
            picked = picked + jnp.sum(
                jnp.where(at_col == wanted, logits[h], 0.0), axis=1, keepdims=True
            )
        lane = lax.broadcasted_iota(jnp.int32, (64, 128), 1)
        st[pl.ds(pl.multiple_of(256 + 64 * r, 64), 64), :] = jnp.where(
            lane == 0, high, jnp.where(lane == 1, total, picked)
        )

    stats = st[pl.ds(256, 256), :].T
    f1[j] = stats[0:8, :]

    @pl.loop(1, 16)
    def _(d):
        to = lax.rem(j + d, 16) * 2 + k
        send(f1.at[j], f1.at[j], f_send.at[0], f_recv.at[0], to, c)

    landed(f1.at[pl.ds(0, 15)], f_recv.at[0])
    top = f1[0][0:1, :]
    for n in range(1, 16):
        top = jnp.maximum(top, f1[n][0:1, :])
    total = jnp.zeros((1, ROWS), F32)
    picked = jnp.zeros((1, ROWS), F32)
    for n in range(16):
        total = total + f1[n][1:2, :] * jnp.exp(f1[n][0:1, :] - top)
        picked = picked + f1[n][2:3, :]
    logprob = picked - top - jnp.log(total)
    group = lax.div(lax.broadcasted_iota(jnp.int32, (8, ROWS), 1), 32)
    whose = lax.broadcasted_iota(jnp.int32, (8, ROWS), 0)
    per = jnp.sum(jnp.where(group == whose, logprob, 0.0), axis=1, keepdims=True) * (1.0 / 32)
    diag = lax.broadcasted_iota(jnp.int32, (8, 128), 0) == lax.broadcasted_iota(jnp.int32, (8, 128), 1)
    row = jnp.sum(jnp.where(diag, per, 0.0), axis=0, keepdims=True)
    f2[8 * k + c] = jnp.broadcast_to(row, (8, 128))

    @pl.loop(1, CAND)
    def _(d):
        to = lax.rem(c + d, CAND)
        send(f2.at[8 * k + c], f2.at[8 * k + c], f_send.at[1], f_recv.at[1], t, to)
        send(f2.at[8 * k + c], f2.at[8 * k + c], f_send.at[1], f_recv.at[1], partner, to)

    send(f2.at[8 * k + c], f2.at[8 * k + c], f_send.at[1], f_recv.at[1], partner, c)
    landed(f2.at[pl.ds(0, 15)], f_recv.at[1])
    lane = lax.broadcasted_iota(jnp.int32, (8, 8, 128), 2)
    cand = lax.broadcasted_iota(jnp.int32, (8, 8, 128), 0) * 8 + lane
    for b in range(2):
        count = counts[b]
        inside = jnp.where((cand < count) & (lane < 8), f2[pl.ds(8 * b, 8)], NEG)
        best_out[b] = jnp.max(inside)
        own_lane = lax.broadcasted_iota(jnp.int32, (1, 128), 1)
        own = f2[8 * b + c][0:1, :]
        scores_out[pl.ds(b, 1), :] = jnp.where(own_lane + 8 * c < count, own, 0.0)[:, :8]

    for n in range(2):
        landed(kb.at[pl.ds(0, 496), :], kv_send.at[n])
    for n in range(7):
        at_ = places[n]
        for slot in range(9):
            landed(at_(c) if slot < 5 else at_(c, (slot - 5) % 2), g_send.at[n, slot])
        if n < 5:
            landed(whole[n](k), g_dsend.at[n])
    for p in range(2):
        for n in range(6):
            landed(sy.at[p, 0], rs_send.at[p, n])
            landed(sz.at[p, 0], rs_send.at[p, 6 + n])
        for n, ref in enumerate(
            [nf.at[p, :, my_rows, :]] * 2 + [nf.at[p, 0, my_rows, :]] * 2
            + [nf.at[p, :, y_rows(0), :]] * 2 + [nf.at[p, 0, y_rows(0), :]] * 2
        ):
            landed(ref, ag_send.at[p, n])
    landed(f1.at[pl.ds(0, 15)], f_send.at[0])
    landed(f2.at[pl.ds(0, 15)], f_send.at[1])


def body(
    dec_hidden, enc_keys, enc_values, enc_lengths, cand_counts, gold_ids, gain_cross, w_query,
    w_out, gain_ffn, w_in_gate, w_in_up, w_ffn_out, gain_final, w_vocab,
):
    units = w_in_gate.shape[1]
    width = w_vocab.shape[1]
    anywhere = pl.BlockSpec(memory_space=pl.ANY)
    vmem = pl.BlockSpec(memory_space=pltpu.VMEM)
    smem = pl.BlockSpec(memory_space=pltpu.SMEM)
    dma = pltpu.SemaphoreType.DMA
    return pl.pallas_call(
        kernel,
        name="layer",
        out_shape=(
            jax.ShapeDtypeStruct((2, 8), F32),
            jax.ShapeDtypeStruct((2,), F32),
        ),
        in_specs=[
            anywhere, anywhere, anywhere, smem, smem, vmem, vmem, anywhere, anywhere, vmem,
            anywhere, anywhere, anywhere, vmem, anywhere,
        ],
        out_specs=(vmem, smem),
        scratch_shapes=[
            pltpu.VMEM((8, 32, D), BF),
            pltpu.VMEM((ROWS, D), BF),
            pltpu.VMEM((2 * ROWS, 128), BF),
            pltpu.VMEM((4096, 128), BF),
            pltpu.VMEM((4096, 128), BF),
            pltpu.VMEM((8, 2 * ROWS, 512), F32),
            pltpu.VMEM((2 * ROWS, 4096), BF),
            pltpu.VMEM((ROWS, 128), BF),
            pltpu.VMEM((8, 128, 256), BF),
            pltpu.VMEM((8, 128, 256), BF),
            pltpu.VMEM((2, 8, 2 * units, 256), BF),
            pltpu.VMEM((8, 2 * units, 256), BF),
            pltpu.VMEM((2, 8, width, 256), BF),
            pltpu.VMEM((2, 2, ROWS, HALF), BF),
            pltpu.VMEM((2, 2, 64, HALF), BF),
            pltpu.VMEM((2, 2, 64, HALF), BF),
            pltpu.VMEM((2, 2, 64, HALF), BF),
            pltpu.VMEM((2, 2, 64, HALF), BF),
            pltpu.VMEM((2, 2, 64, HALF), BF),
            pltpu.VMEM((2, 2, 16, HALF), BF),
            pltpu.VMEM((2, 2, 16, HALF), BF),
            pltpu.VMEM((2, 2, 16, HALF), BF),
            pltpu.VMEM((2, 2, 16, HALF), BF),
            pltpu.VMEM((16, D), F32),
            pltpu.VMEM((2, 2, ROWS, HALF), BF),
            pltpu.VMEM((ROWS, 2 * units), BF),
            pltpu.VMEM((2 * ROWS, 128), F32),
            pltpu.VMEM((16, 8, ROWS), F32),
            pltpu.VMEM((16, 8, 128), F32),
            dma((2,)), dma((2,)), dma((7, 9)), dma((7, 9)), dma((5,)), dma((5,)), dma((5,)),
            dma((2, 12)), dma((2, 12)), dma((2, 8)), dma((2, 8)), dma((2,)), dma((2,)), dma((3,)),
        ],
        compiler_params=pltpu.CompilerParams(
            collective_id=0, has_side_effects=True, vmem_limit_bytes=62 * 1024 * 1024
        ),
    )(
        dec_hidden, enc_keys, enc_values, enc_lengths, cand_counts, gold_ids,
        gain_cross.reshape(1, -1), w_query.T, w_out, gain_ffn.reshape(1, -1), w_in_gate.T, w_in_up.T,
        w_ffn_out,
        gain_final.reshape(1, -1), w_vocab.T,
    )


def solution(mesh):
    in_specs = (
        P(None, "cand", None, None), P(None, "tok", None), P(None, "tok", None), P(), P(),
        P(None, "cand", None), P(), P("cand", "tok"), P("tok", "cand"), P(), P("cand", "tok"),
        P("cand", "tok"), P("tok", "cand"), P(), P("cand", "tok"),
    )
    return jax.shard_map(
        body, mesh=mesh, in_specs=in_specs, out_specs=(P(None, "cand"), P()), check_vma=False
    )
```

```python
import functools

import jax
import jax.numpy as jnp
from jax import lax
from jax.experimental import pallas as pl
from jax.experimental.pallas import tpu as pltpu
from jax.sharding import PartitionSpec as P

MESH = pl.DeviceIdType.MESH
EPS = 0.25
NY, NZ, NX = 4, 4, 4
TOK, CAND = 32, 8
D = 2048
HALF = 1024
ROWS = 256
NEG = -1e30
BF = jnp.bfloat16
F32 = jnp.float32


def rms(v, gain):
    squares = jnp.mean(v * v, axis=-1, keepdims=True)
    return v * lax.rsqrt(squares + EPS) * gain


def gelu(v):
    inner = 0.7978845608028654 * (v + 0.044715 * (v * v * v))
    return 0.5 * v * (1.0 + jnp.tanh(inner))


def dot_t(a, b):
    return lax.dot_general(a, b, (((1,), (1,)), ((), ())), preferred_element_type=F32)


def landed(ref, sem):
    pltpu.make_async_copy(ref, ref, sem).wait()


def kernel(
    x_in, keys, vals, lens, counts, gold, gain1, wq_in, wo_in, gain2, wg_in, wu_in, fo_in, gain3, wv_in,
    scores_out, best_out,
    xv, nx, q2, kb, vb, sc, pb, at,
    wq, wo, wi, fo, wv,
    part, ryf, ryd, rya, sy, by, rzf, rzd, rza, sz, ac, nf,
    hid, st, f1, f2,
    kv_recv, kv_send, g_recv, g_send, g_own, g_dual, g_dsend,
    rs_recv, rs_send, ag_recv, ag_send, f_recv, f_send, l_sem,
):
    t = lax.axis_index("tok")
    c = lax.axis_index("cand")
    k = lax.rem(t, 2)
    j = lax.div(t, 2)
    y = lax.div(j, NZ)
    z = lax.rem(j, NZ)
    xx = lax.div(c, 2)
    zl = lax.rem(c, 2)

    def tok_of(yy, zz):
        return (lax.rem(yy, NY) * NZ + lax.rem(zz, NZ)) * 2 + k

    def cand_of(x_at, z_at):
        return lax.rem(x_at, NX) * 2 + z_at

    partner = t + 1 - 2 * k
    cz = cand_of(xx, 1 - zl)
    cp, cm = cand_of(xx + 1, zl), cand_of(xx + 3, zl)
    cpz, cmz = cand_of(xx + 1, 1 - zl), cand_of(xx + 3, 1 - zl)
    co, coz = cand_of(xx + 2, zl), cand_of(xx + 2, 1 - zl)

    def send(src, dst, s_sem, r_sem, tok, cand):
        pltpu.make_async_remote_copy(
            src_ref=src, dst_ref=dst, send_sem=s_sem, recv_sem=r_sem,
            device_id=(tok, cand), device_id_type=MESH,
        ).start()

    x_copy = pltpu.make_async_copy(x_in.at[k], xv, l_sem.at[0])
    x_copy.start()

    barrier = pltpu.get_barrier_semaphore()

    @pl.loop(1, TOK)
    def _(d):
        pl.semaphore_signal(
            barrier, inc=1, device_id=(lax.rem(t + d, TOK), c), device_id_type=MESH
        )

    @pl.loop(1, CAND)
    def _(d):
        pl.semaphore_signal(
            barrier, inc=1, device_id=(t, lax.rem(c + d, CAND)), device_id_type=MESH
        )
        pl.semaphore_signal(
            barrier, inc=1, device_id=(partner, lax.rem(c + d, CAND)), device_id_type=MESH
        )

    def stacked(ref, size):
        def at_(cc, part=None):
            if part is None:
                return ref.at[cc, pl.ds(size * k, size), :]
            return ref.at[cc, pl.ds(size * k + size // 2 * part, size // 2), :]
        return at_

    def i_at(cc, part=None):
        if part is None:
            return wi.at[:, cc, pl.ds(160 * k, 160), :]
        return wi.at[:, cc, pl.ds(160 * k + 80 * part, 80), :]

    width = wv.shape[2]

    def v_at(cc, part=None):
        if part is None:
            return wv.at[k, cc]
        return wv.at[k, cc, pl.ds(0, 512), :] if part == 0 else wv.at[k, cc, pl.ds(512, width - 512), :]

    def kv_at(ref):
        def at_(cc, part=None):
            if part is None:
                return ref.at[pl.ds(512 * cc, 512), :]
            return ref.at[pl.ds(512 * cc + 256 * part, 256), :]
        return at_

    places = [stacked(wq, 64), stacked(wo, 64), i_at, stacked(fo, 160), v_at, kv_at(kb), kv_at(vb)]
    whole = [
        lambda h: wq.at[:, pl.ds(64 * h, 64), :], lambda h: wo.at[:, pl.ds(64 * h, 64), :],
        lambda h: wi.at[:, :, pl.ds(160 * h, 160), :], lambda h: fo.at[:, pl.ds(160 * h, 160), :],
        lambda h: wv.at[h],
    ]

    def own_copies():
        for n, src in ((0, wq_in), (1, wo_in), (3, fo_in), (4, wv_in)):
            pltpu.make_async_copy(src, places[n](c), g_own.at[n]).start()
        for m, src in enumerate((wg_in, wu_in)):
            pltpu.make_async_copy(
                src, wi.at[m, c, pl.ds(160 * k, 160), :], g_own.at[2]
            ).start()

    def g_send_to(n, slot, src, dst, cand):
        send(src, dst, g_send.at[n, slot], g_recv.at[n, slot], t, cand)

    def step1z(n):
        here = places[n](c)
        if n < 5:
            landed(here, g_own.at[n])
        g_send_to(n, 0, here, here, cz)

    def step1x(n):
        here = places[n](c)
        g_send_to(n, 1, here, here, cp)
        g_send_to(n, 2, here, here, cm)

    def step1(n):
        step1z(n)
        step1x(n)

    def step2a(n):
        at_ = places[n]
        landed(at_(cz), g_recv.at[n, 0])
        g_send_to(n, 3, at_(cz), at_(cz), cp)
        g_send_to(n, 4, at_(cz), at_(cz), cm)

    def step2b(n):
        at_ = places[n]
        landed(at_(cm), g_recv.at[n, 1])
        g_send_to(n, 5, at_(cm, 0), at_(cm, 0), cp)
        landed(at_(cp), g_recv.at[n, 2])
        g_send_to(n, 6, at_(cp, 1), at_(cp, 1), cm)

    def step2(n):
        step2a(n)
        step2b(n)

    def step3(n):
        at_ = places[n]
        landed(at_(cmz), g_recv.at[n, 3])
        g_send_to(n, 7, at_(cmz, 0), at_(cmz, 0), cp)
        landed(at_(cpz), g_recv.at[n, 4])
        g_send_to(n, 8, at_(cpz, 1), at_(cpz, 1), cm)

    def step4(n):
        at_ = places[n]
        landed(at_(co, 0), g_recv.at[n, 5])
        landed(at_(co, 1), g_recv.at[n, 6])
        landed(at_(coz, 0), g_recv.at[n, 7])
        landed(at_(coz, 1), g_recv.at[n, 8])
        if n < 5:
            send(whole[n](k), whole[n](k), g_dsend.at[n], g_dual.at[n], partner, c)

    def both(n):
        landed(whole[n](1 - k), g_dual.at[n])


    own_copies()

    x_copy.wait()

    @pl.loop(0, 8)
    def _(i):
        rows = xv[i].astype(F32)
        nx[pl.ds(pl.multiple_of(32 * i, 32), 32), :] = rms(rows, gain1[...]).astype(BF)

    pl.semaphore_wait(barrier, TOK - 1 + 2 * (CAND - 1))

    step1(0)

    for n, (src, dst) in enumerate(((keys, kb), (vals, vb))):
        here = dst.at[pl.ds(512 * c + 16 * t, 16), :]
        pltpu.make_async_copy(
            src.at[k, pl.ds(16 * c, 16), pl.ds(pl.multiple_of(128 * j, 128), 128)],
            here, l_sem.at[1 + n],
        ).start()

        @pl.loop(1, TOK)
        def _(d, src=src, n=n, here=here):
            to = lax.rem(t + d, TOK)
            send(
                src.at[
                    lax.rem(to, 2), pl.ds(16 * c, 16),
                    pl.ds(pl.multiple_of(128 * lax.div(to, 2), 128), 128),
                ],
                here, kv_send.at[n], kv_recv.at[n], to, c,
            )

    def kv_mine(n):
        ref = (kb, vb)[n]
        pltpu.make_async_copy(
            ref.at[pl.ds(0, 16), :], ref.at[pl.ds(512 * c + 16 * t, 16), :], l_sem.at[1 + n]
        ).wait()
        landed(ref.at[pl.ds(0, 496), :], kv_recv.at[n])

    step2(0)
    step1(3)
    step3(0)
    step1(1)
    step1(2)
    step4(0)
    kv_mine(0)
    step1(5)
    kv_mine(1)
    step1(6)
    step1z(4)
    both(0)
    zero = jnp.zeros((ROWS, 64), BF)
    query = jnp.zeros((ROWS, 128), F32)
    for cc in range(CAND):
        query = query + dot_t(nx[:, 256 * cc : 256 * cc + 256], wq[cc])
    query = query.astype(BF)
    q2[pl.ds(0, ROWS), :] = jnp.concatenate([query[:, :64], zero], axis=1)
    q2[pl.ds(ROWS, ROWS), :] = jnp.concatenate([zero, query[:, 64:]], axis=1)

    length = lens[k]

    def score(cc):
        place = lax.broadcasted_iota(jnp.int32, (1, 512), 1)
        token = lax.div(place, 16) * 128 + 16 * cc + lax.rem(place, 16)
        live = token < length
        block = kb[pl.ds(pl.multiple_of(512 * cc, 512), 512), :]

        @pl.loop(0, 4)
        def _(r):
            rows = pl.ds(pl.multiple_of(128 * r, 128), 128)
            s = dot_t(q2[rows, :], block)
            sc[cc, rows, :] = jnp.where(live, s, NEG)

    step2(5)
    step2(6)
    score(c)
    step3(5)
    score(cz)
    score(cm)
    step3(6)
    step2(1)
    step2(2)
    step2(3)
    score(cp)
    score(cmz)
    score(cpz)
    step4(5)
    score(co)
    score(coz)

    @pl.loop(0, 16)
    def _(r):
        rows = pl.ds(pl.multiple_of(32 * r, 32), 32)
        high = sc[0, rows, :]
        for cc in range(1, CAND):
            high = jnp.maximum(high, sc[cc, rows, :])
        top = jnp.max(high, axis=1, keepdims=True)
        total = jnp.zeros((32, 512), F32)
        for cc in range(CAND):
            w = jnp.exp(sc[cc, rows, :] - top)
            total = total + w
            pb[rows, pl.ds(512 * cc, 512)] = w.astype(BF)
        st[rows, :] = jnp.broadcast_to(jnp.sum(total, axis=1, keepdims=True), (32, 128))

    step3(1)
    step4(6)

    @pl.loop(0, 4)
    def _(r):
        low = pl.ds(pl.multiple_of(64 * r, 64), 64)
        upp = pl.ds(pl.multiple_of(64 * r + ROWS, 64), 64)
        a = jnp.dot(pb[low, :], vb[...], preferred_element_type=F32) / st[low, :]
        b = jnp.dot(pb[upp, :], vb[...], preferred_element_type=F32) / st[upp, :]
        lane = lax.broadcasted_iota(jnp.int32, (64, 128), 1)
        at[low, :] = jnp.where(lane < 64, a, b).astype(BF)

    step4(1)
    both(1)
    for cc in range(CAND):
        part[0, cc // 4, :, pl.ds(256 * (cc % 4), 256)] = jnp.dot(
            at[...], wo[cc], preferred_element_type=F32
        ).astype(BF)

    ty, tm = tok_of(y + 1, z), tok_of(y + 3, z)
    tz, tn = tok_of(y, z + 1), tok_of(y, z + 3)

    def y_rows(dy):
        return pl.ds(pl.multiple_of(64 * lax.rem(y + dy, NY), 64), 64)

    def z_rows(dz):
        return pl.ds(pl.multiple_of(16 * lax.rem(z + dz, NZ), 16), 16)

    def yz_rows(dy, dz):
        at_row = 64 * lax.rem(y + dy, NY) + 16 * lax.rem(z + dz, NZ)
        return pl.ds(pl.multiple_of(at_row, 16), 16)

    order = (2, 1, 3, 0)

    def rs_go(p, n, src, dst, tok):
        send(src, dst, rs_send.at[p, n], rs_recv.at[p, n], tok, c)

    def sums_far(p):
        for dz in order:
            rs_go(p, dz, part.at[p, 0, yz_rows(2, dz)], ryf.at[p, 0, z_rows(dz)], ty)
            rs_go(p, 4 + dz, part.at[p, 1, yz_rows(2, dz)], ryf.at[p, 1, z_rows(dz)], tm)

    def sums_up(p):
        for dz in order:
            rs_go(p, 8 + dz, part.at[p, 1, yz_rows(1, dz)], ryd.at[p, 1, z_rows(dz)], ty)

    def sums_down(p):
        for dz in order:
            rs_go(p, 12 + dz, part.at[p, 0, yz_rows(3, dz)], ryd.at[p, 0, z_rows(dz)], tm)

    def add(out, *terms):
        total = terms[0].astype(F32)
        for term in terms[1:]:
            total = total + term.astype(F32)
        out[...] = total.astype(BF)

    def sums_end(p):
        for dz in order:
            zr = z_rows(dz)
            landed(ryf.at[p, 0, zr], rs_recv.at[p, dz])
            add(sy.at[p, 0, zr], ryf[p, 0, zr], part[p, 0, yz_rows(1, dz)])
            rs_go(p, 16 + dz, sy.at[p, 0, zr], rya.at[p, 0, zr], ty)
            landed(ryf.at[p, 1, zr], rs_recv.at[p, 4 + dz])
            add(sy.at[p, 1, zr], ryf[p, 1, zr], part[p, 1, yz_rows(3, dz)])
            rs_go(p, 20 + dz, sy.at[p, 1, zr], rya.at[p, 1, zr], tm)
        for dz in order:
            zr = z_rows(dz)
            landed(ryd.at[p, 0, zr], rs_recv.at[p, 12 + dz])
            landed(ryd.at[p, 1, zr], rs_recv.at[p, 8 + dz])
            for h in range(2):
                landed(rya.at[p, h, zr], rs_recv.at[p, 16 + 4 * h + dz])
                add(by.at[p, h, zr], rya[p, h, zr], ryd[p, h, zr], part[p, h, yz_rows(0, dz)])
            if dz == 2:
                rs_go(p, 24, by.at[p, 0, zr], rzf.at[p, 0], tz)
                rs_go(p, 25, by.at[p, 1, zr], rzf.at[p, 1], tn)
            elif dz == 1:
                rs_go(p, 26, by.at[p, 1, zr], rzd.at[p, 1], tz)
            elif dz == 3:
                rs_go(p, 27, by.at[p, 0, zr], rzd.at[p, 0], tn)
        landed(rzf.at[p, 0], rs_recv.at[p, 24])
        add(sz.at[p, 0], rzf[p, 0], by[p, 0, z_rows(1)])
        rs_go(p, 28, sz.at[p, 0], rza.at[p, 0], tz)
        landed(rzf.at[p, 1], rs_recv.at[p, 25])
        add(sz.at[p, 1], rzf[p, 1], by[p, 1, z_rows(3)])
        rs_go(p, 29, sz.at[p, 1], rza.at[p, 1], tn)
        landed(rzd.at[p, 1], rs_recv.at[p, 26])
        landed(rzd.at[p, 0], rs_recv.at[p, 27])
        sums = []
        for h in range(2):
            landed(rza.at[p, h], rs_recv.at[p, 28 + h])
            sums.append(
                rza[p, h].astype(F32) + rzd[p, h].astype(F32) + by[p, h, z_rows(0)].astype(F32)
            )
        return jnp.concatenate(sums, axis=1)

    def ag_go(p, n, h, rows, tok):
        where = nf.at[p, h, rows, :]
        send(where, where, ag_send.at[p, n], ag_recv.at[p, n], tok, c)

    def ag_wait(p, n, h, rows):
        landed(nf.at[p, h, rows, :], ag_recv.at[p, n])

    def spread(p, value, work, early, late):
        nf[p, 0, yz_rows(0, 0), :] = value[:, :HALF]
        nf[p, 1, yz_rows(0, 0), :] = value[:, HALF:]

        def along_y(dz):
            rows = yz_rows(0, dz)
            ag_go(p, dz, 0, rows, ty)
            ag_go(p, 4 + dz, 1, rows, tm)
            ag_go(p, 8 + dz, 1, rows, ty)
            ag_go(p, 12 + dz, 0, rows, tm)

        def onward(dz):
            ag_wait(p, dz, 0, yz_rows(3, dz))
            ag_go(p, 16 + dz, 0, yz_rows(3, dz), ty)
            ag_wait(p, 4 + dz, 1, yz_rows(1, dz))
            ag_go(p, 20 + dz, 1, yz_rows(1, dz), tm)

        own = yz_rows(0, 0)
        ag_go(p, 24, 0, own, tz)
        ag_go(p, 25, 1, own, tn)
        ag_go(p, 26, 1, own, tz)
        ag_go(p, 27, 0, own, tn)
        along_y(0)
        early()
        ag_wait(p, 24, 0, yz_rows(0, 3))
        ag_go(p, 28, 0, yz_rows(0, 3), tz)
        ag_wait(p, 25, 1, yz_rows(0, 1))
        ag_go(p, 29, 1, yz_rows(0, 1), tn)
        ag_wait(p, 26, 1, yz_rows(0, 3))
        along_y(3)
        ag_wait(p, 27, 0, yz_rows(0, 1))
        along_y(1)
        onward(0)
        ag_wait(p, 28, 0, yz_rows(0, 2))
        ag_wait(p, 29, 1, yz_rows(0, 2))
        along_y(2)
        late()
        work(0)
        for dz in (3, 1, 2):
            onward(dz)
        for dz in range(4):
            ag_wait(p, 8 + dz, 1, yz_rows(3, dz))
        work(3)
        for dz in range(4):
            ag_wait(p, 12 + dz, 0, yz_rows(1, dz))
        work(1)
        for dz in range(4):
            ag_wait(p, 16 + dz, 0, yz_rows(2, dz))
            ag_wait(p, 20 + dz, 1, yz_rows(2, dz))
        work(2)

    sums_far(0)
    sums_up(0)
    sums_down(0)
    step3(2)
    step3(3)
    step1x(4)
    step2a(4)
    mine = xv[2 * y + lax.div(z, 2), pl.ds(pl.multiple_of(16 * lax.rem(z, 2), 16), 16), :]
    ac[...] = mine.astype(F32) + sums_end(0)

    def feed(dy):
        rows = y_rows(dy)
        gate = up = jnp.zeros((64, 320), F32)
        for cc in range(CAND):
            block = nf[0, cc // 4, rows, pl.ds(256 * (cc % 4), 256)]
            gate = gate + dot_t(block, wi[0, cc])
            up = up + dot_t(block, wi[1, cc])
        hid[rows, :] = (gelu(gate) * up).astype(BF)
        for cc in range(CAND):
            part[1, cc // 4, rows, pl.ds(256 * (cc % 4), 256)] = jnp.dot(
                hid[rows, :], fo[cc], preferred_element_type=F32
            ).astype(BF)
        if dy == 1:
            sums_up(1)
        elif dy == 3:
            sums_down(1)
        elif dy == 2:
            sums_far(1)

    def early_0():
        step4(2)
        step4(3)

    def late_0():
        both(2)
        both(3)
        step2b(4)

    spread(0, rms(ac[...], gain2[...]).astype(BF), feed, early_0, late_0)
    step3(4)
    after = ac[...] + sums_end(1)

    ids = gold[k].astype(F32)
    eye = lax.broadcasted_iota(jnp.int32, (32, 32), 0) == lax.broadcasted_iota(jnp.int32, (32, 32), 1)
    start = [((2 * j + h) * width).astype(F32) for h in range(2)]

    def gold_rows():
        for i in range(8):
            column = jnp.sum(
                jnp.where(eye, jnp.broadcast_to(ids[i : i + 1, :], (32, 32)), 0.0),
                axis=1, keepdims=True,
            )
            st[pl.ds(32 * i, 32), :] = jnp.broadcast_to(column, (32, 128))

    def vocab(dy):
        rows = y_rows(dy)
        wanted = st[rows, :][:, :1]
        logits = []
        for h in range(2):
            one = jnp.zeros((64, width), F32)
            for cc in range(CAND):
                one = one + dot_t(nf[1, cc // 4, rows, pl.ds(256 * (cc % 4), 256)], wv[h, cc])
            logits.append(one)
        high = jnp.maximum(
            jnp.max(logits[0], axis=1, keepdims=True), jnp.max(logits[1], axis=1, keepdims=True)
        )
        total = jnp.zeros((64, 1), F32)
        picked = jnp.zeros((64, 1), F32)
        for h in range(2):
            total = total + jnp.sum(jnp.exp(logits[h] - high), axis=1, keepdims=True)
            at_col = lax.broadcasted_iota(jnp.int32, (64, width), 1).astype(F32) + start[h]
            picked = picked + jnp.sum(
                jnp.where(at_col == wanted, logits[h], 0.0), axis=1, keepdims=True
            )
        lane = lax.broadcasted_iota(jnp.int32, (64, 128), 1)
        st[pl.ds(pl.multiple_of(256 + 64 * lax.rem(y + dy, NY), 64), 64), :] = jnp.where(
            lane == 0, high, jnp.where(lane == 1, total, picked)
        )

    def early_1():
        step4(4)
        gold_rows()

    spread(1, rms(after, gain3[...]).astype(BF), vocab, early_1, lambda: both(4))

    stats = st[pl.ds(256, 256), :].T
    f1[j] = stats[0:8, :]

    @pl.loop(1, 16)
    def _(d):
        to = lax.rem(j + d, 16) * 2 + k
        send(f1.at[j], f1.at[j], f_send.at[0], f_recv.at[0], to, c)

    landed(f1.at[pl.ds(0, 15)], f_recv.at[0])
    top = f1[0][0:1, :]
    for n in range(1, 16):
        top = jnp.maximum(top, f1[n][0:1, :])
    total = jnp.zeros((1, ROWS), F32)
    picked = jnp.zeros((1, ROWS), F32)
    for n in range(16):
        total = total + f1[n][1:2, :] * jnp.exp(f1[n][0:1, :] - top)
        picked = picked + f1[n][2:3, :]
    logprob = picked - top - jnp.log(total)
    group = lax.div(lax.broadcasted_iota(jnp.int32, (8, ROWS), 1), 32)
    whose = lax.broadcasted_iota(jnp.int32, (8, ROWS), 0)
    per = jnp.sum(jnp.where(group == whose, logprob, 0.0), axis=1, keepdims=True) * (1.0 / 32)
    diag = lax.broadcasted_iota(jnp.int32, (8, 128), 0) == lax.broadcasted_iota(jnp.int32, (8, 128), 1)
    row = jnp.sum(jnp.where(diag, per, 0.0), axis=0, keepdims=True)
    f2[8 * k + c] = jnp.broadcast_to(row, (8, 128))

    @pl.loop(1, CAND)
    def _(d):
        to = lax.rem(c + d, CAND)
        send(f2.at[8 * k + c], f2.at[8 * k + c], f_send.at[1], f_recv.at[1], t, to)
        send(f2.at[8 * k + c], f2.at[8 * k + c], f_send.at[1], f_recv.at[1], partner, to)

    send(f2.at[8 * k + c], f2.at[8 * k + c], f_send.at[1], f_recv.at[1], partner, c)
    landed(f2.at[pl.ds(0, 15)], f_recv.at[1])
    lane = lax.broadcasted_iota(jnp.int32, (8, 8, 128), 2)
    cand = lax.broadcasted_iota(jnp.int32, (8, 8, 128), 0) * 8 + lane
    for b in range(2):
        count = counts[b]
        inside = jnp.where((cand < count) & (lane < 8), f2[pl.ds(8 * b, 8)], NEG)
        best_out[b] = jnp.max(inside)
        own_lane = lax.broadcasted_iota(jnp.int32, (1, 128), 1)
        own = f2[8 * b + c][0:1, :]
        scores_out[pl.ds(b, 1), :] = jnp.where(own_lane + 8 * c < count, own, 0.0)[:, :8]

    for n in range(2):
        landed(kb.at[pl.ds(0, 496), :], kv_send.at[n])
    for n in range(7):
        at_ = places[n]
        for slot in range(9):
            landed(at_(c) if slot < 5 else at_(c, (slot - 5) % 2), g_send.at[n, slot])
        if n < 5:
            landed(whole[n](k), g_dsend.at[n])
    @pl.loop(0, 2)
    def _(p):
        @pl.loop(0, 30)
        def _(n):
            landed(sz.at[p, 0], rs_send.at[p, n])
            landed(sz.at[p, 0], ag_send.at[p, n])

    landed(f1.at[pl.ds(0, 15)], f_send.at[0])
    landed(f2.at[pl.ds(0, 15)], f_send.at[1])


def body(
    dec_hidden, enc_keys, enc_values, enc_lengths, cand_counts, gold_ids, gain_cross, w_query,
    w_out, gain_ffn, w_in_gate, w_in_up, w_ffn_out, gain_final, w_vocab,
):
    units = w_in_gate.shape[1]
    width = w_vocab.shape[1]
    anywhere = pl.BlockSpec(memory_space=pl.ANY)
    vmem = pl.BlockSpec(memory_space=pltpu.VMEM)
    smem = pl.BlockSpec(memory_space=pltpu.SMEM)
    dma = pltpu.SemaphoreType.DMA
    return pl.pallas_call(
        kernel,
        name="layer",
        out_shape=(
            jax.ShapeDtypeStruct((2, 8), F32),
            jax.ShapeDtypeStruct((2,), F32),
        ),
        in_specs=[
            anywhere, anywhere, anywhere, smem, smem, vmem, vmem, anywhere, anywhere, vmem,
            anywhere, anywhere, anywhere, vmem, anywhere,
        ],
        out_specs=(vmem, smem),
        scratch_shapes=[
            pltpu.VMEM((8, 32, D), BF),
            pltpu.VMEM((ROWS, D), BF),
            pltpu.VMEM((2 * ROWS, 128), BF),
            pltpu.VMEM((4096, 128), BF),
            pltpu.VMEM((4096, 128), BF),
            pltpu.VMEM((8, 2 * ROWS, 512), F32),
            pltpu.VMEM((2 * ROWS, 4096), BF),
            pltpu.VMEM((ROWS, 128), BF),
            pltpu.VMEM((8, 128, 256), BF),
            pltpu.VMEM((8, 128, 256), BF),
            pltpu.VMEM((2, 8, 2 * units, 256), BF),
            pltpu.VMEM((8, 2 * units, 256), BF),
            pltpu.VMEM((2, 8, width, 256), BF),
            pltpu.VMEM((2, 2, ROWS, HALF), BF),
            pltpu.VMEM((2, 2, 64, HALF), BF),
            pltpu.VMEM((2, 2, 64, HALF), BF),
            pltpu.VMEM((2, 2, 64, HALF), BF),
            pltpu.VMEM((2, 2, 64, HALF), BF),
            pltpu.VMEM((2, 2, 64, HALF), BF),
            pltpu.VMEM((2, 2, 16, HALF), BF),
            pltpu.VMEM((2, 2, 16, HALF), BF),
            pltpu.VMEM((2, 2, 16, HALF), BF),
            pltpu.VMEM((2, 2, 16, HALF), BF),
            pltpu.VMEM((16, D), F32),
            pltpu.VMEM((2, 2, ROWS, HALF), BF),
            pltpu.VMEM((ROWS, 2 * units), BF),
            pltpu.VMEM((2 * ROWS, 128), F32),
            pltpu.VMEM((16, 8, ROWS), F32),
            pltpu.VMEM((16, 8, 128), F32),
            dma((2,)), dma((2,)), dma((7, 9)), dma((7, 9)), dma((5,)), dma((5,)), dma((5,)),
            dma((2, 30)), dma((2, 30)), dma((2, 30)), dma((2, 30)), dma((2,)), dma((2,)), dma((3,)),
        ],
        compiler_params=pltpu.CompilerParams(
            collective_id=0, has_side_effects=True, vmem_limit_bytes=62 * 1024 * 1024
        ),
    )(
        dec_hidden, enc_keys, enc_values, enc_lengths, cand_counts, gold_ids,
        gain_cross.reshape(1, -1), w_query.T, w_out, gain_ffn.reshape(1, -1), w_in_gate.T, w_in_up.T,
        w_ffn_out,
        gain_final.reshape(1, -1), w_vocab.T,
    )


def solution(mesh):
    in_specs = (
        P(None, "cand", None, None), P(None, "tok", None), P(None, "tok", None), P(), P(),
        P(None, "cand", None), P(), P("cand", "tok"), P("tok", "cand"), P(), P("cand", "tok"),
        P("cand", "tok"), P("tok", "cand"), P(), P("cand", "tok"),
    )
    return jax.shard_map(
        body, mesh=mesh, in_specs=in_specs, out_specs=(P(None, "cand"), P()), check_vma=False
    )
```

```python
import functools

import jax
import jax.numpy as jnp
from jax import lax
from jax.experimental import pallas as pl
from jax.experimental.pallas import tpu as pltpu
from jax.sharding import PartitionSpec as P

MESH = pl.DeviceIdType.MESH
EPS = 0.25
NY, NZ, NX = 4, 4, 4
TOK, CAND = 32, 8
D = 2048
HALF = 1024
ROWS = 256
NEG = -1e30
BF = jnp.bfloat16
F32 = jnp.float32


def rms(v, gain):
    squares = jnp.mean(v * v, axis=-1, keepdims=True)
    return v * lax.rsqrt(squares + EPS) * gain


def gelu(v):
    inner = 0.7978845608028654 * (v + 0.044715 * (v * v * v))
    return 0.5 * v * (1.0 + jnp.tanh(inner))


def dot_t(a, b):
    return lax.dot_general(a, b, (((1,), (1,)), ((), ())), preferred_element_type=F32)


def landed(ref, sem):
    pltpu.make_async_copy(ref, ref, sem).wait()


def kernel(
    x_in, keys, vals, lens, counts, gold, gain1, wq_in, wo_in, gain2, wg_in, wu_in, fo_in, gain3, wv_in,
    scores_out, best_out,
    xv, nx, q2, kb, vb, sc, pb,
    wq, wo, wi, fo, wv,
    part, ryf, ryd, rya, sy, by, rzf, rzd, rza, sz, ac, nf,
    st, f1, f2,
    kv_recv, kv_send, g_recv, g_send, g_own, g_dual, g_dsend,
    rs_recv, rs_send, ag_recv, ag_send, f_recv, f_send, l_sem,
):
    t = lax.axis_index("tok")
    c = lax.axis_index("cand")
    k = lax.rem(t, 2)
    j = lax.div(t, 2)
    y = lax.div(j, NZ)
    z = lax.rem(j, NZ)
    xx = lax.div(c, 2)
    zl = lax.rem(c, 2)

    def tok_of(yy, zz):
        return (lax.rem(yy, NY) * NZ + lax.rem(zz, NZ)) * 2 + k

    def cand_of(x_at, z_at):
        return lax.rem(x_at, NX) * 2 + z_at

    partner = t + 1 - 2 * k
    cz = cand_of(xx, 1 - zl)
    cp, cm = cand_of(xx + 1, zl), cand_of(xx + 3, zl)
    cpz, cmz = cand_of(xx + 1, 1 - zl), cand_of(xx + 3, 1 - zl)
    co, coz = cand_of(xx + 2, zl), cand_of(xx + 2, 1 - zl)

    def send(src, dst, s_sem, r_sem, tok, cand):
        pltpu.make_async_remote_copy(
            src_ref=src, dst_ref=dst, send_sem=s_sem, recv_sem=r_sem,
            device_id=(tok, cand), device_id_type=MESH,
        ).start()

    x_copy = pltpu.make_async_copy(x_in.at[k], xv, l_sem.at[0])
    x_copy.start()

    barrier = pltpu.get_barrier_semaphore()

    @pl.loop(1, TOK)
    def _(d):
        pl.semaphore_signal(
            barrier, inc=1, device_id=(lax.rem(t + d, TOK), c), device_id_type=MESH
        )

    @pl.loop(1, CAND)
    def _(d):
        pl.semaphore_signal(
            barrier, inc=1, device_id=(t, lax.rem(c + d, CAND)), device_id_type=MESH
        )
        pl.semaphore_signal(
            barrier, inc=1, device_id=(partner, lax.rem(c + d, CAND)), device_id_type=MESH
        )

    def stacked(ref, size):
        def at_(cc, part=None):
            if part is None:
                return ref.at[cc, pl.ds(size * k, size), :]
            return ref.at[cc, pl.ds(size * k + size // 2 * part, size // 2), :]
        return at_

    def i_at(cc, part=None):
        if part is None:
            return wi.at[:, cc, pl.ds(160 * k, 160), :]
        return wi.at[:, cc, pl.ds(160 * k + 80 * part, 80), :]

    width = wv.shape[2]

    def v_at(cc, part=None):
        if part is None:
            return wv.at[k, cc]
        return wv.at[k, cc, pl.ds(0, 512), :] if part == 0 else wv.at[k, cc, pl.ds(512, width - 512), :]

    def kv_at(ref):
        def at_(cc, part=None):
            if part is None:
                return ref.at[pl.ds(512 * cc, 512), :]
            return ref.at[pl.ds(512 * cc + 256 * part, 256), :]
        return at_

    places = [stacked(wq, 64), stacked(wo, 64), i_at, stacked(fo, 160), v_at, kv_at(kb), kv_at(vb)]
    whole = [
        lambda h: wq.at[:, pl.ds(64 * h, 64), :], lambda h: wo.at[:, pl.ds(64 * h, 64), :],
        lambda h: wi.at[:, :, pl.ds(160 * h, 160), :], lambda h: fo.at[:, pl.ds(160 * h, 160), :],
        lambda h: wv.at[h],
    ]

    def own_copies():
        for n, src in ((0, wq_in), (1, wo_in), (3, fo_in), (4, wv_in)):
            pltpu.make_async_copy(src, places[n](c), g_own.at[n]).start()
        for m, src in enumerate((wg_in, wu_in)):
            pltpu.make_async_copy(
                src, wi.at[m, c, pl.ds(160 * k, 160), :], g_own.at[2]
            ).start()

    def g_send_to(n, slot, src, dst, cand):
        send(src, dst, g_send.at[n, slot], g_recv.at[n, slot], t, cand)

    def step1z(n):
        here = places[n](c)
        if n < 5:
            landed(here, g_own.at[n])
        g_send_to(n, 0, here, here, cz)

    def step1x(n):
        here = places[n](c)
        g_send_to(n, 1, here, here, cp)
        g_send_to(n, 2, here, here, cm)

    def step1(n):
        step1z(n)
        step1x(n)

    def step2a(n):
        at_ = places[n]
        landed(at_(cz), g_recv.at[n, 0])
        g_send_to(n, 3, at_(cz), at_(cz), cp)
        g_send_to(n, 4, at_(cz), at_(cz), cm)

    def step2b(n):
        at_ = places[n]
        landed(at_(cm), g_recv.at[n, 1])
        g_send_to(n, 5, at_(cm, 0), at_(cm, 0), cp)
        landed(at_(cp), g_recv.at[n, 2])
        g_send_to(n, 6, at_(cp, 1), at_(cp, 1), cm)

    def step2(n):
        step2a(n)
        step2b(n)

    def step3(n):
        at_ = places[n]
        landed(at_(cmz), g_recv.at[n, 3])
        g_send_to(n, 7, at_(cmz, 0), at_(cmz, 0), cp)
        landed(at_(cpz), g_recv.at[n, 4])
        g_send_to(n, 8, at_(cpz, 1), at_(cpz, 1), cm)

    def step4(n):
        at_ = places[n]
        landed(at_(co, 0), g_recv.at[n, 5])
        landed(at_(co, 1), g_recv.at[n, 6])
        landed(at_(coz, 0), g_recv.at[n, 7])
        landed(at_(coz, 1), g_recv.at[n, 8])
        if n < 5:
            send(whole[n](k), whole[n](k), g_dsend.at[n], g_dual.at[n], partner, c)

    def both(n):
        landed(whole[n](1 - k), g_dual.at[n])


    own_copies()

    x_copy.wait()

    @pl.loop(0, 8)
    def _(i):
        rows = xv[i].astype(F32)
        nx[pl.ds(pl.multiple_of(32 * i, 32), 32), :] = rms(rows, gain1[...]).astype(BF)

    pl.semaphore_wait(barrier, TOK - 1 + 2 * (CAND - 1))

    step1(0)
    step1(1)

    for n, (src, dst) in enumerate(((keys, kb), (vals, vb))):
        here = dst.at[pl.ds(512 * c + 16 * t, 16), :]
        pltpu.make_async_copy(
            src.at[k, pl.ds(16 * c, 16), pl.ds(pl.multiple_of(128 * j, 128), 128)],
            here, l_sem.at[1 + n],
        ).start()

        @pl.loop(1, TOK)
        def _(d, src=src, n=n, here=here):
            to = lax.rem(t + d, TOK)
            send(
                src.at[
                    lax.rem(to, 2), pl.ds(16 * c, 16),
                    pl.ds(pl.multiple_of(128 * lax.div(to, 2), 128), 128),
                ],
                here, kv_send.at[n], kv_recv.at[n], to, c,
            )

    def kv_mine(n):
        ref = (kb, vb)[n]
        pltpu.make_async_copy(
            ref.at[pl.ds(0, 16), :], ref.at[pl.ds(512 * c + 16 * t, 16), :], l_sem.at[1 + n]
        ).wait()
        landed(ref.at[pl.ds(0, 496), :], kv_recv.at[n])

    step2(0)
    step2(1)
    step3(0)
    step3(1)
    step1(2)
    step1(3)
    kv_mine(0)
    step1(5)
    kv_mine(1)
    step1(6)
    step1z(4)
    step4(0)
    step4(1)
    both(0)
    zero = jnp.zeros((ROWS, 64), BF)
    query = jnp.zeros((ROWS, 128), F32)
    for cc in range(CAND):
        query = query + dot_t(nx[:, 256 * cc : 256 * cc + 256], wq[cc])
    query = query.astype(BF)
    q2[pl.ds(0, ROWS), :] = jnp.concatenate([query[:, :64], zero], axis=1)
    q2[pl.ds(ROWS, ROWS), :] = jnp.concatenate([zero, query[:, 64:]], axis=1)

    length = lens[k]

    def score(cc):
        place = lax.broadcasted_iota(jnp.int32, (1, 512), 1)
        token = lax.div(place, 16) * 128 + 16 * cc + lax.rem(place, 16)
        live = token < length
        block = kb[pl.ds(pl.multiple_of(512 * cc, 512), 512), :]

        @pl.loop(0, 4)
        def _(r):
            rows = pl.ds(pl.multiple_of(128 * r, 128), 128)
            s = dot_t(q2[rows, :], block)
            sc[cc, rows, :] = jnp.where(live, s, NEG)

    step2(5)
    score(c)
    score(cz)
    score(cm)
    step3(5)
    step2(6)
    score(cp)
    score(cmz)
    score(cpz)
    step4(5)
    score(co)
    score(coz)
    step3(6)
    step2(2)
    step2(3)

    @pl.loop(0, 16)
    def _(r):
        rows = pl.ds(pl.multiple_of(32 * r, 32), 32)
        high = sc[0, rows, :]
        for cc in range(1, CAND):
            high = jnp.maximum(high, sc[cc, rows, :])
        top = jnp.max(high, axis=1, keepdims=True)
        total = jnp.zeros((32, 512), F32)
        for cc in range(CAND):
            w = jnp.exp(sc[cc, rows, :] - top)
            total = total + w
            pb[rows, pl.ds(512 * cc, 512)] = w.astype(BF)
        st[rows, :] = jnp.broadcast_to(jnp.sum(total, axis=1, keepdims=True), (32, 128))

    both(1)
    step4(6)

    ty, tm = tok_of(y + 1, z), tok_of(y + 3, z)
    tz, tn = tok_of(y, z + 1), tok_of(y, z + 3)

    def y_rows(dy):
        return pl.ds(pl.multiple_of(64 * lax.rem(y + dy, NY), 64), 64)

    def z_rows(dz):
        return pl.ds(pl.multiple_of(16 * lax.rem(z + dz, NZ), 16), 16)

    def yz_rows(dy, dz):
        at_row = 64 * lax.rem(y + dy, NY) + 16 * lax.rem(z + dz, NZ)
        return pl.ds(pl.multiple_of(at_row, 16), 16)

    order = (2, 1, 3, 0)

    def rs_go(p, n, src, dst, tok):
        send(src, dst, rs_send.at[p, n], rs_recv.at[p, n], tok, c)

    def sums_far(p):
        for dz in order:
            rs_go(p, dz, part.at[p, 0, yz_rows(2, dz)], ryf.at[p, 0, z_rows(dz)], ty)
            rs_go(p, 4 + dz, part.at[p, 1, yz_rows(2, dz)], ryf.at[p, 1, z_rows(dz)], tm)

    def sums_up(p):
        for dz in order:
            rs_go(p, 8 + dz, part.at[p, 1, yz_rows(1, dz)], ryd.at[p, 1, z_rows(dz)], ty)

    def sums_down(p):
        for dz in order:
            rs_go(p, 12 + dz, part.at[p, 0, yz_rows(3, dz)], ryd.at[p, 0, z_rows(dz)], tm)

    def add(out, *terms):
        total = terms[0].astype(F32)
        for term in terms[1:]:
            total = total + term.astype(F32)
        out[...] = total.astype(BF)

    def sums_end(p, mid):
        for dz in order:
            zr = z_rows(dz)
            landed(ryf.at[p, 0, zr], rs_recv.at[p, dz])
            add(sy.at[p, 0, zr], ryf[p, 0, zr], part[p, 0, yz_rows(1, dz)])
            rs_go(p, 16 + dz, sy.at[p, 0, zr], rya.at[p, 0, zr], ty)
            landed(ryf.at[p, 1, zr], rs_recv.at[p, 4 + dz])
            add(sy.at[p, 1, zr], ryf[p, 1, zr], part[p, 1, yz_rows(3, dz)])
            rs_go(p, 20 + dz, sy.at[p, 1, zr], rya.at[p, 1, zr], tm)
        mid()
        for dz in order:
            zr = z_rows(dz)
            landed(ryd.at[p, 0, zr], rs_recv.at[p, 12 + dz])
            landed(ryd.at[p, 1, zr], rs_recv.at[p, 8 + dz])
            for h in range(2):
                landed(rya.at[p, h, zr], rs_recv.at[p, 16 + 4 * h + dz])
                add(by.at[p, h, zr], rya[p, h, zr], ryd[p, h, zr], part[p, h, yz_rows(0, dz)])
            if dz == 2:
                rs_go(p, 24, by.at[p, 0, zr], rzf.at[p, 0], tz)
                rs_go(p, 25, by.at[p, 1, zr], rzf.at[p, 1], tn)
            elif dz == 1:
                rs_go(p, 26, by.at[p, 1, zr], rzd.at[p, 1], tz)
            elif dz == 3:
                rs_go(p, 27, by.at[p, 0, zr], rzd.at[p, 0], tn)
        landed(rzf.at[p, 0], rs_recv.at[p, 24])
        add(sz.at[p, 0], rzf[p, 0], by[p, 0, z_rows(1)])
        rs_go(p, 28, sz.at[p, 0], rza.at[p, 0], tz)
        landed(rzf.at[p, 1], rs_recv.at[p, 25])
        add(sz.at[p, 1], rzf[p, 1], by[p, 1, z_rows(3)])
        rs_go(p, 29, sz.at[p, 1], rza.at[p, 1], tn)
        landed(rzd.at[p, 1], rs_recv.at[p, 26])
        landed(rzd.at[p, 0], rs_recv.at[p, 27])
        sums = []
        for h in range(2):
            landed(rza.at[p, h], rs_recv.at[p, 28 + h])
            sums.append(
                rza[p, h].astype(F32) + rzd[p, h].astype(F32) + by[p, h, z_rows(0)].astype(F32)
            )
        return jnp.concatenate(sums, axis=1)

    def ag_go(p, n, h, rows, tok):
        where = nf.at[p, h, rows, :]
        send(where, where, ag_send.at[p, n], ag_recv.at[p, n], tok, c)

    def ag_wait(p, n, h, rows):
        landed(nf.at[p, h, rows, :], ag_recv.at[p, n])

    def spread(p, value, work, early, late):
        nf[p, 0, yz_rows(0, 0), :] = value[:, :HALF]
        nf[p, 1, yz_rows(0, 0), :] = value[:, HALF:]

        def along_y(dz):
            rows = yz_rows(0, dz)
            ag_go(p, dz, 0, rows, ty)
            ag_go(p, 4 + dz, 1, rows, tm)
            ag_go(p, 8 + dz, 1, rows, ty)
            ag_go(p, 12 + dz, 0, rows, tm)

        def onward(dz):
            ag_wait(p, dz, 0, yz_rows(3, dz))
            ag_go(p, 16 + dz, 0, yz_rows(3, dz), ty)
            ag_wait(p, 4 + dz, 1, yz_rows(1, dz))
            ag_go(p, 20 + dz, 1, yz_rows(1, dz), tm)

        own = yz_rows(0, 0)
        ag_go(p, 24, 0, own, tz)
        ag_go(p, 25, 1, own, tn)
        ag_go(p, 26, 1, own, tz)
        ag_go(p, 27, 0, own, tn)
        along_y(0)
        early()
        ag_wait(p, 24, 0, yz_rows(0, 3))
        ag_go(p, 28, 0, yz_rows(0, 3), tz)
        ag_wait(p, 25, 1, yz_rows(0, 1))
        ag_go(p, 29, 1, yz_rows(0, 1), tn)
        ag_wait(p, 26, 1, yz_rows(0, 3))
        along_y(3)
        ag_wait(p, 27, 0, yz_rows(0, 1))
        along_y(1)
        onward(0)
        ag_wait(p, 28, 0, yz_rows(0, 2))
        ag_wait(p, 29, 1, yz_rows(0, 2))
        along_y(2)
        late()
        work((0,))
        for dz in (3, 1, 2):
            onward(dz)
        for dz in range(4):
            ag_wait(p, 8 + dz, 1, yz_rows(3, dz))
            ag_wait(p, 12 + dz, 0, yz_rows(1, dz))
        work((3, 1))
        for dz in range(4):
            ag_wait(p, 16 + dz, 0, yz_rows(2, dz))
            ag_wait(p, 20 + dz, 1, yz_rows(2, dz))
        work((2,))

    def blocks(p, cc, dys):
        pieces = [nf[p, cc // 4, y_rows(dy), pl.ds(256 * (cc % 4), 256)] for dy in dys]
        return pieces[0] if len(pieces) == 1 else jnp.concatenate(pieces, axis=0)

    def attend(dy):
        low = y_rows(dy)
        upp = pl.ds(pl.multiple_of(64 * lax.rem(y + dy, NY) + ROWS, 64), 64)
        a = jnp.dot(pb[low, :], vb[...], preferred_element_type=F32) / st[low, :]
        b = jnp.dot(pb[upp, :], vb[...], preferred_element_type=F32) / st[upp, :]
        lane = lax.broadcasted_iota(jnp.int32, (64, 128), 1)
        heads = jnp.where(lane < 64, a, b).astype(BF)
        for cc in range(CAND):
            part[0, cc // 4, low, pl.ds(256 * (cc % 4), 256)] = jnp.dot(
                heads, wo[cc], preferred_element_type=F32
            ).astype(BF)

    attend(2)
    sums_far(0)
    attend(1)
    sums_up(0)
    attend(3)
    sums_down(0)
    attend(0)

    def mid_0():
        step3(2)
        step3(3)
        step1x(4)
        step2a(4)

    mine = xv[2 * y + lax.div(z, 2), pl.ds(pl.multiple_of(16 * lax.rem(z, 2), 16), 16), :]
    ac[...] = mine.astype(F32) + sums_end(0, mid_0)

    def feed(dys):
        gate = up = jnp.zeros((64 * len(dys), 320), F32)
        for cc in range(CAND):
            block = blocks(0, cc, dys)
            gate = gate + dot_t(block, wi[0, cc])
            up = up + dot_t(block, wi[1, cc])
        hidden = (gelu(gate) * up).astype(BF)
        for cc in range(CAND):
            down = jnp.dot(hidden, fo[cc], preferred_element_type=F32).astype(BF)
            for n, dy in enumerate(dys):
                part[1, cc // 4, y_rows(dy), pl.ds(256 * (cc % 4), 256)] = down[
                    64 * n : 64 * n + 64
                ]
        if len(dys) == 2:
            sums_up(1)
            sums_down(1)
            step3(4)
        elif dys[0] == 2:
            sums_far(1)

    def early_0():
        step4(2)
        step4(3)

    def late_0():
        both(2)
        both(3)
        step2b(4)

    spread(0, rms(ac[...], gain2[...]).astype(BF), feed, early_0, late_0)
    after = ac[...] + sums_end(1, lambda: step4(4))

    ids = gold[k].astype(F32)
    eye = lax.broadcasted_iota(jnp.int32, (32, 32), 0) == lax.broadcasted_iota(jnp.int32, (32, 32), 1)
    start = [((2 * j + h) * width).astype(F32) for h in range(2)]

    def gold_rows():
        for i in range(8):
            column = jnp.sum(
                jnp.where(eye, jnp.broadcast_to(ids[i : i + 1, :], (32, 32)), 0.0),
                axis=1, keepdims=True,
            )
            st[pl.ds(32 * i, 32), :] = jnp.broadcast_to(column, (32, 128))

    def vocab(dys):
        size = 64 * len(dys)
        wanted = [st[y_rows(dy), :][:, :1] for dy in dys]
        wanted = wanted[0] if len(dys) == 1 else jnp.concatenate(wanted, axis=0)
        logits = []
        for h in range(2):
            one = jnp.zeros((size, width), F32)
            for cc in range(CAND):
                one = one + dot_t(blocks(1, cc, dys), wv[h, cc])
            logits.append(one)
        high = jnp.maximum(
            jnp.max(logits[0], axis=1, keepdims=True), jnp.max(logits[1], axis=1, keepdims=True)
        )
        total = jnp.zeros((size, 1), F32)
        picked = jnp.zeros((size, 1), F32)
        for h in range(2):
            total = total + jnp.sum(jnp.exp(logits[h] - high), axis=1, keepdims=True)
            at_col = lax.broadcasted_iota(jnp.int32, (size, width), 1).astype(F32) + start[h]
            picked = picked + jnp.sum(
                jnp.where(at_col == wanted, logits[h], 0.0), axis=1, keepdims=True
            )
        lane = lax.broadcasted_iota(jnp.int32, (size, 128), 1)
        found = jnp.where(lane == 0, high, jnp.where(lane == 1, total, picked))
        for n, dy in enumerate(dys):
            at_row = 256 + 64 * lax.rem(y + dy, NY)
            st[pl.ds(pl.multiple_of(at_row, 64), 64), :] = found[64 * n : 64 * n + 64]

    def early_1():
        gold_rows()

    spread(1, rms(after, gain3[...]).astype(BF), vocab, early_1, lambda: both(4))

    stats = st[pl.ds(256, 256), :].T
    f1[j] = stats[0:8, :]

    @pl.loop(1, 16)
    def _(d):
        to = lax.rem(j + d, 16) * 2 + k
        send(f1.at[j], f1.at[j], f_send.at[0], f_recv.at[0], to, c)

    landed(f1.at[pl.ds(0, 15)], f_recv.at[0])
    top = f1[0][0:1, :]
    for n in range(1, 16):
        top = jnp.maximum(top, f1[n][0:1, :])
    total = jnp.zeros((1, ROWS), F32)
    picked = jnp.zeros((1, ROWS), F32)
    for n in range(16):
        total = total + f1[n][1:2, :] * jnp.exp(f1[n][0:1, :] - top)
        picked = picked + f1[n][2:3, :]
    logprob = picked - top - jnp.log(total)
    group = lax.div(lax.broadcasted_iota(jnp.int32, (8, ROWS), 1), 32)
    whose = lax.broadcasted_iota(jnp.int32, (8, ROWS), 0)
    per = jnp.sum(jnp.where(group == whose, logprob, 0.0), axis=1, keepdims=True) * (1.0 / 32)
    diag = lax.broadcasted_iota(jnp.int32, (8, 128), 0) == lax.broadcasted_iota(jnp.int32, (8, 128), 1)
    row = jnp.sum(jnp.where(diag, per, 0.0), axis=0, keepdims=True)
    f2[8 * k + c] = jnp.broadcast_to(row, (8, 128))

    @pl.loop(1, CAND)
    def _(d):
        to = lax.rem(c + d, CAND)
        send(f2.at[8 * k + c], f2.at[8 * k + c], f_send.at[1], f_recv.at[1], t, to)
        send(f2.at[8 * k + c], f2.at[8 * k + c], f_send.at[1], f_recv.at[1], partner, to)

    send(f2.at[8 * k + c], f2.at[8 * k + c], f_send.at[1], f_recv.at[1], partner, c)
    landed(f2.at[pl.ds(0, 15)], f_recv.at[1])
    lane = lax.broadcasted_iota(jnp.int32, (8, 8, 128), 2)
    cand = lax.broadcasted_iota(jnp.int32, (8, 8, 128), 0) * 8 + lane
    for b in range(2):
        count = counts[b]
        inside = jnp.where((cand < count) & (lane < 8), f2[pl.ds(8 * b, 8)], NEG)
        best_out[b] = jnp.max(inside)
        own_lane = lax.broadcasted_iota(jnp.int32, (1, 128), 1)
        own = f2[8 * b + c][0:1, :]
        scores_out[pl.ds(b, 1), :] = jnp.where(own_lane + 8 * c < count, own, 0.0)[:, :8]

    for n in range(2):
        landed(kb.at[pl.ds(0, 496), :], kv_send.at[n])
    for n in range(7):
        at_ = places[n]
        for slot in range(9):
            landed(at_(c) if slot < 5 else at_(c, (slot - 5) % 2), g_send.at[n, slot])
        if n < 5:
            landed(whole[n](k), g_dsend.at[n])
    @pl.loop(0, 2)
    def _(p):
        @pl.loop(0, 30)
        def _(n):
            landed(sz.at[p, 0], rs_send.at[p, n])
            landed(sz.at[p, 0], ag_send.at[p, n])

    landed(f1.at[pl.ds(0, 15)], f_send.at[0])
    landed(f2.at[pl.ds(0, 15)], f_send.at[1])


def body(
    dec_hidden, enc_keys, enc_values, enc_lengths, cand_counts, gold_ids, gain_cross, w_query,
    w_out, gain_ffn, w_in_gate, w_in_up, w_ffn_out, gain_final, w_vocab,
):
    units = w_in_gate.shape[1]
    width = w_vocab.shape[1]
    anywhere = pl.BlockSpec(memory_space=pl.ANY)
    vmem = pl.BlockSpec(memory_space=pltpu.VMEM)
    smem = pl.BlockSpec(memory_space=pltpu.SMEM)
    dma = pltpu.SemaphoreType.DMA
    return pl.pallas_call(
        kernel,
        name="layer",
        out_shape=(
            jax.ShapeDtypeStruct((2, 8), F32),
            jax.ShapeDtypeStruct((2,), F32),
        ),
        in_specs=[
            anywhere, anywhere, anywhere, smem, smem, vmem, vmem, anywhere, anywhere, vmem,
            anywhere, anywhere, anywhere, vmem, anywhere,
        ],
        out_specs=(vmem, smem),
        scratch_shapes=[
            pltpu.VMEM((8, 32, D), BF),
            pltpu.VMEM((ROWS, D), BF),
            pltpu.VMEM((2 * ROWS, 128), BF),
            pltpu.VMEM((4096, 128), BF),
            pltpu.VMEM((4096, 128), BF),
            pltpu.VMEM((8, 2 * ROWS, 512), F32),
            pltpu.VMEM((2 * ROWS, 4096), BF),
            pltpu.VMEM((8, 128, 256), BF),
            pltpu.VMEM((8, 128, 256), BF),
            pltpu.VMEM((2, 8, 2 * units, 256), BF),
            pltpu.VMEM((8, 2 * units, 256), BF),
            pltpu.VMEM((2, 8, width, 256), BF),
            pltpu.VMEM((2, 2, ROWS, HALF), BF),
            pltpu.VMEM((2, 2, 64, HALF), BF),
            pltpu.VMEM((2, 2, 64, HALF), BF),
            pltpu.VMEM((2, 2, 64, HALF), BF),
            pltpu.VMEM((2, 2, 64, HALF), BF),
            pltpu.VMEM((2, 2, 64, HALF), BF),
            pltpu.VMEM((2, 2, 16, HALF), BF),
            pltpu.VMEM((2, 2, 16, HALF), BF),
            pltpu.VMEM((2, 2, 16, HALF), BF),
            pltpu.VMEM((2, 2, 16, HALF), BF),
            pltpu.VMEM((16, D), F32),
            pltpu.VMEM((2, 2, ROWS, HALF), BF),
            pltpu.VMEM((2 * ROWS, 128), F32),
            pltpu.VMEM((16, 8, ROWS), F32),
            pltpu.VMEM((16, 8, 128), F32),
            dma((2,)), dma((2,)), dma((7, 9)), dma((7, 9)), dma((5,)), dma((5,)), dma((5,)),
            dma((2, 30)), dma((2, 30)), dma((2, 30)), dma((2, 30)), dma((2,)), dma((2,)), dma((3,)),
        ],
        compiler_params=pltpu.CompilerParams(
            collective_id=0, has_side_effects=True, vmem_limit_bytes=62 * 1024 * 1024
        ),
    )(
        dec_hidden, enc_keys, enc_values, enc_lengths, cand_counts, gold_ids,
        gain_cross.reshape(1, -1), w_query.T, w_out, gain_ffn.reshape(1, -1), w_in_gate.T, w_in_up.T,
        w_ffn_out,
        gain_final.reshape(1, -1), w_vocab.T,
    )


def solution(mesh):
    in_specs = (
        P(None, "cand", None, None), P(None, "tok", None), P(None, "tok", None), P(), P(),
        P(None, "cand", None), P(), P("cand", "tok"), P("tok", "cand"), P(), P("cand", "tok"),
        P("cand", "tok"), P("tok", "cand"), P(), P("cand", "tok"),
    )
    return jax.shard_map(
        body, mesh=mesh, in_specs=in_specs, out_specs=(P(None, "cand"), P()), check_vma=False
    )
```

```python
import functools

import jax
import jax.numpy as jnp
from jax import lax
from jax.experimental import pallas as pl
from jax.experimental.pallas import tpu as pltpu
from jax.sharding import PartitionSpec as P

MESH = pl.DeviceIdType.MESH
EPS = 0.25
NY, NZ, NX = 4, 4, 4
TOK, CAND = 32, 8
D = 2048
HALF = 1024
ROWS = 256
NEG = -1e30
BF = jnp.bfloat16
F32 = jnp.float32


def rms(v, gain):
    squares = jnp.mean(v * v, axis=-1, keepdims=True)
    return v * lax.rsqrt(squares + EPS) * gain


def gelu(v):
    inner = 0.7978845608028654 * (v + 0.044715 * (v * v * v))
    return 0.5 * v * (1.0 + jnp.tanh(inner))


def dot_t(a, b):
    return lax.dot_general(a, b, (((1,), (1,)), ((), ())), preferred_element_type=F32)


def landed(ref, sem):
    pltpu.make_async_copy(ref, ref, sem).wait()


def kernel(
    x_in, keys, vals, lens, counts, gold, gain1, wq_in, wo_in, gain2, wg_in, wu_in, fo_in, gain3, wv_in,
    scores_out, best_out,
    xv, nx, q2, kb, vb, sc, pb,
    wq, wo, wi, fo, wv,
    part, ry, by, rz, ac, nf,
    st, f1, f2,
    kv_recv, kv_send, g_recv, g_send, g_own, g_dual, g_dsend,
    rs_recv, rs_send, ag_recv, ag_send, f_recv, f_send, l_sem,
):
    t = lax.axis_index("tok")
    c = lax.axis_index("cand")
    k = lax.rem(t, 2)
    j = lax.div(t, 2)
    y = lax.div(j, NZ)
    z = lax.rem(j, NZ)
    xx = lax.div(c, 2)
    zl = lax.rem(c, 2)

    def tok_of(yy, zz):
        return (lax.rem(yy, NY) * NZ + lax.rem(zz, NZ)) * 2 + k

    def cand_of(x_at, z_at):
        return lax.rem(x_at, NX) * 2 + z_at

    partner = t + 1 - 2 * k
    cz = cand_of(xx, 1 - zl)
    cp, cm = cand_of(xx + 1, zl), cand_of(xx + 3, zl)
    cpz, cmz = cand_of(xx + 1, 1 - zl), cand_of(xx + 3, 1 - zl)
    co, coz = cand_of(xx + 2, zl), cand_of(xx + 2, 1 - zl)

    def send(src, dst, s_sem, r_sem, tok, cand):
        pltpu.make_async_remote_copy(
            src_ref=src, dst_ref=dst, send_sem=s_sem, recv_sem=r_sem,
            device_id=(tok, cand), device_id_type=MESH,
        ).start()

    x_copy = pltpu.make_async_copy(x_in.at[k], xv, l_sem.at[0])
    x_copy.start()

    barrier = pltpu.get_barrier_semaphore()

    @pl.loop(1, TOK)
    def _(d):
        pl.semaphore_signal(
            barrier, inc=1, device_id=(lax.rem(t + d, TOK), c), device_id_type=MESH
        )

    @pl.loop(1, CAND)
    def _(d):
        pl.semaphore_signal(
            barrier, inc=1, device_id=(t, lax.rem(c + d, CAND)), device_id_type=MESH
        )
        pl.semaphore_signal(
            barrier, inc=1, device_id=(partner, lax.rem(c + d, CAND)), device_id_type=MESH
        )

    def stacked(ref, size):
        def at_(cc, part=None):
            if part is None:
                return ref.at[cc, pl.ds(size * k, size), :]
            return ref.at[cc, pl.ds(size * k + size // 2 * part, size // 2), :]
        return at_

    def i_at(cc, part=None):
        if part is None:
            return wi.at[:, cc, pl.ds(160 * k, 160), :]
        return wi.at[:, cc, pl.ds(160 * k + 80 * part, 80), :]

    width = wv.shape[2]

    def v_at(cc, part=None):
        if part is None:
            return wv.at[k, cc]
        return wv.at[k, cc, pl.ds(0, 512), :] if part == 0 else wv.at[k, cc, pl.ds(512, width - 512), :]

    def kv_at(ref):
        def at_(cc, part=None):
            if part is None:
                return ref.at[pl.ds(512 * cc, 512), :]
            return ref.at[pl.ds(512 * cc + 256 * part, 256), :]
        return at_

    places = [stacked(wq, 64), stacked(wo, 64), i_at, stacked(fo, 160), v_at, kv_at(kb), kv_at(vb)]
    whole = [
        lambda h: wq.at[:, pl.ds(64 * h, 64), :], lambda h: wo.at[:, pl.ds(64 * h, 64), :],
        lambda h: wi.at[:, :, pl.ds(160 * h, 160), :], lambda h: fo.at[:, pl.ds(160 * h, 160), :],
        lambda h: wv.at[h],
    ]

    def own_copies():
        for n, src in ((0, wq_in), (1, wo_in), (3, fo_in), (4, wv_in)):
            pltpu.make_async_copy(src, places[n](c), g_own.at[n]).start()
        for m, src in enumerate((wg_in, wu_in)):
            pltpu.make_async_copy(
                src, wi.at[m, c, pl.ds(160 * k, 160), :], g_own.at[2]
            ).start()

    def g_send_to(n, slot, src, dst, cand):
        send(src, dst, g_send.at[n, slot], g_recv.at[n, slot], t, cand)

    def ready(n):
        landed(places[n](c), g_own.at[n])

    def step1z(n):
        here = places[n](c)
        g_send_to(n, 0, here, here, cz)

    def step1x(n):
        here = places[n](c)
        g_send_to(n, 1, here, here, cp)
        g_send_to(n, 2, here, here, cm)

    def step1(n):
        step1z(n)
        step1x(n)

    def step2a(n):
        at_ = places[n]
        landed(at_(cz), g_recv.at[n, 0])
        g_send_to(n, 3, at_(cz), at_(cz), cp)
        g_send_to(n, 4, at_(cz), at_(cz), cm)

    def step2b(n):
        at_ = places[n]
        landed(at_(cm), g_recv.at[n, 1])
        g_send_to(n, 5, at_(cm, 0), at_(cm, 0), cp)
        landed(at_(cp), g_recv.at[n, 2])
        g_send_to(n, 6, at_(cp, 1), at_(cp, 1), cm)

    def step2(n):
        step2a(n)
        step2b(n)

    def step3(n):
        at_ = places[n]
        landed(at_(cmz), g_recv.at[n, 3])
        g_send_to(n, 7, at_(cmz, 0), at_(cmz, 0), cp)
        landed(at_(cpz), g_recv.at[n, 4])
        g_send_to(n, 8, at_(cpz, 1), at_(cpz, 1), cm)

    def across(which):
        for cc in which:
            send(v_at(cc), v_at(cc), g_dsend.at[4], g_dual.at[4], partner, c)

    def step4(n):
        at_ = places[n]
        landed(at_(co, 0), g_recv.at[n, 5])
        landed(at_(co, 1), g_recv.at[n, 6])
        landed(at_(coz, 0), g_recv.at[n, 7])
        landed(at_(coz, 1), g_recv.at[n, 8])
        if n < 5:
            if n < 4:
                send(whole[n](k), whole[n](k), g_dsend.at[n], g_dual.at[n], partner, c)
            else:
                across((cmz, cpz, co, coz))

    def both(n):
        landed(whole[n](1 - k), g_dual.at[n])


    own_copies()

    x_copy.wait()

    @pl.loop(0, 8)
    def _(i):
        rows = xv[i].astype(F32)
        nx[pl.ds(pl.multiple_of(32 * i, 32), 32), :] = rms(rows, gain1[...]).astype(BF)

    pl.semaphore_wait(barrier, TOK - 1 + 2 * (CAND - 1))

    ready(0)
    ready(1)
    step1(0)
    step1(1)

    for n, (src, dst) in enumerate(((keys, kb), (vals, vb))):
        here = dst.at[pl.ds(512 * c + 16 * t, 16), :]
        pltpu.make_async_copy(
            src.at[k, pl.ds(16 * c, 16), pl.ds(pl.multiple_of(128 * j, 128), 128)],
            here, l_sem.at[1 + n],
        ).start()

        @pl.loop(1, TOK)
        def _(d, src=src, n=n, here=here):
            to = lax.rem(t + d, TOK)
            send(
                src.at[
                    lax.rem(to, 2), pl.ds(16 * c, 16),
                    pl.ds(pl.multiple_of(128 * lax.div(to, 2), 128), 128),
                ],
                here, kv_send.at[n], kv_recv.at[n], to, c,
            )

    def kv_mine(n):
        ref = (kb, vb)[n]
        pltpu.make_async_copy(
            ref.at[pl.ds(0, 16), :], ref.at[pl.ds(512 * c + 16 * t, 16), :], l_sem.at[1 + n]
        ).wait()
        landed(ref.at[pl.ds(0, 496), :], kv_recv.at[n])

    ready(2)
    ready(3)
    step1x(2)
    step1x(3)
    step2(0)
    step2(1)
    step3(0)
    step3(1)
    kv_mine(0)
    step1(5)
    kv_mine(1)
    step1(6)
    ready(4)
    step1z(2)
    step1z(3)
    step1z(4)
    step4(0)
    step4(1)
    both(0)
    zero = jnp.zeros((ROWS, 64), BF)
    query = jnp.zeros((ROWS, 128), F32)
    for cc in range(CAND):
        query = query + dot_t(nx[:, 256 * cc : 256 * cc + 256], wq[cc])
    query = query.astype(BF)
    q2[pl.ds(0, ROWS), :] = jnp.concatenate([query[:, :64], zero], axis=1)
    q2[pl.ds(ROWS, ROWS), :] = jnp.concatenate([zero, query[:, 64:]], axis=1)

    length = lens[k]

    def score(cc, opening=False):
        place = lax.broadcasted_iota(jnp.int32, (1, 512), 1)
        token = lax.div(place, 16) * 128 + 16 * cc + lax.rem(place, 16)
        live = token < length
        block = kb[pl.ds(pl.multiple_of(512 * cc, 512), 512), :]

        @pl.loop(0, 4)
        def _(r):
            rows = pl.ds(pl.multiple_of(128 * r, 128), 128)
            s = dot_t(q2[rows, :], block)
            s = jnp.where(live, s, NEG)
            sc[cc, rows, :] = s
            high = jnp.maximum(
                jnp.maximum(s[:, :128], s[:, 128:256]), jnp.maximum(s[:, 256:384], s[:, 384:])
            )
            st[rows, :] = high if opening else jnp.maximum(st[rows, :], high)

    step2(5)
    score(c, True)
    score(cz)
    score(cm)
    step3(5)
    step2(6)
    score(cp)
    score(cmz)
    score(cpz)
    step4(5)
    score(co)
    score(coz)
    step3(6)
    step2(2)
    step2(3)

    @pl.loop(0, 16)
    def _(r):
        rows = pl.ds(pl.multiple_of(32 * r, 32), 32)
        top = jnp.max(st[rows, :], axis=1, keepdims=True)
        total = jnp.zeros((32, 512), F32)
        for cc in range(CAND):
            w = jnp.exp(sc[cc, rows, :] - top)
            total = total + w
            pb[rows, pl.ds(512 * cc, 512)] = w.astype(BF)
        st[rows, :] = jnp.broadcast_to(jnp.sum(total, axis=1, keepdims=True), (32, 128))

    both(1)
    step4(6)

    def y_rows(dy):
        return pl.ds(pl.multiple_of(64 * lax.rem(y + dy, NY), 64), 64)

    def z_rows(dz):
        return pl.ds(pl.multiple_of(16 * lax.rem(z + dz, NZ), 16), 16)

    def yz_rows(dy, dz):
        at_row = 64 * lax.rem(y + dy, NY) + 16 * lax.rem(z + dz, NZ)
        return pl.ds(pl.multiple_of(at_row, 16), 16)

    order = (2, 1, 3, 0)

    def sums_send(p):
        for dz in order:
            for dy in (2, 1, 3):
                n = 4 * (dy - 1) + dz
                send(
                    part.at[p, :, yz_rows(dy, dz), :], ry.at[p, dy - 1, :, z_rows(dz), :],
                    rs_send.at[p, n], rs_recv.at[p, n], tok_of(y + dy, z), c,
                )

    def sums_end(p, mid, tail):
        for dz in order:
            zr = z_rows(dz)
            total = part[p, :, yz_rows(0, dz), :].astype(F32)
            for dy in (1, 3, 2):
                landed(ry.at[p, dy - 1, :, zr, :], rs_recv.at[p, 4 * (dy - 1) + dz])
                total = total + ry[p, dy - 1, :, zr, :].astype(F32)
            by[p, :, zr, :] = total.astype(BF)
            if dz:
                send(
                    by.at[p, :, zr, :], rz.at[p, dz - 1], rs_send.at[p, 11 + dz],
                    rs_recv.at[p, 11 + dz], tok_of(y, z + dz), c,
                )
            if dz == 2:
                mid()
        tail()
        total = by[p, :, z_rows(0), :].astype(F32)
        for dz in (1, 3, 2):
            landed(rz.at[p, dz - 1], rs_recv.at[p, 11 + dz])
            total = total + rz[p, dz - 1].astype(F32)
        return jnp.concatenate([total[0], total[1]], axis=1)

    def spread(p, value, work, early, late):
        nf[p, 0, yz_rows(0, 0), :] = value[:, :HALF]
        nf[p, 1, yz_rows(0, 0), :] = value[:, HALF:]

        def go(n, rows, tok):
            where = nf.at[p, :, rows, :]
            send(where, where, ag_send.at[p, n], ag_recv.at[p, n], tok, c)

        def along_y(dz):
            for dy in (2, 1, 3):
                go(4 * (dy - 1) + dz, yz_rows(0, dz), tok_of(y + dy, z))

        for dz in (2, 1, 3):
            go(11 + dz, yz_rows(0, 0), tok_of(y, z + dz))
        along_y(0)
        early()
        for dz in (1, 3, 2):
            landed(nf.at[p, :, yz_rows(0, 4 - dz), :], ag_recv.at[p, 11 + dz])
            along_y(4 - dz)
        late()
        work((0,))
        for dz in (0, 3, 1, 2):
            for dy in (1, 3, 2):
                landed(nf.at[p, :, yz_rows(4 - dy, dz), :], ag_recv.at[p, 4 * (dy - 1) + dz])
        work((2, 1, 3))

    def blocks(p, cc, dys):
        pieces = [nf[p, cc // 4, y_rows(dy), pl.ds(256 * (cc % 4), 256)] for dy in dys]
        return pieces[0] if len(pieces) == 1 else jnp.concatenate(pieces, axis=0)

    def attend(dy):
        low = y_rows(dy)
        upp = pl.ds(pl.multiple_of(64 * lax.rem(y + dy, NY) + ROWS, 64), 64)
        a = jnp.dot(pb[low, :], vb[...], preferred_element_type=F32) / st[low, :]
        b = jnp.dot(pb[upp, :], vb[...], preferred_element_type=F32) / st[upp, :]
        lane = lax.broadcasted_iota(jnp.int32, (64, 128), 1)
        heads = jnp.where(lane < 64, a, b).astype(BF)
        for cc in range(CAND):
            part[0, cc // 4, low, pl.ds(256 * (cc % 4), 256)] = jnp.dot(
                heads, wo[cc], preferred_element_type=F32
            ).astype(BF)

    attend(2)
    attend(1)
    attend(3)
    sums_send(0)
    attend(0)

    def mid_0():
        step3(2)
        step3(3)
        step1x(4)
        step2a(4)

    mine = xv[2 * y + lax.div(z, 2), pl.ds(pl.multiple_of(16 * lax.rem(z, 2), 16), 16), :]
    ac[...] = mine.astype(F32) + sums_end(0, mid_0, lambda: None)

    def feed(dys):
        gate = up = jnp.zeros((64 * len(dys), 320), F32)
        for cc in range(CAND):
            block = blocks(0, cc, dys)
            gate = gate + dot_t(block, wi[0, cc])
            up = up + dot_t(block, wi[1, cc])
        hidden = (gelu(gate) * up).astype(BF)
        for cc in range(CAND):
            down = jnp.dot(hidden, fo[cc], preferred_element_type=F32).astype(BF)
            for n, dy in enumerate(dys):
                part[1, cc // 4, y_rows(dy), pl.ds(256 * (cc % 4), 256)] = down[
                    64 * n : 64 * n + 64
                ]
        if len(dys) > 1:
            sums_send(1)

    def early_0():
        step4(2)
        step4(3)

    def late_0():
        both(2)
        both(3)
        step2b(4)

    spread(0, rms(ac[...], gain2[...]).astype(BF), feed, early_0, late_0)
    def mid_1():
        step3(4)
        across((c, cz, cm, cp))

    after = ac[...] + sums_end(1, mid_1, lambda: step4(4))

    ids = gold[k].astype(F32)
    eye = lax.broadcasted_iota(jnp.int32, (32, 32), 0) == lax.broadcasted_iota(jnp.int32, (32, 32), 1)
    start = [((2 * j + h) * width).astype(F32) for h in range(2)]

    def gold_rows():
        for i in range(8):
            column = jnp.sum(
                jnp.where(eye, jnp.broadcast_to(ids[i : i + 1, :], (32, 32)), 0.0),
                axis=1, keepdims=True,
            )
            st[pl.ds(32 * i, 32), :] = jnp.broadcast_to(column, (32, 128))

    def vocab(dys):
        size = 64 * len(dys)
        wanted = [st[y_rows(dy), :][:, :1] for dy in dys]
        wanted = wanted[0] if len(dys) == 1 else jnp.concatenate(wanted, axis=0)
        logits = []
        for h in range(2):
            one = jnp.zeros((size, width), F32)
            for cc in range(CAND):
                one = one + dot_t(blocks(1, cc, dys), wv[h, cc])
            logits.append(one)
        high = jnp.maximum(
            jnp.max(logits[0], axis=1, keepdims=True), jnp.max(logits[1], axis=1, keepdims=True)
        )
        total = jnp.zeros((size, 1), F32)
        picked = jnp.zeros((size, 1), F32)
        for h in range(2):
            total = total + jnp.sum(jnp.exp(logits[h] - high), axis=1, keepdims=True)
            at_col = lax.broadcasted_iota(jnp.int32, (size, width), 1).astype(F32) + start[h]
            picked = picked + jnp.sum(
                jnp.where(at_col == wanted, logits[h], 0.0), axis=1, keepdims=True
            )
        lane = lax.broadcasted_iota(jnp.int32, (size, 128), 1)
        found = jnp.where(lane == 0, high, jnp.where(lane == 1, total, picked))
        for n, dy in enumerate(dys):
            at_row = 256 + 64 * lax.rem(y + dy, NY)
            st[pl.ds(pl.multiple_of(at_row, 64), 64), :] = found[64 * n : 64 * n + 64]

    def early_1():
        gold_rows()

    spread(1, rms(after, gain3[...]).astype(BF), vocab, early_1, lambda: both(4))

    stats = st[pl.ds(256, 256), :].T
    f1[j] = stats[0:8, :]

    @pl.loop(1, 16)
    def _(d):
        to = lax.rem(j + d, 16) * 2 + k
        send(f1.at[j], f1.at[j], f_send.at[0], f_recv.at[0], to, c)

    landed(f1.at[pl.ds(0, 15)], f_recv.at[0])
    top = f1[0][0:1, :]
    for n in range(1, 16):
        top = jnp.maximum(top, f1[n][0:1, :])
    total = jnp.zeros((1, ROWS), F32)
    picked = jnp.zeros((1, ROWS), F32)
    for n in range(16):
        total = total + f1[n][1:2, :] * jnp.exp(f1[n][0:1, :] - top)
        picked = picked + f1[n][2:3, :]
    logprob = picked - top - jnp.log(total)
    group = lax.div(lax.broadcasted_iota(jnp.int32, (8, ROWS), 1), 32)
    whose = lax.broadcasted_iota(jnp.int32, (8, ROWS), 0)
    per = jnp.sum(jnp.where(group == whose, logprob, 0.0), axis=1, keepdims=True) * (1.0 / 32)
    diag = lax.broadcasted_iota(jnp.int32, (8, 128), 0) == lax.broadcasted_iota(jnp.int32, (8, 128), 1)
    row = jnp.sum(jnp.where(diag, per, 0.0), axis=0, keepdims=True)
    f2[8 * k + c] = jnp.broadcast_to(row, (8, 128))

    @pl.loop(1, CAND)
    def _(d):
        to = lax.rem(c + d, CAND)
        send(f2.at[8 * k + c], f2.at[8 * k + c], f_send.at[1], f_recv.at[1], t, to)
        send(f2.at[8 * k + c], f2.at[8 * k + c], f_send.at[1], f_recv.at[1], partner, to)

    send(f2.at[8 * k + c], f2.at[8 * k + c], f_send.at[1], f_recv.at[1], partner, c)
    landed(f2.at[pl.ds(0, 15)], f_recv.at[1])
    lane = lax.broadcasted_iota(jnp.int32, (8, 8, 128), 2)
    cand = lax.broadcasted_iota(jnp.int32, (8, 8, 128), 0) * 8 + lane
    for b in range(2):
        count = counts[b]
        inside = jnp.where((cand < count) & (lane < 8), f2[pl.ds(8 * b, 8)], NEG)
        best_out[b] = jnp.max(inside)
        own_lane = lax.broadcasted_iota(jnp.int32, (1, 128), 1)
        own = f2[8 * b + c][0:1, :]
        scores_out[pl.ds(b, 1), :] = jnp.where(own_lane + 8 * c < count, own, 0.0)[:, :8]

    for n in range(2):
        landed(kb.at[pl.ds(0, 496), :], kv_send.at[n])
    for n in range(7):
        at_ = places[n]
        for slot in range(9):
            landed(at_(c) if slot < 5 else at_(c, (slot - 5) % 2), g_send.at[n, slot])
        if n < 5:
            landed(whole[n](k), g_dsend.at[n])
    @pl.loop(0, 2)
    def _(p):
        @pl.loop(0, 15)
        def _(n):
            landed(rz.at[p, 0], rs_send.at[p, n])
            landed(rz.at[p, 0], ag_send.at[p, n])

    landed(f1.at[pl.ds(0, 15)], f_send.at[0])
    landed(f2.at[pl.ds(0, 15)], f_send.at[1])


def body(
    dec_hidden, enc_keys, enc_values, enc_lengths, cand_counts, gold_ids, gain_cross, w_query,
    w_out, gain_ffn, w_in_gate, w_in_up, w_ffn_out, gain_final, w_vocab,
):
    units = w_in_gate.shape[1]
    width = w_vocab.shape[1]
    anywhere = pl.BlockSpec(memory_space=pl.ANY)
    vmem = pl.BlockSpec(memory_space=pltpu.VMEM)
    smem = pl.BlockSpec(memory_space=pltpu.SMEM)
    dma = pltpu.SemaphoreType.DMA
    return pl.pallas_call(
        kernel,
        name="layer",
        out_shape=(
            jax.ShapeDtypeStruct((2, 8), F32),
            jax.ShapeDtypeStruct((2,), F32),
        ),
        in_specs=[
            anywhere, anywhere, anywhere, smem, smem, vmem, vmem, anywhere, anywhere, vmem,
            anywhere, anywhere, anywhere, vmem, anywhere,
        ],
        out_specs=(vmem, smem),
        scratch_shapes=[
            pltpu.VMEM((8, 32, D), BF),
            pltpu.VMEM((ROWS, D), BF),
            pltpu.VMEM((2 * ROWS, 128), BF),
            pltpu.VMEM((4096, 128), BF),
            pltpu.VMEM((4096, 128), BF),
            pltpu.VMEM((8, 2 * ROWS, 512), F32),
            pltpu.VMEM((2 * ROWS, 4096), BF),
            pltpu.VMEM((8, 128, 256), BF),
            pltpu.VMEM((8, 128, 256), BF),
            pltpu.VMEM((2, 8, 2 * units, 256), BF),
            pltpu.VMEM((8, 2 * units, 256), BF),
            pltpu.VMEM((2, 8, width, 256), BF),
            pltpu.VMEM((2, 2, ROWS, HALF), BF),
            pltpu.VMEM((2, 3, 2, 64, HALF), BF),
            pltpu.VMEM((2, 2, 64, HALF), BF),
            pltpu.VMEM((2, 3, 2, 16, HALF), BF),
            pltpu.VMEM((16, D), F32),
            pltpu.VMEM((2, 2, ROWS, HALF), BF),
            pltpu.VMEM((2 * ROWS, 128), F32),
            pltpu.VMEM((16, 8, ROWS), F32),
            pltpu.VMEM((16, 8, 128), F32),
            dma((2,)), dma((2,)), dma((7, 9)), dma((7, 9)), dma((5,)), dma((5,)), dma((5,)),
            dma((2, 15)), dma((2, 15)), dma((2, 15)), dma((2, 15)), dma((2,)), dma((2,)), dma((3,)),
        ],
        compiler_params=pltpu.CompilerParams(
            collective_id=0, has_side_effects=True, vmem_limit_bytes=62 * 1024 * 1024
        ),
    )(
        dec_hidden, enc_keys, enc_values, enc_lengths, cand_counts, gold_ids,
        gain_cross.reshape(1, -1), w_query.T, w_out, gain_ffn.reshape(1, -1), w_in_gate.T, w_in_up.T,
        w_ffn_out,
        gain_final.reshape(1, -1), w_vocab.T,
    )


def solution(mesh):
    in_specs = (
        P(None, "cand", None, None), P(None, "tok", None), P(None, "tok", None), P(), P(),
        P(None, "cand", None), P(), P("cand", "tok"), P("tok", "cand"), P(), P("cand", "tok"),
        P("cand", "tok"), P("tok", "cand"), P(), P("cand", "tok"),
    )
    return jax.shard_map(
        body, mesh=mesh, in_specs=in_specs, out_specs=(P(None, "cand"), P()), check_vma=False
    )
```

```python
import functools

import jax
import jax.numpy as jnp
from jax import lax
from jax.experimental import pallas as pl
from jax.experimental.pallas import tpu as pltpu
from jax.sharding import PartitionSpec as P

MESH = pl.DeviceIdType.MESH
EPS = 0.25
NY, NZ, NX = 4, 4, 4
TOK, CAND = 32, 8
D = 2048
HALF = 1024
ROWS = 256
NEG = -1e30
BF = jnp.bfloat16
F32 = jnp.float32


def rms(v, gain):
    squares = jnp.mean(v * v, axis=-1, keepdims=True)
    return v * lax.rsqrt(squares + EPS) * gain


def gelu(v):
    inner = 0.7978845608028654 * (v + 0.044715 * (v * v * v))
    return 0.5 * v * (1.0 + jnp.tanh(inner))


def dot_t(a, b):
    return lax.dot_general(a, b, (((1,), (1,)), ((), ())), preferred_element_type=F32)


def landed(ref, sem):
    pltpu.make_async_copy(ref, ref, sem).wait()


def kernel(
    x_in, keys, vals, lens, counts, gold, gain1, wq_in, wo_in, gain2, wg_in, wu_in, fo_in, gain3, wv_in,
    out,
    xv, nx, q2, kb, vb, sc, pb,
    wq, wo, wi, fo, wv,
    part, ry, by, rz, ac, nf,
    st, f1, f2,
    kv_recv, kv_send, g_recv, g_send, g_own, g_dual, g_dsend,
    rs_recv, rs_send, ag_recv, ag_send, f_recv, f_send, l_sem,
):
    t = lax.axis_index("tok")
    c = lax.axis_index("cand")
    k = lax.rem(t, 2)
    j = lax.div(t, 2)
    y = lax.div(j, NZ)
    z = lax.rem(j, NZ)
    xx = lax.div(c, 2)
    zl = lax.rem(c, 2)

    def tok_of(yy, zz):
        return (lax.rem(yy, NY) * NZ + lax.rem(zz, NZ)) * 2 + k

    def cand_of(x_at, z_at):
        return lax.rem(x_at, NX) * 2 + z_at

    partner = t + 1 - 2 * k
    cz = cand_of(xx, 1 - zl)
    cp, cm = cand_of(xx + 1, zl), cand_of(xx + 3, zl)
    cpz, cmz = cand_of(xx + 1, 1 - zl), cand_of(xx + 3, 1 - zl)
    co, coz = cand_of(xx + 2, zl), cand_of(xx + 2, 1 - zl)

    def send(src, dst, s_sem, r_sem, tok, cand):
        pltpu.make_async_remote_copy(
            src_ref=src, dst_ref=dst, send_sem=s_sem, recv_sem=r_sem,
            device_id=(tok, cand), device_id_type=MESH,
        ).start()

    x_copy = pltpu.make_async_copy(x_in.at[k], xv, l_sem.at[0])
    x_copy.start()

    barrier = pltpu.get_barrier_semaphore()

    @pl.loop(1, TOK)
    def _(d):
        pl.semaphore_signal(
            barrier, inc=1, device_id=(lax.rem(t + d, TOK), c), device_id_type=MESH
        )

    @pl.loop(1, CAND)
    def _(d):
        pl.semaphore_signal(
            barrier, inc=1, device_id=(t, lax.rem(c + d, CAND)), device_id_type=MESH
        )
        pl.semaphore_signal(
            barrier, inc=1, device_id=(partner, lax.rem(c + d, CAND)), device_id_type=MESH
        )

    def stacked(ref, size):
        def at_(cc, part=None):
            if part is None:
                return ref.at[cc, pl.ds(size * k, size), :]
            return ref.at[cc, pl.ds(size * k + size // 2 * part, size // 2), :]
        return at_

    def i_at(cc, part=None):
        if part is None:
            return wi.at[:, cc, pl.ds(160 * k, 160), :]
        return wi.at[:, cc, pl.ds(160 * k + 80 * part, 80), :]

    width = wv.shape[2]

    def v_at(cc, part=None):
        if part is None:
            return wv.at[k, cc]
        return wv.at[k, cc, pl.ds(0, 512), :] if part == 0 else wv.at[k, cc, pl.ds(512, width - 512), :]

    def kv_at(ref):
        def at_(cc, part=None):
            if part is None:
                return ref.at[pl.ds(512 * cc, 512), :]
            return ref.at[pl.ds(512 * cc + 256 * part, 256), :]
        return at_

    places = [stacked(wq, 64), stacked(wo, 64), i_at, stacked(fo, 160), v_at, kv_at(kb), kv_at(vb)]
    whole = [
        lambda h: wq.at[:, pl.ds(64 * h, 64), :], lambda h: wo.at[:, pl.ds(64 * h, 64), :],
        lambda h: wi.at[:, :, pl.ds(160 * h, 160), :], lambda h: fo.at[:, pl.ds(160 * h, 160), :],
        lambda h: wv.at[h],
    ]

    def own_copies():
        for n, src in ((0, wq_in), (1, wo_in), (3, fo_in), (4, wv_in)):
            pltpu.make_async_copy(src, places[n](c), g_own.at[n]).start()
        for m, src in enumerate((wg_in, wu_in)):
            pltpu.make_async_copy(
                src, wi.at[m, c, pl.ds(160 * k, 160), :], g_own.at[2]
            ).start()

    def g_send_to(n, slot, src, dst, cand):
        send(src, dst, g_send.at[n, slot], g_recv.at[n, slot], t, cand)

    def ready(n):
        landed(places[n](c), g_own.at[n])

    def step1z(n):
        here = places[n](c)
        g_send_to(n, 0, here, here, cz)

    def step1x(n):
        here = places[n](c)
        g_send_to(n, 1, here, here, cp)
        g_send_to(n, 2, here, here, cm)

    def step1(n):
        step1z(n)
        step1x(n)

    def step2a(n):
        at_ = places[n]
        landed(at_(cz), g_recv.at[n, 0])
        g_send_to(n, 3, at_(cz), at_(cz), cp)
        g_send_to(n, 4, at_(cz), at_(cz), cm)

    def step2b(n):
        at_ = places[n]
        landed(at_(cm), g_recv.at[n, 1])
        g_send_to(n, 5, at_(cm, 0), at_(cm, 0), cp)
        landed(at_(cp), g_recv.at[n, 2])
        g_send_to(n, 6, at_(cp, 1), at_(cp, 1), cm)

    def step2(n):
        step2a(n)
        step2b(n)

    def step3(n):
        at_ = places[n]
        landed(at_(cmz), g_recv.at[n, 3])
        g_send_to(n, 7, at_(cmz, 0), at_(cmz, 0), cp)
        landed(at_(cpz), g_recv.at[n, 4])
        g_send_to(n, 8, at_(cpz, 1), at_(cpz, 1), cm)

    def across(which):
        for cc in which:
            send(v_at(cc), v_at(cc), g_dsend.at[4], g_dual.at[4], partner, c)

    def step4(n):
        at_ = places[n]
        landed(at_(co, 0), g_recv.at[n, 5])
        landed(at_(co, 1), g_recv.at[n, 6])
        landed(at_(coz, 0), g_recv.at[n, 7])
        landed(at_(coz, 1), g_recv.at[n, 8])
        if n < 5:
            if n < 4:
                send(whole[n](k), whole[n](k), g_dsend.at[n], g_dual.at[n], partner, c)
            else:
                across((cmz, cpz, co, coz))

    def both(n):
        landed(whole[n](1 - k), g_dual.at[n])


    own_copies()

    x_copy.wait()

    @pl.loop(0, 8)
    def _(i):
        rows = xv[i].astype(F32)
        nx[pl.ds(pl.multiple_of(32 * i, 32), 32), :] = rms(rows, gain1[...]).astype(BF)

    pl.semaphore_wait(barrier, TOK - 1 + 2 * (CAND - 1))

    ready(0)
    ready(1)
    step1(0)
    step1(1)

    for n, (src, dst) in enumerate(((keys, kb), (vals, vb))):
        here = dst.at[pl.ds(512 * c + 16 * t, 16), :]
        pltpu.make_async_copy(
            src.at[k, pl.ds(16 * c, 16), pl.ds(pl.multiple_of(128 * j, 128), 128)],
            here, l_sem.at[1 + n],
        ).start()

        @pl.loop(1, TOK)
        def _(d, src=src, n=n, here=here):
            to = lax.rem(t + d, TOK)
            send(
                src.at[
                    lax.rem(to, 2), pl.ds(16 * c, 16),
                    pl.ds(pl.multiple_of(128 * lax.div(to, 2), 128), 128),
                ],
                here, kv_send.at[n], kv_recv.at[n], to, c,
            )

    def value_far():
        for n, cc in enumerate((co, coz)):
            here = vb.at[pl.ds(512 * cc + 16 * t, 16), :]
            pltpu.make_async_copy(
                vals.at[k, pl.ds(16 * cc, 16), pl.ds(pl.multiple_of(128 * j, 128), 128)],
                here, l_sem.at[3 + n],
            ).start()

            @pl.loop(1, TOK)
            def _(d, here=here, cc=cc):
                to = lax.rem(t + d, TOK)
                send(
                    vals.at[
                        lax.rem(to, 2), pl.ds(16 * cc, 16),
                        pl.ds(pl.multiple_of(128 * lax.div(to, 2), 128), 128),
                    ],
                    here, kv_send.at[2], kv_recv.at[2], to, c,
                )

    def value_end():
        for n, cc in enumerate((co, coz)):
            pltpu.make_async_copy(
                vb.at[pl.ds(0, 16), :], vb.at[pl.ds(512 * cc + 16 * t, 16), :], l_sem.at[3 + n]
            ).wait()
        landed(vb.at[pl.ds(0, 992), :], kv_recv.at[2])
        at_ = places[6]
        for slot, came in ((1, cm), (2, cp), (3, cmz), (4, cpz)):
            landed(at_(came), g_recv.at[6, slot])

    def kv_mine(n):
        ref = (kb, vb)[n]
        pltpu.make_async_copy(
            ref.at[pl.ds(0, 16), :], ref.at[pl.ds(512 * c + 16 * t, 16), :], l_sem.at[1 + n]
        ).wait()
        landed(ref.at[pl.ds(0, 496), :], kv_recv.at[n])

    ready(2)
    ready(3)
    step1(2)
    step1(3)
    step2(0)
    step2(1)
    step3(0)
    step3(1)
    kv_mine(0)
    step1(5)
    kv_mine(1)
    step1(6)
    value_far()
    ready(4)
    step1z(4)
    step4(0)
    step4(1)
    both(0)
    zero = jnp.zeros((ROWS, 64), BF)
    query = jnp.zeros((ROWS, 128), F32)
    for cc in range(CAND):
        query = query + dot_t(nx[:, 256 * cc : 256 * cc + 256], wq[cc])
    query = query.astype(BF)
    q2[pl.ds(0, ROWS), :] = jnp.concatenate([query[:, :64], zero], axis=1)
    q2[pl.ds(ROWS, ROWS), :] = jnp.concatenate([zero, query[:, 64:]], axis=1)

    length = lens[k]

    def score(cc, opening=False):
        place = lax.broadcasted_iota(jnp.int32, (1, 512), 1)
        token = lax.div(place, 16) * 128 + 16 * cc + lax.rem(place, 16)
        live = token < length
        block = kb[pl.ds(pl.multiple_of(512 * cc, 512), 512), :]

        for r in range(4):
            rows = pl.ds(128 * r, 128)
            s = dot_t(q2[rows, :], block)
            s = jnp.where(live, s, NEG)
            sc[cc, rows, :] = s
            high = jnp.maximum(
                jnp.maximum(s[:, :128], s[:, 128:256]), jnp.maximum(s[:, 256:384], s[:, 384:])
            )
            st[rows, :] = high if opening else jnp.maximum(st[rows, :], high)

    step2(5)
    score(c, True)
    score(cz)
    score(cm)
    step3(5)
    step2a(6)
    score(cp)
    score(cmz)
    score(cpz)
    step4(5)
    score(co)
    score(coz)
    step2(2)
    step2(3)

    for r in range(8):
        rows = pl.ds(64 * r, 64)
        top = jnp.max(st[rows, :], axis=1, keepdims=True)
        total = jnp.zeros((64, 256), F32)
        for at in range(16):
            w = jnp.exp(sc[at // 2, rows, pl.ds(256 * (at % 2), 256)] - top)
            total = total + w
            pb[rows, pl.ds(256 * at, 256)] = w.astype(BF)
        st[rows, :] = jnp.broadcast_to(jnp.sum(total, axis=1, keepdims=True), (64, 128))

    both(1)
    value_end()

    def y_rows(dy):
        return pl.ds(pl.multiple_of(64 * lax.rem(y + dy, NY), 64), 64)

    def z_rows(dz):
        return pl.ds(pl.multiple_of(16 * lax.rem(z + dz, NZ), 16), 16)

    def yz_rows(dy, dz):
        at_row = 64 * lax.rem(y + dy, NY) + 16 * lax.rem(z + dz, NZ)
        return pl.ds(pl.multiple_of(at_row, 16), 16)

    order = (2, 1, 3, 0)

    def sums_send(p):
        for dz in order:
            for dy in (2, 1, 3):
                n = 4 * (dy - 1) + dz
                send(
                    part.at[p, :, yz_rows(dy, dz), :], ry.at[p, dy - 1, :, z_rows(dz), :],
                    rs_send.at[p, n], rs_recv.at[p, n], tok_of(y + dy, z), c,
                )

    def sums_end(p, mid, tail):
        for dz in order:
            zr = z_rows(dz)
            total = part[p, :, yz_rows(0, dz), :].astype(F32)
            for dy in (1, 3, 2):
                landed(ry.at[p, dy - 1, :, zr, :], rs_recv.at[p, 4 * (dy - 1) + dz])
                total = total + ry[p, dy - 1, :, zr, :].astype(F32)
            by[p, :, zr, :] = total.astype(BF)
            if dz:
                send(
                    by.at[p, :, zr, :], rz.at[p, dz - 1], rs_send.at[p, 11 + dz],
                    rs_recv.at[p, 11 + dz], tok_of(y, z + dz), c,
                )
            if dz == 2:
                mid()
        tail()
        total = by[p, :, z_rows(0), :].astype(F32)
        for dz in (1, 3, 2):
            landed(rz.at[p, dz - 1], rs_recv.at[p, 11 + dz])
            total = total + rz[p, dz - 1].astype(F32)
        return jnp.concatenate([total[0], total[1]], axis=1)

    def spread(p, value, work, early, late):
        nf[p, 0, yz_rows(0, 0), :] = value[:, :HALF]
        nf[p, 1, yz_rows(0, 0), :] = value[:, HALF:]

        def go(n, rows, tok):
            where = nf.at[p, :, rows, :]
            send(where, where, ag_send.at[p, n], ag_recv.at[p, n], tok, c)

        def along_y(dz):
            for dy in (2, 1, 3):
                go(4 * (dy - 1) + dz, yz_rows(0, dz), tok_of(y + dy, z))

        for dz in (2, 1, 3):
            go(11 + dz, yz_rows(0, 0), tok_of(y, z + dz))
        along_y(0)
        early()
        for dz in (1, 3, 2):
            landed(nf.at[p, :, yz_rows(0, 4 - dz), :], ag_recv.at[p, 11 + dz])
            along_y(4 - dz)
        late()
        work((0,))
        for dz in (0, 3, 1, 2):
            for dy in (1, 3, 2):
                landed(nf.at[p, :, yz_rows(4 - dy, dz), :], ag_recv.at[p, 4 * (dy - 1) + dz])
        work((2, 1, 3))

    def blocks(p, cc, dys):
        pieces = [nf[p, cc // 4, y_rows(dy), pl.ds(256 * (cc % 4), 256)] for dy in dys]
        return pieces[0] if len(pieces) == 1 else jnp.concatenate(pieces, axis=0)

    halves = [
        jnp.dot(pb[pl.ds(ROWS * h, ROWS), :], vb[...], preferred_element_type=F32)
        / st[pl.ds(ROWS * h, ROWS), :]
        for h in range(2)
    ]
    lane = lax.broadcasted_iota(jnp.int32, (ROWS, 128), 1)
    attended = jnp.where(lane < 64, halves[0], halves[1]).astype(BF)
    for cc in range(CAND):
        part[0, cc // 4, :, pl.ds(256 * (cc % 4), 256)] = jnp.dot(
            attended, wo[cc], preferred_element_type=F32
        ).astype(BF)
    sums_send(0)

    def mid_0():
        step3(2)
        step3(3)
        step1x(4)
        step2a(4)

    mine = xv[2 * y + lax.div(z, 2), pl.ds(pl.multiple_of(16 * lax.rem(z, 2), 16), 16), :]
    ac[...] = mine.astype(F32) + sums_end(0, mid_0, lambda: None)

    def feed(dys):
        gate = up = jnp.zeros((64 * len(dys), 320), F32)
        for cc in range(CAND):
            block = blocks(0, cc, dys)
            gate = gate + dot_t(block, wi[0, cc])
            up = up + dot_t(block, wi[1, cc])
        hidden = (gelu(gate) * up).astype(BF)
        for cc in range(CAND):
            down = jnp.dot(hidden, fo[cc], preferred_element_type=F32).astype(BF)
            for n, dy in enumerate(dys):
                part[1, cc // 4, y_rows(dy), pl.ds(256 * (cc % 4), 256)] = down[
                    64 * n : 64 * n + 64
                ]
        if len(dys) > 1:
            sums_send(1)

    def early_0():
        step4(2)
        step4(3)

    def late_0():
        both(2)
        both(3)
        step2b(4)

    spread(0, rms(ac[...], gain2[...]).astype(BF), feed, early_0, late_0)
    def mid_1():
        step3(4)
        across((c, cz, cm, cp))

    after = ac[...] + sums_end(1, mid_1, lambda: step4(4))

    ids = gold[k].astype(F32)
    eye = lax.broadcasted_iota(jnp.int32, (32, 32), 0) == lax.broadcasted_iota(jnp.int32, (32, 32), 1)
    start = [((2 * j + h) * width).astype(F32) for h in range(2)]

    def gold_rows():
        for i in range(8):
            column = jnp.sum(
                jnp.where(eye, jnp.broadcast_to(ids[i : i + 1, :], (32, 32)), 0.0),
                axis=1, keepdims=True,
            )
            st[pl.ds(32 * i, 32), :] = jnp.broadcast_to(column, (32, 128))

    def vocab(dys):
        size = 64 * len(dys)
        wanted = [st[y_rows(dy), :][:, :1] for dy in dys]
        wanted = wanted[0] if len(dys) == 1 else jnp.concatenate(wanted, axis=0)
        logits = []
        for h in range(2):
            one = jnp.zeros((size, width), F32)
            for cc in range(CAND):
                one = one + dot_t(blocks(1, cc, dys), wv[h, cc])
            logits.append(one)
        high = jnp.maximum(
            jnp.max(logits[0], axis=1, keepdims=True), jnp.max(logits[1], axis=1, keepdims=True)
        )
        total = jnp.zeros((size, 1), F32)
        picked = jnp.zeros((size, 1), F32)
        for h in range(2):
            total = total + jnp.sum(jnp.exp(logits[h] - high), axis=1, keepdims=True)
            at_col = lax.broadcasted_iota(jnp.int32, (size, width), 1).astype(F32) + start[h]
            picked = picked + jnp.sum(
                jnp.where(at_col == wanted, logits[h], 0.0), axis=1, keepdims=True
            )
        lane = lax.broadcasted_iota(jnp.int32, (size, 128), 1)
        found = jnp.where(lane == 0, high, jnp.where(lane == 1, total, picked))
        for n, dy in enumerate(dys):
            at_row = 256 + 64 * lax.rem(y + dy, NY)
            st[pl.ds(pl.multiple_of(at_row, 64), 64), :] = found[64 * n : 64 * n + 64]

    def early_1():
        gold_rows()

    spread(1, rms(after, gain3[...]).astype(BF), vocab, early_1, lambda: both(4))

    stats = st[pl.ds(256, 256), :].T
    f1[j] = stats[0:8, :]

    @pl.loop(1, 16)
    def _(d):
        to = lax.rem(j + d, 16) * 2 + k
        send(f1.at[j], f1.at[j], f_send.at[0], f_recv.at[0], to, c)

    landed(f1.at[pl.ds(0, 15)], f_recv.at[0])
    top = f1[0][0:1, :]
    for n in range(1, 16):
        top = jnp.maximum(top, f1[n][0:1, :])
    total = jnp.zeros((1, ROWS), F32)
    picked = jnp.zeros((1, ROWS), F32)
    for n in range(16):
        total = total + f1[n][1:2, :] * jnp.exp(f1[n][0:1, :] - top)
        picked = picked + f1[n][2:3, :]
    logprob = picked - top - jnp.log(total)
    group = lax.div(lax.broadcasted_iota(jnp.int32, (8, ROWS), 1), 32)
    whose = lax.broadcasted_iota(jnp.int32, (8, ROWS), 0)
    per = jnp.sum(jnp.where(group == whose, logprob, 0.0), axis=1, keepdims=True) * (1.0 / 32)
    diag = lax.broadcasted_iota(jnp.int32, (8, 128), 0) == lax.broadcasted_iota(jnp.int32, (8, 128), 1)
    row = jnp.sum(jnp.where(diag, per, 0.0), axis=0, keepdims=True)
    f2[8 * k + c] = jnp.broadcast_to(row, (8, 128))

    @pl.loop(1, CAND)
    def _(d):
        to = lax.rem(c + d, CAND)
        send(f2.at[8 * k + c], f2.at[8 * k + c], f_send.at[1], f_recv.at[1], t, to)
        send(f2.at[8 * k + c], f2.at[8 * k + c], f_send.at[1], f_recv.at[1], partner, to)

    send(f2.at[8 * k + c], f2.at[8 * k + c], f_send.at[1], f_recv.at[1], partner, c)
    landed(f2.at[pl.ds(0, 15)], f_recv.at[1])
    lane = lax.broadcasted_iota(jnp.int32, (8, 8, 128), 2)
    cand = lax.broadcasted_iota(jnp.int32, (8, 8, 128), 0) * 8 + lane
    own_lane = lax.broadcasted_iota(jnp.int32, (1, 128), 1)
    for b in range(2):
        count = counts[b]
        inside = jnp.where((cand < count) & (lane < 8), f2[pl.ds(8 * b, 8)], NEG)
        own = jnp.where(own_lane + 8 * c < count, f2[8 * b + c][0:1, :], 0.0)
        out[pl.ds(b, 1), :] = jnp.where(own_lane < 8, own, jnp.max(inside))

    for n in range(2):
        landed(kb.at[pl.ds(0, 496), :], kv_send.at[n])
    landed(kb.at[pl.ds(0, 992), :], kv_send.at[2])
    for n in range(7):
        at_ = places[n]
        for slot in range(5 if n == 6 else 9):
            landed(at_(c) if slot < 5 else at_(c, (slot - 5) % 2), g_send.at[n, slot])
        if n < 5:
            landed(whole[n](k), g_dsend.at[n])
    @pl.loop(0, 2)
    def _(p):
        @pl.loop(0, 15)
        def _(n):
            landed(rz.at[p, 0], rs_send.at[p, n])
            landed(rz.at[p, 0], ag_send.at[p, n])

    landed(f1.at[pl.ds(0, 15)], f_send.at[0])
    landed(f2.at[pl.ds(0, 15)], f_send.at[1])


def body(
    dec_hidden, enc_keys, enc_values, enc_lengths, cand_counts, gold_ids, gain_cross, w_query,
    w_out, gain_ffn, w_in_gate, w_in_up, w_ffn_out, gain_final, w_vocab,
):
    units = w_in_gate.shape[1]
    width = w_vocab.shape[1]
    anywhere = pl.BlockSpec(memory_space=pl.ANY)
    vmem = pl.BlockSpec(memory_space=pltpu.VMEM)
    smem = pl.BlockSpec(memory_space=pltpu.SMEM)
    dma = pltpu.SemaphoreType.DMA
    found = pl.pallas_call(
        kernel,
        name="layer",
        out_shape=jax.ShapeDtypeStruct((2, 128), F32),
        in_specs=[
            anywhere, anywhere, anywhere, smem, smem, vmem, vmem, anywhere, anywhere, vmem,
            anywhere, anywhere, anywhere, vmem, anywhere,
        ],
        out_specs=vmem,
        scratch_shapes=[
            pltpu.VMEM((8, 32, D), BF),
            pltpu.VMEM((ROWS, D), BF),
            pltpu.VMEM((2 * ROWS, 128), BF),
            pltpu.VMEM((4096, 128), BF),
            pltpu.VMEM((4096, 128), BF),
            pltpu.VMEM((8, 2 * ROWS, 512), F32),
            pltpu.VMEM((2 * ROWS, 4096), BF),
            pltpu.VMEM((8, 128, 256), BF),
            pltpu.VMEM((8, 128, 256), BF),
            pltpu.VMEM((2, 8, 2 * units, 256), BF),
            pltpu.VMEM((8, 2 * units, 256), BF),
            pltpu.VMEM((2, 8, width, 256), BF),
            pltpu.VMEM((2, 2, ROWS, HALF), BF),
            pltpu.VMEM((2, 3, 2, 64, HALF), BF),
            pltpu.VMEM((2, 2, 64, HALF), BF),
            pltpu.VMEM((2, 3, 2, 16, HALF), BF),
            pltpu.VMEM((16, D), F32),
            pltpu.VMEM((2, 2, ROWS, HALF), BF),
            pltpu.VMEM((2 * ROWS, 128), F32),
            pltpu.VMEM((16, 8, ROWS), F32),
            pltpu.VMEM((16, 8, 128), F32),
            dma((3,)), dma((3,)), dma((7, 9)), dma((7, 9)), dma((5,)), dma((5,)), dma((5,)),
            dma((2, 15)), dma((2, 15)), dma((2, 15)), dma((2, 15)), dma((2,)), dma((2,)), dma((5,)),
        ],
        compiler_params=pltpu.CompilerParams(
            collective_id=0, has_side_effects=True, vmem_limit_bytes=62 * 1024 * 1024
        ),
    )(
        dec_hidden, enc_keys, enc_values, enc_lengths, cand_counts, gold_ids,
        gain_cross.reshape(1, -1), w_query.T, w_out, gain_ffn.reshape(1, -1), w_in_gate.T, w_in_up.T,
        w_ffn_out,
        gain_final.reshape(1, -1), w_vocab.T,
    )
    return found[:, :8], found[:, 8]


def solution(mesh):
    in_specs = (
        P(None, "cand", None, None), P(None, "tok", None), P(None, "tok", None), P(), P(),
        P(None, "cand", None), P(), P("cand", "tok"), P("tok", "cand"), P(), P("cand", "tok"),
        P("cand", "tok"), P("tok", "cand"), P(), P("cand", "tok"),
    )
    return jax.shard_map(
        body, mesh=mesh, in_specs=in_specs, out_specs=(P(None, "cand"), P()), check_vma=False
    )
```

```python
import functools

import jax
import jax.numpy as jnp
from jax import lax
from jax.experimental import pallas as pl
from jax.experimental.pallas import tpu as pltpu
from jax.sharding import PartitionSpec as P

MESH = pl.DeviceIdType.MESH
EPS = 0.25
NY, NZ, NX = 4, 4, 4
TOK, CAND = 32, 8
D = 2048
HALF = 1024
ROWS = 256
NEG = -1e30
BF = jnp.bfloat16
F32 = jnp.float32


def rms(v, gain):
    squares = jnp.mean(v * v, axis=-1, keepdims=True)
    return v * lax.rsqrt(squares + EPS) * gain


def gelu(v):
    inner = 0.7978845608028654 * (v + 0.044715 * (v * v * v))
    return 0.5 * v * (1.0 + jnp.tanh(inner))


def dot_t(a, b):
    return lax.dot_general(a, b, (((1,), (1,)), ((), ())), preferred_element_type=F32)


def landed(ref, sem):
    pltpu.make_async_copy(ref, ref, sem).wait()


def kernel(
    x_in, keys, vals, lens_in, counts_in, gold_in, gain1_in, wq_in, wo_in, gain2_in, wg_in, wu_in,
    fo_in, gain3_in, wv_in,
    out,
    xv, nx, q2, kb, vb, sc, pb,
    wq, wo, wi, fo, wv,
    part, ry, by, rz, ac, nf,
    st, f1, f2, lens, counts, gold, gain1, gain2, gain3,
    kv_recv, kv_send, g_recv, g_send, g_own, g_dual, g_dsend,
    rs_recv, rs_send, ag_recv, ag_send, f_recv, f_send, l_sem, s_sem,
):
    t = lax.axis_index("tok")
    c = lax.axis_index("cand")
    k = lax.rem(t, 2)
    j = lax.div(t, 2)
    y = lax.div(j, NZ)
    z = lax.rem(j, NZ)
    xx = lax.div(c, 2)
    zl = lax.rem(c, 2)

    def tok_of(yy, zz):
        return (lax.rem(yy, NY) * NZ + lax.rem(zz, NZ)) * 2 + k

    def cand_of(x_at, z_at):
        return lax.rem(x_at, NX) * 2 + z_at

    partner = t + 1 - 2 * k
    cz = cand_of(xx, 1 - zl)
    cp, cm = cand_of(xx + 1, zl), cand_of(xx + 3, zl)
    cpz, cmz = cand_of(xx + 1, 1 - zl), cand_of(xx + 3, 1 - zl)
    co, coz = cand_of(xx + 2, zl), cand_of(xx + 2, 1 - zl)

    def send(src, dst, s_sem, r_sem, tok, cand):
        pltpu.make_async_remote_copy(
            src_ref=src, dst_ref=dst, send_sem=s_sem, recv_sem=r_sem,
            device_id=(tok, cand), device_id_type=MESH,
        ).start()

    x_copy = pltpu.make_async_copy(x_in.at[k], xv, l_sem.at[0])
    x_copy.start()
    small = [
        pltpu.make_async_copy(src, dst, s_sem.at[n])
        for n, (src, dst) in enumerate((
            (gain1_in, gain1), (lens_in, lens), (counts_in, counts), (gold_in, gold),
            (gain2_in, gain2), (gain3_in, gain3),
        ))
    ]
    for copy in small:
        copy.start()

    barrier = pltpu.get_barrier_semaphore()

    @pl.loop(1, TOK)
    def _(d):
        pl.semaphore_signal(
            barrier, inc=1, device_id=(lax.rem(t + d, TOK), c), device_id_type=MESH
        )

    @pl.loop(1, CAND)
    def _(d):
        pl.semaphore_signal(
            barrier, inc=1, device_id=(t, lax.rem(c + d, CAND)), device_id_type=MESH
        )
        pl.semaphore_signal(
            barrier, inc=1, device_id=(partner, lax.rem(c + d, CAND)), device_id_type=MESH
        )

    def stacked(ref, size):
        def at_(cc, part=None):
            if part is None:
                return ref.at[cc, pl.ds(size * k, size), :]
            return ref.at[cc, pl.ds(size * k + size // 2 * part, size // 2), :]
        return at_

    def i_at(cc, part=None):
        if part is None:
            return wi.at[:, cc, pl.ds(160 * k, 160), :]
        return wi.at[:, cc, pl.ds(160 * k + 80 * part, 80), :]

    width = wv.shape[2]

    def v_at(cc, part=None):
        if part is None:
            return wv.at[k, cc]
        return wv.at[k, cc, pl.ds(0, 512), :] if part == 0 else wv.at[k, cc, pl.ds(512, width - 512), :]

    def kv_at(ref):
        def at_(cc, part=None):
            if part is None:
                return ref.at[pl.ds(512 * cc, 512), :]
            return ref.at[pl.ds(512 * cc + 256 * part, 256), :]
        return at_

    places = [stacked(wq, 64), stacked(wo, 64), i_at, stacked(fo, 160), v_at, kv_at(kb), kv_at(vb)]
    whole = [
        lambda h: wq.at[:, pl.ds(64 * h, 64), :], lambda h: wo.at[:, pl.ds(64 * h, 64), :],
        lambda h: wi.at[:, :, pl.ds(160 * h, 160), :], lambda h: fo.at[:, pl.ds(160 * h, 160), :],
        lambda h: wv.at[h],
    ]

    def own_copies():
        for n, src in ((0, wq_in), (1, wo_in), (3, fo_in), (4, wv_in)):
            pltpu.make_async_copy(src, places[n](c), g_own.at[n]).start()
        for m, src in enumerate((wg_in, wu_in)):
            pltpu.make_async_copy(
                src, wi.at[m, c, pl.ds(160 * k, 160), :], g_own.at[2]
            ).start()

    def g_send_to(n, slot, src, dst, cand):
        send(src, dst, g_send.at[n, slot], g_recv.at[n, slot], t, cand)

    def ready(n):
        landed(places[n](c), g_own.at[n])

    def step1z(n):
        here = places[n](c)
        g_send_to(n, 0, here, here, cz)

    def step1x(n):
        here = places[n](c)
        g_send_to(n, 1, here, here, cp)
        g_send_to(n, 2, here, here, cm)

    def step1(n):
        step1z(n)
        step1x(n)

    def step2a(n):
        at_ = places[n]
        landed(at_(cz), g_recv.at[n, 0])
        g_send_to(n, 3, at_(cz), at_(cz), cp)
        g_send_to(n, 4, at_(cz), at_(cz), cm)

    def step2b(n):
        at_ = places[n]
        landed(at_(cm), g_recv.at[n, 1])
        g_send_to(n, 5, at_(cm, 0), at_(cm, 0), cp)
        landed(at_(cp), g_recv.at[n, 2])
        g_send_to(n, 6, at_(cp, 1), at_(cp, 1), cm)

    def step2(n):
        step2a(n)
        step2b(n)

    def step3(n):
        at_ = places[n]
        landed(at_(cmz), g_recv.at[n, 3])
        g_send_to(n, 7, at_(cmz, 0), at_(cmz, 0), cp)
        landed(at_(cpz), g_recv.at[n, 4])
        g_send_to(n, 8, at_(cpz, 1), at_(cpz, 1), cm)

    def across(which):
        for cc in which:
            send(v_at(cc), v_at(cc), g_dsend.at[4], g_dual.at[4], partner, c)

    def step4(n):
        at_ = places[n]
        landed(at_(co, 0), g_recv.at[n, 5])
        landed(at_(co, 1), g_recv.at[n, 6])
        landed(at_(coz, 0), g_recv.at[n, 7])
        landed(at_(coz, 1), g_recv.at[n, 8])
        if n < 5:
            if n < 4:
                send(whole[n](k), whole[n](k), g_dsend.at[n], g_dual.at[n], partner, c)
            else:
                across((cmz, cpz, co, coz))

    def both(n):
        landed(whole[n](1 - k), g_dual.at[n])


    own_copies()

    x_copy.wait()
    for copy in small:
        copy.wait()

    @pl.loop(0, 8)
    def _(i):
        rows = xv[i].astype(F32)
        nx[pl.ds(pl.multiple_of(32 * i, 32), 32), :] = rms(rows, gain1[...]).astype(BF)

    pl.semaphore_wait(barrier, TOK - 1 + 2 * (CAND - 1))

    ready(0)
    ready(1)
    step1(0)
    step1(1)

    for n, (src, dst) in enumerate(((keys, kb), (vals, vb))):
        here = dst.at[pl.ds(512 * c + 16 * t, 16), :]
        pltpu.make_async_copy(
            src.at[k, pl.ds(16 * c, 16), pl.ds(pl.multiple_of(128 * j, 128), 128)],
            here, l_sem.at[1 + n],
        ).start()

        @pl.loop(1, TOK)
        def _(d, src=src, n=n, here=here):
            to = lax.rem(t + d, TOK)
            send(
                src.at[
                    lax.rem(to, 2), pl.ds(16 * c, 16),
                    pl.ds(pl.multiple_of(128 * lax.div(to, 2), 128), 128),
                ],
                here, kv_send.at[n], kv_recv.at[n], to, c,
            )

    def value_far():
        for n, cc in enumerate((co, coz)):
            here = vb.at[pl.ds(512 * cc + 16 * t, 16), :]
            pltpu.make_async_copy(
                vals.at[k, pl.ds(16 * cc, 16), pl.ds(pl.multiple_of(128 * j, 128), 128)],
                here, l_sem.at[3 + n],
            ).start()

            @pl.loop(1, TOK)
            def _(d, here=here, cc=cc):
                to = lax.rem(t + d, TOK)
                send(
                    vals.at[
                        lax.rem(to, 2), pl.ds(16 * cc, 16),
                        pl.ds(pl.multiple_of(128 * lax.div(to, 2), 128), 128),
                    ],
                    here, kv_send.at[2], kv_recv.at[2], to, c,
                )

    def value_end():
        for n, cc in enumerate((co, coz)):
            pltpu.make_async_copy(
                vb.at[pl.ds(0, 16), :], vb.at[pl.ds(512 * cc + 16 * t, 16), :], l_sem.at[3 + n]
            ).wait()
        landed(vb.at[pl.ds(0, 992), :], kv_recv.at[2])
        at_ = places[6]
        for slot, came in ((1, cm), (2, cp), (3, cmz), (4, cpz)):
            landed(at_(came), g_recv.at[6, slot])

    def kv_mine(n):
        ref = (kb, vb)[n]
        pltpu.make_async_copy(
            ref.at[pl.ds(0, 16), :], ref.at[pl.ds(512 * c + 16 * t, 16), :], l_sem.at[1 + n]
        ).wait()
        landed(ref.at[pl.ds(0, 496), :], kv_recv.at[n])

    ready(2)
    ready(3)
    step1(2)
    step1(3)
    step2(0)
    step2(1)
    step3(0)
    step3(1)
    kv_mine(0)
    step1(5)
    kv_mine(1)
    step1(6)
    value_far()
    ready(4)
    step1z(4)
    step4(0)
    step4(1)
    both(0)
    zero = jnp.zeros((ROWS, 64), BF)
    query = jnp.zeros((ROWS, 128), F32)
    for cc in range(CAND):
        query = query + dot_t(nx[:, 256 * cc : 256 * cc + 256], wq[cc])
    query = query.astype(BF)
    q2[pl.ds(0, ROWS), :] = jnp.concatenate([query[:, :64], zero], axis=1)
    q2[pl.ds(ROWS, ROWS), :] = jnp.concatenate([zero, query[:, 64:]], axis=1)

    length = lens[k]

    def score(cc, opening=False):
        place = lax.broadcasted_iota(jnp.int32, (1, 512), 1)
        token = lax.div(place, 16) * 128 + 16 * cc + lax.rem(place, 16)
        live = token < length
        block = kb[pl.ds(pl.multiple_of(512 * cc, 512), 512), :]

        for r in range(4):
            rows = pl.ds(128 * r, 128)
            s = dot_t(q2[rows, :], block)
            s = jnp.where(live, s, NEG)
            sc[cc, rows, :] = s
            high = jnp.maximum(
                jnp.maximum(s[:, :128], s[:, 128:256]), jnp.maximum(s[:, 256:384], s[:, 384:])
            )
            st[rows, :] = high if opening else jnp.maximum(st[rows, :], high)

    step2(5)
    score(c, True)
    score(cz)
    score(cm)
    step3(5)
    step2a(6)
    score(cp)
    score(cmz)
    score(cpz)
    step4(5)
    score(co)
    score(coz)
    step2(2)
    step2(3)

    for r in range(8):
        rows = pl.ds(64 * r, 64)
        top = jnp.max(st[rows, :], axis=1, keepdims=True)
        total = jnp.zeros((64, 256), F32)
        for at in range(16):
            w = jnp.exp(sc[at // 2, rows, pl.ds(256 * (at % 2), 256)] - top)
            total = total + w
            pb[rows, pl.ds(256 * at, 256)] = w.astype(BF)
        st[rows, :] = jnp.broadcast_to(jnp.sum(total, axis=1, keepdims=True), (64, 128))

    both(1)
    value_end()

    def y_rows(dy):
        return pl.ds(pl.multiple_of(64 * lax.rem(y + dy, NY), 64), 64)

    def z_rows(dz):
        return pl.ds(pl.multiple_of(16 * lax.rem(z + dz, NZ), 16), 16)

    def yz_rows(dy, dz):
        at_row = 64 * lax.rem(y + dy, NY) + 16 * lax.rem(z + dz, NZ)
        return pl.ds(pl.multiple_of(at_row, 16), 16)

    order = (2, 1, 3, 0)

    def sums_send(p):
        for dz in order:
            for dy in (2, 1, 3):
                n = 4 * (dy - 1) + dz
                send(
                    part.at[p, :, yz_rows(dy, dz), :], ry.at[p, dy - 1, :, z_rows(dz), :],
                    rs_send.at[p, n], rs_recv.at[p, n], tok_of(y + dy, z), c,
                )

    def sums_end(p, mid, tail):
        for dz in order:
            zr = z_rows(dz)
            total = part[p, :, yz_rows(0, dz), :].astype(F32)
            for dy in (1, 3, 2):
                landed(ry.at[p, dy - 1, :, zr, :], rs_recv.at[p, 4 * (dy - 1) + dz])
                total = total + ry[p, dy - 1, :, zr, :].astype(F32)
            by[p, :, zr, :] = total.astype(BF)
            if dz:
                send(
                    by.at[p, :, zr, :], rz.at[p, dz - 1], rs_send.at[p, 11 + dz],
                    rs_recv.at[p, 11 + dz], tok_of(y, z + dz), c,
                )
            if dz == 2:
                mid()
        tail()
        total = by[p, :, z_rows(0), :].astype(F32)
        for dz in (1, 3, 2):
            landed(rz.at[p, dz - 1], rs_recv.at[p, 11 + dz])
            total = total + rz[p, dz - 1].astype(F32)
        return jnp.concatenate([total[0], total[1]], axis=1)

    def spread(p, value, work, early, late):
        nf[p, 0, yz_rows(0, 0), :] = value[:, :HALF]
        nf[p, 1, yz_rows(0, 0), :] = value[:, HALF:]

        def go(n, rows, tok):
            where = nf.at[p, :, rows, :]
            send(where, where, ag_send.at[p, n], ag_recv.at[p, n], tok, c)

        def along_y(dz):
            for dy in (2, 1, 3):
                go(4 * (dy - 1) + dz, yz_rows(0, dz), tok_of(y + dy, z))

        for dz in (2, 1, 3):
            go(11 + dz, yz_rows(0, 0), tok_of(y, z + dz))
        along_y(0)
        early()
        for dz in (1, 3, 2):
            landed(nf.at[p, :, yz_rows(0, 4 - dz), :], ag_recv.at[p, 11 + dz])
            along_y(4 - dz)
        late()
        work((0,))
        for dz in (0, 3, 1, 2):
            for dy in (1, 3, 2):
                landed(nf.at[p, :, yz_rows(4 - dy, dz), :], ag_recv.at[p, 4 * (dy - 1) + dz])
        work((2, 1, 3))

    def blocks(p, cc, dys):
        pieces = [nf[p, cc // 4, y_rows(dy), pl.ds(256 * (cc % 4), 256)] for dy in dys]
        return pieces[0] if len(pieces) == 1 else jnp.concatenate(pieces, axis=0)

    halves = [
        jnp.dot(pb[pl.ds(ROWS * h, ROWS), :], vb[...], preferred_element_type=F32)
        / st[pl.ds(ROWS * h, ROWS), :]
        for h in range(2)
    ]
    lane = lax.broadcasted_iota(jnp.int32, (ROWS, 128), 1)
    attended = jnp.where(lane < 64, halves[0], halves[1]).astype(BF)
    for cc in range(CAND):
        part[0, cc // 4, :, pl.ds(256 * (cc % 4), 256)] = jnp.dot(
            attended, wo[cc], preferred_element_type=F32
        ).astype(BF)
    sums_send(0)

    def mid_0():
        step3(2)
        step3(3)
        step1x(4)
        step2a(4)

    mine = xv[2 * y + lax.div(z, 2), pl.ds(pl.multiple_of(16 * lax.rem(z, 2), 16), 16), :]
    ac[...] = mine.astype(F32) + sums_end(0, mid_0, lambda: None)

    def feed(dys):
        gate = up = jnp.zeros((64 * len(dys), 320), F32)
        for cc in range(CAND):
            block = blocks(0, cc, dys)
            gate = gate + dot_t(block, wi[0, cc])
            up = up + dot_t(block, wi[1, cc])
        hidden = (gelu(gate) * up).astype(BF)
        for cc in range(CAND):
            down = jnp.dot(hidden, fo[cc], preferred_element_type=F32).astype(BF)
            for n, dy in enumerate(dys):
                part[1, cc // 4, y_rows(dy), pl.ds(256 * (cc % 4), 256)] = down[
                    64 * n : 64 * n + 64
                ]
        if len(dys) > 1:
            sums_send(1)

    def early_0():
        step4(2)
        step4(3)

    def late_0():
        both(2)
        both(3)
        step2b(4)

    spread(0, rms(ac[...], gain2[...]).astype(BF), feed, early_0, late_0)
    def mid_1():
        step3(4)
        across((c, cz, cm, cp))

    after = ac[...] + sums_end(1, mid_1, lambda: step4(4))

    ids = gold[k].astype(F32)
    eye = lax.broadcasted_iota(jnp.int32, (32, 32), 0) == lax.broadcasted_iota(jnp.int32, (32, 32), 1)
    start = [((2 * j + h) * width).astype(F32) for h in range(2)]

    def gold_rows():
        for i in range(8):
            column = jnp.sum(
                jnp.where(eye, jnp.broadcast_to(ids[i : i + 1, :], (32, 32)), 0.0),
                axis=1, keepdims=True,
            )
            st[pl.ds(32 * i, 32), :] = jnp.broadcast_to(column, (32, 128))

    def vocab(dys):
        size = 64 * len(dys)
        wanted = [st[y_rows(dy), :][:, :1] for dy in dys]
        wanted = wanted[0] if len(dys) == 1 else jnp.concatenate(wanted, axis=0)
        logits = []
        for h in range(2):
            one = jnp.zeros((size, width), F32)
            for cc in range(CAND):
                one = one + dot_t(blocks(1, cc, dys), wv[h, cc])
            logits.append(one)
        high = jnp.maximum(
            jnp.max(logits[0], axis=1, keepdims=True), jnp.max(logits[1], axis=1, keepdims=True)
        )
        total = jnp.zeros((size, 1), F32)
        picked = jnp.zeros((size, 1), F32)
        for h in range(2):
            total = total + jnp.sum(jnp.exp(logits[h] - high), axis=1, keepdims=True)
            at_col = lax.broadcasted_iota(jnp.int32, (size, width), 1).astype(F32) + start[h]
            picked = picked + jnp.sum(
                jnp.where(at_col == wanted, logits[h], 0.0), axis=1, keepdims=True
            )
        lane = lax.broadcasted_iota(jnp.int32, (size, 128), 1)
        found = jnp.where(lane == 0, high, jnp.where(lane == 1, total, picked))
        for n, dy in enumerate(dys):
            at_row = 256 + 64 * lax.rem(y + dy, NY)
            st[pl.ds(pl.multiple_of(at_row, 64), 64), :] = found[64 * n : 64 * n + 64]

    def early_1():
        gold_rows()

    spread(1, rms(after, gain3[...]).astype(BF), vocab, early_1, lambda: both(4))

    stats = st[pl.ds(256, 256), :].T
    f1[j] = stats[0:8, :]

    @pl.loop(1, 16)
    def _(d):
        to = lax.rem(j + d, 16) * 2 + k
        send(f1.at[j], f1.at[j], f_send.at[0], f_recv.at[0], to, c)

    landed(f1.at[pl.ds(0, 15)], f_recv.at[0])
    top = f1[0][0:1, :]
    for n in range(1, 16):
        top = jnp.maximum(top, f1[n][0:1, :])
    total = jnp.zeros((1, ROWS), F32)
    picked = jnp.zeros((1, ROWS), F32)
    for n in range(16):
        total = total + f1[n][1:2, :] * jnp.exp(f1[n][0:1, :] - top)
        picked = picked + f1[n][2:3, :]
    logprob = picked - top - jnp.log(total)
    group = lax.div(lax.broadcasted_iota(jnp.int32, (8, ROWS), 1), 32)
    whose = lax.broadcasted_iota(jnp.int32, (8, ROWS), 0)
    per = jnp.sum(jnp.where(group == whose, logprob, 0.0), axis=1, keepdims=True) * (1.0 / 32)
    diag = lax.broadcasted_iota(jnp.int32, (8, 128), 0) == lax.broadcasted_iota(jnp.int32, (8, 128), 1)
    row = jnp.sum(jnp.where(diag, per, 0.0), axis=0, keepdims=True)
    f2[8 * k + c] = jnp.broadcast_to(row, (8, 128))

    @pl.loop(1, CAND)
    def _(d):
        to = lax.rem(c + d, CAND)
        send(f2.at[8 * k + c], f2.at[8 * k + c], f_send.at[1], f_recv.at[1], t, to)
        send(f2.at[8 * k + c], f2.at[8 * k + c], f_send.at[1], f_recv.at[1], partner, to)

    send(f2.at[8 * k + c], f2.at[8 * k + c], f_send.at[1], f_recv.at[1], partner, c)
    landed(f2.at[pl.ds(0, 15)], f_recv.at[1])
    lane = lax.broadcasted_iota(jnp.int32, (8, 8, 128), 2)
    cand = lax.broadcasted_iota(jnp.int32, (8, 8, 128), 0) * 8 + lane
    own_lane = lax.broadcasted_iota(jnp.int32, (1, 128), 1)
    for b in range(2):
        count = counts[b]
        inside = jnp.where((cand < count) & (lane < 8), f2[pl.ds(8 * b, 8)], NEG)
        own = jnp.where(own_lane + 8 * c < count, f2[8 * b + c][0:1, :], 0.0)
        out[pl.ds(b, 1), :] = jnp.where(own_lane < 8, own, jnp.max(inside))

    for n in range(2):
        landed(kb.at[pl.ds(0, 496), :], kv_send.at[n])
    landed(kb.at[pl.ds(0, 992), :], kv_send.at[2])
    for n in range(7):
        at_ = places[n]
        for slot in range(5 if n == 6 else 9):
            landed(at_(c) if slot < 5 else at_(c, (slot - 5) % 2), g_send.at[n, slot])
        if n < 5:
            landed(whole[n](k), g_dsend.at[n])
    @pl.loop(0, 2)
    def _(p):
        @pl.loop(0, 15)
        def _(n):
            landed(rz.at[p, 0], rs_send.at[p, n])
            landed(rz.at[p, 0], ag_send.at[p, n])

    landed(f1.at[pl.ds(0, 15)], f_send.at[0])
    landed(f2.at[pl.ds(0, 15)], f_send.at[1])


def body(
    dec_hidden, enc_keys, enc_values, enc_lengths, cand_counts, gold_ids, gain_cross, w_query,
    w_out, gain_ffn, w_in_gate, w_in_up, w_ffn_out, gain_final, w_vocab,
):
    units = w_in_gate.shape[1]
    width = w_vocab.shape[1]
    anywhere = pl.BlockSpec(memory_space=pl.ANY)
    vmem = pl.BlockSpec(memory_space=pltpu.VMEM)
    dma = pltpu.SemaphoreType.DMA
    found = pl.pallas_call(
        kernel,
        name="layer",
        out_shape=jax.ShapeDtypeStruct((2, 128), F32),
        in_specs=[anywhere] * 15,
        out_specs=vmem,
        scratch_shapes=[
            pltpu.VMEM((8, 32, D), BF),
            pltpu.VMEM((ROWS, D), BF),
            pltpu.VMEM((2 * ROWS, 128), BF),
            pltpu.VMEM((4096, 128), BF),
            pltpu.VMEM((4096, 128), BF),
            pltpu.VMEM((8, 2 * ROWS, 512), F32),
            pltpu.VMEM((2 * ROWS, 4096), BF),
            pltpu.VMEM((8, 128, 256), BF),
            pltpu.VMEM((8, 128, 256), BF),
            pltpu.VMEM((2, 8, 2 * units, 256), BF),
            pltpu.VMEM((8, 2 * units, 256), BF),
            pltpu.VMEM((2, 8, width, 256), BF),
            pltpu.VMEM((2, 2, ROWS, HALF), BF),
            pltpu.VMEM((2, 3, 2, 64, HALF), BF),
            pltpu.VMEM((2, 2, 64, HALF), BF),
            pltpu.VMEM((2, 3, 2, 16, HALF), BF),
            pltpu.VMEM((16, D), F32),
            pltpu.VMEM((2, 2, ROWS, HALF), BF),
            pltpu.VMEM((2 * ROWS, 128), F32),
            pltpu.VMEM((16, 8, ROWS), F32),
            pltpu.VMEM((16, 8, 128), F32),
            pltpu.SMEM((2,), jnp.int32),
            pltpu.SMEM((2,), jnp.int32),
            pltpu.VMEM(gold_ids.shape, jnp.int32),
            pltpu.VMEM((1, D), F32),
            pltpu.VMEM((1, D), F32),
            pltpu.VMEM((1, D), F32),
            dma((3,)), dma((3,)), dma((7, 9)), dma((7, 9)), dma((5,)), dma((5,)), dma((5,)),
            dma((2, 15)), dma((2, 15)), dma((2, 15)), dma((2, 15)), dma((2,)), dma((2,)), dma((5,)), dma((6,)),
        ],
        compiler_params=pltpu.CompilerParams(
            collective_id=0, has_side_effects=True, vmem_limit_bytes=62 * 1024 * 1024
        ),
    )(
        dec_hidden, enc_keys, enc_values, enc_lengths, cand_counts, gold_ids,
        gain_cross.reshape(1, -1), w_query.T, w_out, gain_ffn.reshape(1, -1), w_in_gate.T, w_in_up.T,
        w_ffn_out,
        gain_final.reshape(1, -1), w_vocab.T,
    )
    return found[:, :8], found[:, 8]


def solution(mesh):
    in_specs = (
        P(None, "cand", None, None), P(None, "tok", None), P(None, "tok", None), P(), P(),
        P(None, "cand", None), P(), P("cand", "tok"), P("tok", "cand"), P(), P("cand", "tok"),
        P("cand", "tok"), P("tok", "cand"), P(), P("cand", "tok"),
    )
    return jax.shard_map(
        body, mesh=mesh, in_specs=in_specs, out_specs=(P(None, "cand"), P()), check_vma=False
    )
```
